128 devices in a mesh: aux: 8 (over z, core), orb: 16 (over x, y).
Axes of the slice: x: 4, y: 4, z: 4, core: 2. Of those that a mesh axis runs over, the one named last changes fastest.
Arguments:
- half: bfloat16 [128, 384, 3072], P('aux', 'orb'), may hold values from -1 to 1
- metric: bfloat16 [128, 128], P('aux'), may hold values from -1 to 2
- survive: int32 [8, 16, 24], P('aux', 'orb'), may hold values 0 or 1
Outputs:
- exchange_k: float32 [3072, 3072], P('orb', 'aux')
The draws below stay inside these ranges and needn't reach their ends.
All inputs are finite; a program needn't handle non-finite values. No bound on the sum of `survive` on one device may be relied on, other than what follows from the above.
Results may differ from the reference program's by a relative error of at most 0.00098.
Values may be sent and summed in bfloat16 or wider, within the bound.
A program may use at most 128 MiB of HBM per device.

```python
import jax
import jax.numpy as jnp
from jax import lax

NOCC = 384
OCCB = 24
NAO = 3072
AOBLK = 128
NAUX = 128
N_AUX = 8


def draw_metric(key, part):
    first_key = jax.random.fold_in(key, 11)
    second_key = jax.random.fold_in(key, 12)
    spread = jax.random.normal(first_key, (NAUX, NAUX), jnp.float32) * (0.6 / NAUX ** 0.5)
    diagonal_part = jax.random.uniform(second_key, (NAUX,), jnp.float32, 0.9, 1.1)
    return (spread + jnp.diag(diagonal_part)).astype(jnp.bfloat16)


def set_ends(entries, own_key, low, largest):
    shape = entries.shape
    place = [jax.random.randint(jax.random.fold_in(own_key, axis), (), 0, shape[axis]) for axis in range(len(shape))]
    entries = entries.at[tuple(place)].set(low)
    longest = shape.index(max(shape))
    place[longest] = (place[longest] + 1) % shape[longest]
    return entries.at[tuple(place)].set(largest)


def steps_of(key, shape, cuts, low, largest):
    def one(axis_at, shards_of):
        draws = jax.random.uniform(jax.random.fold_in(jax.random.fold_in(key, 6), axis_at), (shards_of,), jnp.float32, low / len(cuts), largest / len(cuts))
        return jnp.repeat(jnp.exp(draws), shape[axis_at] // shards_of).reshape((-1,) + (1,) * (len(shape) - axis_at - 1))

    level = one(*cuts[0])
    for cut in cuts[1:]:
        level = level * one(*cut)
    return level


def bell_draw(key, shape, scale, most, shards=(), kind=jnp.bfloat16):
    factor_of = steps_of(key, shape, shards, -0.22, 0.18) if shards else 1.0
    values = jax.random.normal(key, shape, jnp.float32) * scale * factor_of
    return jnp.minimum(jnp.maximum(values, -most), most).astype(kind)


def setup_inputs(seed: int = 0) -> dict:
    key_of = jax.random.split(jax.random.key(seed), 4)
    half = bell_draw(key_of[0], (NAUX, NOCC, NAO), ((NAUX * NOCC) ** -0.25), 1.0, ((0, 8), (1, 16)))
    metric = draw_metric(jax.random.fold_in(key_of[3], 71), 0)
    survive = set_ends((jax.random.randint(key_of[2], (N_AUX, NOCC // OCCB, NAO // AOBLK), 0, 3) < 2).astype(jnp.int32), jax.random.fold_in(key_of[2], 1), 0, 1)
    return dict(half=half, metric=metric, survive=survive)


def reference(half, metric, survive):
    blocks_aux, blocks_occ, blocks_ao = survive.shape
    aux_count, occ_count, ao_count = half.shape
    gate = survive.astype(jnp.bfloat16)
    shaped = half.reshape(blocks_aux, aux_count // blocks_aux, blocks_occ, occ_count // blocks_occ, blocks_ao, ao_count // blocks_ao)
    masked = (shaped * gate[:, None, :, None, :, None]).reshape(aux_count, occ_count, ao_count)
    occ_width = occ_count // blocks_occ

    def accumulate(totals, block_index):
        occ_rows = lax.dynamic_slice_in_dim(masked, block_index * occ_width, occ_width, 1)
        fitted = jnp.dot(metric, occ_rows.reshape(aux_count, -1), preferred_element_type=jnp.float32)
        fitted = fitted.astype(jnp.bfloat16).reshape(-1, ao_count)
        update = lax.dot_general(fitted, fitted, (((0,), (0,)), ((), ())), preferred_element_type=jnp.float32)
        return totals + update, None

    exchange_k, _ = lax.scan(accumulate, jnp.zeros((ao_count, ao_count), jnp.float32), jnp.arange(blocks_occ, dtype=jnp.int32))
    return exchange_k
```

```python
import jax
import jax.numpy as jnp
import numpy as np
from jax import lax
from jax.experimental import pallas as pl
from jax.experimental.pallas import tpu as pltpu
from jax.sharding import PartitionSpec as P

MESH = pl.DeviceIdType.MESH
CH = 384
NCH = 8
TR = 192
HR = 96
TOP = 32700.0
TINY = 1e-36


def perm_matrix():
    m = np.zeros((CH, CH), np.float32)
    for d in range(8):
        for aux in range(16):
            for i in range(3):
                m[d * 48 + aux * 3 + i, aux * 24 + 3 * d + i] = 1.0
    return m


def kernel(half, mask, kron, perm, out, snd, rcv, rel, m3, fb, ft, dv, cs, csi, rb, rbi,
           s1f, s1n, r1f, r1n, kown, s2f, s2n, r2f, r2n, s3, r3, s4, r4,
           p1s, p1r, rls, rlr, fws, ks, kr, fs, fr, ds_, dr,
           q1fs, q1fr, q1ns, q1nr, q2fs, q2fr, q2ns, q2nr, q3s, q3r, q4s, q4r):
    f32 = jnp.float32
    aux = lax.axis_index("aux")
    orb = lax.axis_index("orb")
    z, c = aux // 2, aux % 2
    x, y = orb // 4, orb % 4
    me1 = x * (1 - c) + y * c
    me2 = y * (1 - c) + x * c
    sib = 2 * z + 1 - c

    def row_of(t, u):
        return t * (4 - 3 * c) + u * (1 + 3 * c)

    def ring1(o):
        return (aux, row_of((me1 + o) % 4, me2))

    def ring2(o):
        return (aux, row_of(me1, (me2 + o) % 4))

    def zdev(o, core):
        return (2 * ((z + o) % 4) + core, orb)

    pr = orb // 2
    mirror = [(2 * aux + h, pr) for h in range(2)]
    has_mirror = aux != pr

    bar = pltpu.get_barrier_semaphore()
    for o in range(1, 8):
        pl.semaphore_signal(bar, inc=1, device_id=((aux + o) % 8, orb), device_id_type=MESH)
    for o in range(1, 4):
        pl.semaphore_signal(bar, inc=1, device_id=ring1(o), device_id_type=MESH)
        pl.semaphore_signal(bar, inc=1, device_id=ring2(o), device_id_type=MESH)

    @pl.when(has_mirror)
    def _():
        for o, a in mirror:
            pl.semaphore_signal(bar, inc=1, device_id=(a, o), device_id_type=MESH)
        pl.semaphore_wait(bar, 15)

    @pl.when(jnp.logical_not(has_mirror))
    def _():
        pl.semaphore_wait(bar, 13)

    def rcopy(src, dst, ss, rs, dev):
        return pltpu.make_async_remote_copy(src_ref=src, dst_ref=dst, send_sem=ss, recv_sem=rs,
                                            device_id=dev, device_id_type=MESH)

    def al48(v):
        return pl.ds(pl.multiple_of(v * 48, 16), 48)

    def al96(v):
        return pl.ds(pl.multiple_of(v * 96, 16), 96)

    def krcopy(o):
        dst = m3.at[al48(aux)]
        return rcopy(kron, dst, ks.at[o], kr.at[o], ((aux + o) % 8, orb))

    for o in range(1, 8):
        krcopy(o).start()
    m3[al48(aux), :] = kron[...]

    step = 1 - 2 * c + 4
    zr = (z + step) % 4
    zf = (z + 4 - (step - 4)) % 4

    def near(q, o, core):
        dst_dev = zdev(o, core)
        rows = 2 * ((z + o) % 4) + core
        return rcopy(snd.at[q, al48(rows)], rcv.at[q, al48(aux)],
                     p1s.at[q, 2 * (o - 1) + core], p1r.at[q, aux], dst_dev)

    def sibling(q):
        return rcopy(snd.at[q, al48(sib)], rcv.at[q, al48(aux)], p1s.at[q, 2], p1r.at[q, aux], (sib, orb))

    def relay(q):
        return rcopy(snd.at[q, al96((z + 2) % 4)], rel.at[q], rls.at[q], rlr.at[q], (2 * zr + c, orb))

    def forward(q, core):
        src_aux = 2 * zf + c
        return rcopy(rel.at[q, pl.ds(48 * core, 48)], rcv.at[q, al48(src_aux)],
                     fws.at[q, core], p1r.at[q, src_aux], (2 * zr + core, orb))

    def arrival(q, a):
        return rcopy(rcv.at[q, al48(a)], rcv.at[q, al48(a)], p1s.at[q, 0], p1r.at[q, a], (sib, orb))

    def cut(q):
        return pl.ds(pl.multiple_of(q * CH, 128), CH)

    @pl.loop(0, NCH)
    def _(q):
        block = half[:, cut(q)] * mask[:, cut(q)]
        snd[q] = jnp.dot(perm[...], block, preferred_element_type=f32).astype(jnp.bfloat16)
        relay(q).start()
        for core in range(2):
            near(q, 1, core).start()
            near(q, 3, core).start()
        sibling(q).start()
        rcv[q, al48(aux), :] = snd[q, al48(aux), :]

    for o in range(1, 8):
        src = (aux + 8 - o) % 8
        rcopy(kron, m3.at[al48(src)], ks.at[o], kr.at[o], (sib, orb)).wait_recv()

    def fcopy(q):
        return rcopy(fb.at[q, pl.ds(0, CH)], fb.at[q, pl.ds(CH, CH)], fs.at[q], fr.at[q], (sib, orb))

    @pl.loop(0, NCH)
    def _(q):
        relay(q).wait_recv()
        for core in range(2):
            forward(q, core).start()

    @pl.loop(0, NCH)
    def _(q):
        for o in range(1, 8):
            arrival(q, (aux + o) % 8).wait_recv()
        fb[q, 0:CH, :] = jnp.dot(m3[...], rcv[q], preferred_element_type=f32).astype(jnp.bfloat16)
        fcopy(q).start()

    @pl.loop(0, NCH)
    def _(q):
        fcopy(q).wait_recv()
        both = fb[q]
        ft[q] = both.T
        wide = both.astype(f32)
        dv[0, pl.ds(q, 1), :] = jnp.sum(wide * wide, axis=0, keepdims=True)

    def tables(first, terms):
        for n, val in enumerate(terms):
            val = jnp.maximum(val, TINY)
            lane = lax.broadcasted_iota(jnp.int32, val.shape, 1)
            inv = lax.rsqrt(val)
            csi[first + n] = inv
            cs[first + n] = val * inv
            for h in range(2):
                part = jnp.where((lane >= TR) == (h == 1), val, TINY)
                top = jnp.broadcast_to(jnp.max(part, axis=1, keepdims=True), val.shape)
                tinv = lax.rsqrt(top)
                rbi[first + n, h] = tinv * TOP
                rb[first + n, h] = top * tinv * (1.0 / TOP)

    def gather(level, dev):
        base = 4 * level
        for o in range(1, 4):
            rcopy(dv.at[base], dv.at[base + 4 - o], ds_.at[base + o], dr.at[base + 4 - o], dev(o)).start()

    def gathered(level, dev):
        base = 4 * level
        for o in range(1, 4):
            rcopy(dv.at[base], dv.at[base + o], ds_.at[base + o], dr.at[base + o], dev(o)).wait_recv()
        return [dv[base + o] for o in range(4)]

    def ring_terms(d):
        return [d[0], d[3], d[1], d[0] + d[3], d[0] + d[1], d[3] + d[2], d[1] + d[2]]

    gather(0, ring1)
    d0 = gathered(0, ring1)
    tables(0, ring_terms(d0))
    dv[4] = d0[0] + d0[1] + d0[2] + d0[3]
    gather(1, ring2)

    def enc(val, n, h, p, q):
        inv = csi[n, pl.ds(q, 1), :] * rbi[n, h, pl.ds(p, 1), :]
        return jnp.round(val * inv).astype(jnp.int32).astype(jnp.int16)

    def dec(val, n, h, p, q):
        sc = cs[n, pl.ds(q, 1), :] * rb[n, h, pl.ds(p, 1), :]
        return val.astype(jnp.int32).astype(f32) * sc

    def where(t, u, m):
        r = row_of(t, u)
        p = r // 2
        k = (p + c) % 2 + 2 * m
        return r % 2, p, (p + k) % 8, k + p // 4 <= 4

    def ktile(h, p, q):
        rows = ft[p, pl.ds(pl.multiple_of(h * TR, 64), TR), :]
        return jnp.dot(rows, fb[q], preferred_element_type=f32)

    tp, tm, tf = (me1 + 1) % 4, (me1 + 3) % 4, (me1 + 2) % 4

    def slot(j):
        ju = j // 3
        off = (2 + 3 * ju + 3 * (ju // 2) - 2 * (ju // 3)) % 4
        return (me2 + off) % 4, j % 3

    def far1(i, half_at):
        rows = pl.ds(half_at * HR, HR)
        dst = 0 if half_at == 0 else 1
        return rcopy(s1f.at[i, rows], r1f.at[dst, i], q1fs.at[i, half_at], q1fr.at[dst, i],
                     ring1(1 if half_at == 0 else 3))

    def near1(i, way):
        return rcopy(s1n.at[way, i], r1n.at[way, i], q1ns.at[way, i], q1nr.at[way, i],
                     ring1(1 if way == 0 else 3))

    @pl.loop(0, 12)
    def _(j):
        u, m = slot(j)
        h, p, q, ok = where(tf, u, m)
        i = u * 3 + m

        @pl.when(ok)
        def _():
            s1f[i] = enc(ktile(h, p, q), 0, h, p, q)
            far1(i, 0).start()
            far1(i, 1).start()

    @pl.loop(0, 12)
    def _(j):
        u, m = slot(j)
        i = u * 3 + m
        for way, t in ((0, tp), (1, tm)):
            h, p, q, ok = where(t, u, m)

            @pl.when(ok)
            def _():
                tile = ktile(h, p, q)
                far1(i, way).wait_recv()
                add = dec(r1f[way, i], 1 + way, h, p, q)
                low, high = tile[:HR], tile[HR:]
                if way == 0:
                    low = low + add
                else:
                    high = high + add
                s1n[way, i, 0:HR, :] = enc(low, 3 + way, h, p, q)
                s1n[way, i, HR:TR, :] = enc(high, 3 + way, h, p, q)
                near1(i, way).start()

    d1 = gathered(1, ring2)
    tables(7, ring_terms(d1))
    dv[8] = d1[0] + d1[1] + d1[2] + d1[3]

    def zline(o):
        return zdev(o, c)

    gather(2, zline)

    def own1(u, m, then):
        h, p, q, ok = where(me1, u, m)
        i = u * 3 + m

        @pl.when(ok)
        def _():
            tile = ktile(h, p, q)
            near1(i, 0).wait_recv()
            near1(i, 1).wait_recv()
            tile = tile + dec(r1n[0, i], 5, h, p, q) + dec(r1n[1, i], 6, h, p, q)
            then(tile, h, p, q)

    def far2(m, half_at):
        rows = pl.ds(half_at * HR, HR)
        dst = 0 if half_at == 0 else 1
        return rcopy(s2f.at[m, rows], r2f.at[dst, m], q2fs.at[m, half_at], q2fr.at[dst, m],
                     ring2(1 if half_at == 0 else 3))

    def near2(m, way):
        return rcopy(s2n.at[way, m], r2n.at[way, m], q2ns.at[way, m], q2nr.at[way, m],
                     ring2(1 if way == 0 else 3))

    uf, up, um = (me2 + 2) % 4, (me2 + 1) % 4, (me2 + 3) % 4

    @pl.loop(0, 3)
    def _(m):
        def then(tile, h, p, q):
            s2f[m] = enc(tile, 7, h, p, q)
            far2(m, 0).start()
            far2(m, 1).start()

        own1(uf, m, then)

    for way, u in ((0, up), (1, um)):
        @pl.loop(0, 3)
        def _(m):
            def then(tile, h, p, q):
                far2(m, way).wait_recv()
                add = dec(r2f[way, m], 8 + way, h, p, q)
                low, high = tile[:HR], tile[HR:]
                if way == 0:
                    low = low + add
                else:
                    high = high + add
                s2n[way, m, 0:HR, :] = enc(low, 10 + way, h, p, q)
                s2n[way, m, HR:TR, :] = enc(high, 10 + way, h, p, q)
                near2(m, way).start()

            own1(u, m, then)

    d2 = gathered(2, zline)
    tables(14, d2)

    def last(m, o):
        return rcopy(s3.at[m], r3.at[o - 1], q3s.at[m], q3r.at[o - 1], zdev(4 - o, c))

    @pl.loop(0, 3)
    def _(m):
        def then(tile, h, p, q):
            near2(m, 0).wait_recv()
            near2(m, 1).wait_recv()
            tile = tile + dec(r2n[0, m], 12, h, p, q) + dec(r2n[1, m], 13, h, p, q)
            kown[m] = tile
            o = (z + 4 - q // 2) % 4

            @pl.when(o > 0)
            def _():
                s3[m] = enc(tile, 14, h, p, q)
                last(m, o).start()

        own1(me2, m, then)

    def mir(h):
        return rcopy(s4.at[h], r4.at[orb % 2], q4s.at[h], q4r.at[orb % 2], (mirror[h][1], mirror[h][0]))

    kk = (aux + 8 - pr) % 8
    owner = kk + pr // 4 <= 4

    @pl.when(owner)
    def _():
        h = orb % 2
        m = kk // 2
        tile = kown[m]
        for o in range(1, 4):
            rcopy(s3.at[0], r3.at[o - 1], q3s.at[0], q3r.at[o - 1], zdev(o, c)).wait_recv()
            tile = tile + dec(r3[o - 1], 14 + o, h, pr, aux)
        out[...] = tile

        @pl.when(has_mirror)
        def _():
            turned = tile.T
            for h2 in range(2):
                s4[h2] = turned[h2 * TR:(h2 + 1) * TR]
                mir(h2).start()

    @pl.when(jnp.logical_not(owner))
    def _():
        for h2 in range(2):
            rcopy(s4.at[0], r4.at[h2], q4s.at[0], q4r.at[h2], (mirror[h2][1], mirror[h2][0])).wait_recv()
        out[...] = jnp.concatenate([r4[0], r4[1]], axis=1)

    for o in range(1, 8):
        krcopy(o).wait_send()

    @pl.loop(0, NCH)
    def _(q):
        relay(q).wait_send()
        for core in range(2):
            near(q, 1, core).wait_send()
            near(q, 3, core).wait_send()
            forward(q, core).wait_send()
        sibling(q).wait_send()
        fcopy(q).wait_send()

    for level, dev in ((0, ring1), (1, ring2), (2, zline)):
        for o in range(1, 4):
            rcopy(dv.at[4 * level], dv.at[4 * level], ds_.at[4 * level + o], dr.at[4 * level], dev(o)).wait_send()

    @pl.loop(0, 12)
    def _(j):
        u, m = j // 3, j % 3

        @pl.when(where(tf, u, m)[3])
        def _():
            far1(j, 0).wait_send()
            far1(j, 1).wait_send()

        for way, t in ((0, tp), (1, tm)):
            @pl.when(where(t, u, m)[3])
            def _():
                near1(j, way).wait_send()

    @pl.loop(0, 3)
    def _(m):
        @pl.when(where(me1, uf, m)[3])
        def _():
            far2(m, 0).wait_send()
            far2(m, 1).wait_send()

        for way, u in ((0, up), (1, um)):
            @pl.when(where(me1, u, m)[3])
            def _():
                near2(m, way).wait_send()

        _, _, q, ok = where(me1, me2, m)
        o = (z + 4 - q // 2) % 4

        @pl.when(jnp.logical_and(ok, o > 0))
        def _():
            last(m, o).wait_send()

    @pl.when(jnp.logical_and(owner, has_mirror))
    def _():
        for h2 in range(2):
            mir(h2).wait_send()


def shards(half, metric, survive):
    bf, f32, i16 = jnp.bfloat16, jnp.float32, jnp.int16
    rows = half.reshape(CH, half.shape[-1])
    mask = jnp.repeat(survive.reshape(-1).astype(bf), 128).reshape(1, -1)
    eye = jnp.eye(3, dtype=bf)
    kron = (metric[:, None, :, None] * eye[None, :, None, :]).reshape(48, CH)
    perm = jnp.asarray(perm_matrix(), bf)
    vm, dma = pltpu.VMEM, pltpu.SemaphoreType.DMA
    scratch = [
        vm((NCH, CH, CH), bf), vm((NCH, CH, CH), bf), vm((NCH, 96, CH), bf), vm((CH, CH), bf),
        vm((NCH, 2 * CH, CH), bf), vm((NCH, CH, 2 * CH), bf),
        vm((12, 8, CH), f32), vm((18, 8, CH), f32), vm((18, 8, CH), f32),
        vm((18, 2, 8, CH), f32), vm((18, 2, 8, CH), f32),
        vm((12, TR, CH), i16), vm((2, 12, TR, CH), i16), vm((2, 12, HR, CH), i16), vm((2, 12, TR, CH), i16),
        vm((3, TR, CH), f32),
        vm((3, TR, CH), i16), vm((2, 3, TR, CH), i16), vm((2, 3, HR, CH), i16), vm((2, 3, TR, CH), i16),
        vm((3, TR, CH), i16), vm((3, TR, CH), i16),
        vm((2, TR, TR), f32), vm((2, TR, TR), f32),
        dma((NCH, 6)), dma((NCH, 8)), dma((NCH,)), dma((NCH,)), dma((NCH, 2)),
        dma((8,)), dma((8,)), dma((NCH,)), dma((NCH,)), dma((12,)), dma((12,)),
        dma((12, 2)), dma((2, 12)), dma((2, 12)), dma((2, 12)),
        dma((3, 2)), dma((2, 3)), dma((2, 3)), dma((2, 3)),
        dma((3,)), dma((3,)), dma((2,)), dma((2,)),
    ]
    return pl.pallas_call(
        kernel,
        out_shape=jax.ShapeDtypeStruct((TR, CH), f32),
        in_specs=[pl.BlockSpec(memory_space=pltpu.VMEM)] * 4,
        out_specs=pl.BlockSpec(memory_space=pltpu.VMEM),
        scratch_shapes=scratch,
        compiler_params=pltpu.CompilerParams(collective_id=0, has_side_effects=True,
                                             vmem_limit_bytes=62 * 1024 * 1024),
    )(rows, mask, kron, perm)


def solution(mesh):
    placed = (P("aux", "orb", None), P("aux", None), P("aux", "orb", None))
    return jax.shard_map(shards, mesh=mesh, in_specs=placed, out_specs=P("orb", "aux"), check_vma=False)
```

```python
import jax
import jax.numpy as jnp
import numpy as np
from jax import lax
from jax.experimental import pallas as pl
from jax.experimental.pallas import tpu as pltpu
from jax.sharding import PartitionSpec as P

MESH = pl.DeviceIdType.MESH
CH = 384
NCH = 8
TR = 192
HR = 96
MR = 112
TOP = 32700.0
TINY = 1e-36


def perm_matrix():
    m = np.zeros((CH, CH), np.float32)
    for d in range(8):
        for aux in range(16):
            for i in range(3):
                m[d * 48 + aux * 3 + i, aux * 24 + 3 * d + i] = 1.0
    return m


def spread(metric):
    f32, bf = jnp.float32, jnp.bfloat16

    def third(n):
        return jnp.floor((n.astype(f32) + 0.5) * (1.0 / 3.0))

    def iota(shape, dim):
        return lax.broadcasted_iota(jnp.int32, shape, dim)

    left = (third(iota((48, 16), 0)) == iota((48, 16), 1).astype(f32)).astype(f32).astype(bf)
    right = (third(iota((128, CH), 1)) == iota((128, CH), 0).astype(f32)).astype(f32).astype(bf)
    rows = jnp.dot(left, metric, preferred_element_type=f32).astype(bf)
    wide = jnp.dot(rows, right, preferred_element_type=f32)
    a, b = iota((48, CH), 0), iota((48, CH), 1)
    same = (a.astype(f32) - 3.0 * third(a)) == (b.astype(f32) - 3.0 * third(b))
    return jnp.where(same, wide, 0.0).astype(bf)


def kernel(half, survive, metric, perm, out, block, kron, snd, rcv, rel, m3, fb, ft, dv, cs, csi, rb, rbi,
           s1f, s1n, r1f, r1n, kown, s2f, s2n, r2f, r2n, s3, r3, s4, r4,
           p1s, p1r, rls, rlr, fws, ks, kr, fs, fr, ds_, dr,
           q1fs, q1fr, q1ns, q1nr, q2fs, q2fr, q2ns, q2nr, q3s, q3r, q4s, q4r, lds):
    f32 = jnp.float32
    aux = lax.axis_index("aux")
    orb = lax.axis_index("orb")
    z, c = aux // 2, aux % 2
    x, y = orb // 4, orb % 4
    me1 = x * (1 - c) + y * c
    me2 = y * (1 - c) + x * c
    sib = 2 * z + 1 - c

    def row_of(t, u):
        return t * (4 - 3 * c) + u * (1 + 3 * c)

    def ring1(o):
        return (aux, row_of((me1 + o) % 4, me2))

    def ring2(o):
        return (aux, row_of(me1, (me2 + o) % 4))

    def zdev(o, core):
        return (2 * ((z + o) % 4) + core, orb)

    pr = orb // 2
    mirror = [(2 * aux + h, pr) for h in range(2)]
    has_mirror = aux != pr

    def cut(q):
        return pl.ds(pl.multiple_of(q * CH, 128), CH)

    def load(q):
        return pltpu.make_async_copy(half.at[:, cut(q)], block.at[q], lds.at[q])

    for q in range(NCH):
        load(q).start()

    bar = pltpu.get_barrier_semaphore()
    for o in range(1, 8):
        pl.semaphore_signal(bar, inc=1, device_id=((aux + o) % 8, orb), device_id_type=MESH)
    for o in range(1, 4):
        pl.semaphore_signal(bar, inc=1, device_id=ring1(o), device_id_type=MESH)
        pl.semaphore_signal(bar, inc=1, device_id=ring2(o), device_id_type=MESH)

    kron[...] = spread(metric[...])

    @pl.when(has_mirror)
    def _():
        for o, a in mirror:
            pl.semaphore_signal(bar, inc=1, device_id=(a, o), device_id_type=MESH)
        pl.semaphore_wait(bar, 15)

    @pl.when(jnp.logical_not(has_mirror))
    def _():
        pl.semaphore_wait(bar, 13)

    def rcopy(src, dst, ss, rs, dev):
        return pltpu.make_async_remote_copy(src_ref=src, dst_ref=dst, send_sem=ss, recv_sem=rs,
                                            device_id=dev, device_id_type=MESH)

    def al48(v):
        return pl.ds(pl.multiple_of(v * 48, 16), 48)

    def al96(v):
        return pl.ds(pl.multiple_of(v * 96, 16), 96)

    def krcopy(o):
        dst = m3.at[al48(aux)]
        return rcopy(kron, dst, ks.at[o], kr.at[o], ((aux + o) % 8, orb))

    for o in range(1, 8):
        krcopy(o).start()
    m3[al48(aux), :] = kron[...]

    step = 1 - 2 * c + 4
    zr = (z + step) % 4
    zf = (z + 4 - (step - 4)) % 4

    def near(q, o, core):
        dst_dev = zdev(o, core)
        rows = 2 * ((z + o) % 4) + core
        return rcopy(snd.at[q, al48(rows)], rcv.at[q, al48(aux)],
                     p1s.at[q, 2 * (o - 1) + core], p1r.at[q, aux], dst_dev)

    def sibling(q):
        return rcopy(snd.at[q, al48(sib)], rcv.at[q, al48(aux)], p1s.at[q, 2], p1r.at[q, aux], (sib, orb))

    def relay(q):
        return rcopy(snd.at[q, al96((z + 2) % 4)], rel.at[q], rls.at[q], rlr.at[q], (2 * zr + c, orb))

    def forward(q, core):
        src_aux = 2 * zf + c
        return rcopy(rel.at[q, pl.ds(48 * core, 48)], rcv.at[q, al48(src_aux)],
                     fws.at[q, core], p1r.at[q, src_aux], (2 * zr + core, orb))

    def arrival(q, a):
        return rcopy(rcv.at[q, al48(a)], rcv.at[q, al48(a)], p1s.at[q, 0], p1r.at[q, a], (sib, orb))

    def gate(q):
        flags = [jnp.full((1, 128), survive[0, 0, 3 * q + n].astype(f32)) for n in range(3)]
        return jnp.concatenate(flags, axis=1).astype(jnp.bfloat16)

    def nears(q):
        for core in range(2):
            near(q, 1, core).start()
            near(q, 3, core).start()

    @pl.loop(0, NCH)
    def _(q):
        load(q).wait()
        kept = block[q] * gate(q)
        snd[q] = jnp.dot(perm[...], kept, preferred_element_type=f32).astype(jnp.bfloat16)
        relay(q).start()
        sibling(q).start()
        rcv[q, al48(aux), :] = snd[q, al48(aux), :]

    nears(0)
    nears(1)

    def fcopy(q):
        return rcopy(fb.at[q, pl.ds(0, CH)], fb.at[q, pl.ds(CH, CH)], fs.at[q], fr.at[q], (sib, orb))

    for o in range(1, 8):
        src = (aux + 8 - o) % 8
        rcopy(kron, m3.at[al48(src)], ks.at[o], kr.at[o], (sib, orb)).wait_recv()

    @pl.loop(0, NCH)
    def _(q):
        relay(q).wait_recv()
        for core in range(2):
            forward(q, core).start()

        @pl.when(q < NCH - 2)
        def _():
            nears(q + 2)

    def pair(q):
        fcopy(q).wait_recv()
        both = fb[q]
        ft[q] = both.T
        wide = both.astype(f32)
        dv[0, pl.ds(q, 1), :] = jnp.sum(wide * wide, axis=0, keepdims=True)

    @pl.loop(0, NCH)
    def _(q):
        for o in range(1, 8):
            arrival(q, (aux + o) % 8).wait_recv()
        fb[q, 0:CH, :] = jnp.dot(m3[...], rcv[q], preferred_element_type=f32).astype(jnp.bfloat16)
        fcopy(q).start()

        @pl.when(q > 0)
        def _():
            pair(q - 1)

    pair(NCH - 1)

    def tables(first, terms):
        for n, val in enumerate(terms):
            val = jnp.maximum(val, TINY)
            lane = lax.broadcasted_iota(jnp.int32, val.shape, 1)
            inv = lax.rsqrt(val)
            csi[first + n] = inv
            cs[first + n] = val * inv
            for h in range(2):
                part = jnp.where((lane >= TR) == (h == 1), val, TINY)
                top = jnp.broadcast_to(jnp.max(part, axis=1, keepdims=True), val.shape)
                tinv = lax.rsqrt(top)
                rbi[first + n, h] = tinv * TOP
                rb[first + n, h] = top * tinv * (1.0 / TOP)

    def gather(level, dev):
        base = 4 * level
        for o in range(1, 4):
            rcopy(dv.at[base], dv.at[base + 4 - o], ds_.at[base + o], dr.at[base + 4 - o], dev(o)).start()

    def gathered(level, dev):
        base = 4 * level
        for o in range(1, 4):
            rcopy(dv.at[base], dv.at[base + o], ds_.at[base + o], dr.at[base + o], dev(o)).wait_recv()
        return [dv[base + o] for o in range(4)]

    def ring_terms(d):
        return [d[0], d[3], d[1], d[0] + d[3], d[0] + d[1], d[3] + d[2], d[1] + d[2]]

    def drain(level=9):
        for o in range(1, 8):
            krcopy(o).wait_send()

        @pl.loop(0, NCH)
        def _(q):
            relay(q).wait_send()
            for core in range(2):
                near(q, 1, core).wait_send()
                near(q, 3, core).wait_send()
                forward(q, core).wait_send()
            sibling(q).wait_send()
            fcopy(q).wait_send()

        if level < 2:
            return

        for lv, dev in ((0, ring1), (1, ring2), (2, zline))[:level if level > 1 else 0]:
            for o in range(1, 4):
                rcopy(dv.at[4 * lv], dv.at[4 * lv], ds_.at[4 * lv + o], dr.at[4 * lv], dev(o)).wait_send()
        if level < 2:
            return

        @pl.loop(0, 12)
        def _(j):
            u, m = j // 3, j % 3

            @pl.when(where(tf, u, m)[3])
            def _():
                far1(j, 0).wait_send()
                far1(j, 1).wait_send()

            for way, t in ((0, tp), (1, tm)):
                @pl.when(where(t, u, m)[3])
                def _():
                    near1(j, way).wait_send()
        if level < 3:
            return

        @pl.loop(0, 3)
        def _(m):
            @pl.when(where(me1, uf, m)[3])
            def _():
                far2(m, 0).wait_send()
                far2(m, 1).wait_send()

            for way, u in ((0, up), (1, um)):
                @pl.when(where(me1, u, m)[3])
                def _():
                    near2(m, way).wait_send()

            _, _, q, ok = where(me1, me2, m)
            o = (z + 4 - q // 2) % 4

            if level >= 4:
                @pl.when(jnp.logical_and(ok, o > 0))
                def _():
                    last(m, o).wait_send()
        if level < 5:
            return

        @pl.when(jnp.logical_and(owner, has_mirror))
        def _():
            for h2 in range(2):
                mir(h2).wait_send()

    gather(0, ring1)
    d0 = gathered(0, ring1)
    tables(0, ring_terms(d0))
    dv[4] = d0[0] + d0[1] + d0[2] + d0[3]
    gather(1, ring2)

    def enc(val, n, h, p, q):
        inv = csi[n, pl.ds(q, 1), :] * rbi[n, h, pl.ds(p, 1), :]
        return jnp.round(val * inv).astype(jnp.int32).astype(jnp.int16)

    def dec(val, n, h, p, q):
        sc = cs[n, pl.ds(q, 1), :] * rb[n, h, pl.ds(p, 1), :]
        return val.astype(jnp.int32).astype(f32) * sc

    def where(t, u, m):
        r = row_of(t, u)
        p = r // 2
        k = (p + c) % 2 + 2 * m
        return r % 2, p, (p + k) % 8, k + p // 4 <= 4

    def ktile(h, p, q):
        rows = ft[p, pl.ds(pl.multiple_of(h * TR, 64), TR), :]
        return jnp.dot(rows, fb[q], preferred_element_type=f32)

    tp, tm, tf = (me1 + 1) % 4, (me1 + 3) % 4, (me1 + 2) % 4

    def slot(j):
        ju = j // 3
        off = (2 + 3 * ju + 3 * (ju // 2) - 2 * (ju // 3)) % 4
        return (me2 + off) % 4, j % 3

    def far1(i, half_at):
        rows = pl.ds(half_at * HR, HR)
        dst = 0 if half_at == 0 else 1
        return rcopy(s1f.at[i, rows], r1f.at[dst, i], q1fs.at[i, half_at], q1fr.at[dst, i],
                     ring1(1 if half_at == 0 else 3))

    def near1(i, way):
        return rcopy(s1n.at[way, i], r1n.at[way, i], q1ns.at[way, i], q1nr.at[way, i],
                     ring1(1 if way == 0 else 3))

    @pl.loop(0, 12)
    def _(j):
        u, m = slot(j)
        h, p, q, ok = where(tf, u, m)
        i = u * 3 + m

        @pl.when(ok)
        def _():
            s1f[i] = enc(ktile(h, p, q), 0, h, p, q)
            far1(i, 0).start()
            far1(i, 1).start()

    @pl.loop(0, 12)
    def _(j):
        u, m = slot(j)
        i = u * 3 + m
        for way, t in ((0, tp), (1, tm)):
            h, p, q, ok = where(t, u, m)

            @pl.when(ok)
            def _():
                tile = ktile(h, p, q)
                far1(i, way).wait_recv()
                add = dec(r1f[way, i], 1 + way, h, p, q)
                low, high = tile[:HR], tile[HR:]
                if way == 0:
                    low = low + add
                else:
                    high = high + add
                s1n[way, i, 0:HR, :] = enc(low, 3 + way, h, p, q)
                s1n[way, i, HR:TR, :] = enc(high, 3 + way, h, p, q)
                near1(i, way).start()

    d1 = gathered(1, ring2)
    tables(7, ring_terms(d1))
    dv[8] = d1[0] + d1[1] + d1[2] + d1[3]

    def zline(o):
        return zdev(o, c)

    def own1(u, m, then):
        h, p, q, ok = where(me1, u, m)
        i = u * 3 + m

        @pl.when(ok)
        def _():
            tile = ktile(h, p, q)
            near1(i, 0).wait_recv()
            near1(i, 1).wait_recv()
            tile = tile + dec(r1n[0, i], 5, h, p, q) + dec(r1n[1, i], 6, h, p, q)
            then(tile, h, p, q)

    gather(2, zline)

    def far2(m, half_at):
        rows = pl.ds(half_at * HR, HR)
        dst = 0 if half_at == 0 else 1
        return rcopy(s2f.at[m, rows], r2f.at[dst, m], q2fs.at[m, half_at], q2fr.at[dst, m],
                     ring2(1 if half_at == 0 else 3))

    def near2(m, way):
        return rcopy(s2n.at[way, m], r2n.at[way, m], q2ns.at[way, m], q2nr.at[way, m],
                     ring2(1 if way == 0 else 3))

    uf, up, um = (me2 + 2) % 4, (me2 + 1) % 4, (me2 + 3) % 4

    @pl.loop(0, 3)
    def _(m):
        def then(tile, h, p, q):
            s2f[m] = enc(tile, 7, h, p, q)
            far2(m, 0).start()
            far2(m, 1).start()

        own1(uf, m, then)

    for way, u in ((0, up), (1, um)):
        @pl.loop(0, 3)
        def _(m):
            def then(tile, h, p, q):
                far2(m, way).wait_recv()
                add = dec(r2f[way, m], 8 + way, h, p, q)
                low, high = tile[:HR], tile[HR:]
                if way == 0:
                    low = low + add
                else:
                    high = high + add
                s2n[way, m, 0:HR, :] = enc(low, 10 + way, h, p, q)
                s2n[way, m, HR:TR, :] = enc(high, 10 + way, h, p, q)
                near2(m, way).start()

            own1(u, m, then)

    d2 = gathered(2, zline)
    tables(14, d2)

    def last(m, o):
        return rcopy(s3.at[m], r3.at[o - 1], q3s.at[m], q3r.at[o - 1], zdev(4 - o, c))

    @pl.loop(0, 3)
    def _(m):
        def then(tile, h, p, q):
            near2(m, 0).wait_recv()
            near2(m, 1).wait_recv()
            tile = tile + dec(r2n[0, m], 12, h, p, q) + dec(r2n[1, m], 13, h, p, q)
            kown[m] = tile
            o = (z + 4 - q // 2) % 4

            @pl.when(o > 0)
            def _():
                s3[m] = enc(tile, 14, h, p, q)
                last(m, o).start()

        own1(me2, m, then)

    def mir(h):
        return rcopy(s4.at[h], r4.at[orb % 2], q4s.at[h], q4r.at[orb % 2], (mirror[h][1], mirror[h][0]))

    kk = (aux + 8 - pr) % 8
    owner = kk + pr // 4 <= 4

    @pl.when(owner)
    def _():
        h = orb % 2
        m = kk // 2
        tile = kown[m]
        for o in range(1, 4):
            rcopy(s3.at[0], r3.at[o - 1], q3s.at[0], q3r.at[o - 1], zdev(o, c)).wait_recv()
            tile = tile + dec(r3[o - 1], 14 + o, h, pr, aux)
        out[...] = tile

        @pl.when(has_mirror)
        def _():
            turned = tile.T
            for h2 in range(2):
                part = turned[h2 * TR:(h2 + 1) * TR]
                flat = jnp.concatenate([part[:HR], part[HR:]], axis=1)
                top = jnp.max(jnp.abs(flat), axis=0, keepdims=True)
                power = jnp.ceil(jnp.log2(jnp.maximum(top, TINY)))
                s4[h2, 0:HR, :] = jnp.round(flat * (jnp.exp2(-power) * TOP)).astype(jnp.int32).astype(jnp.int16)
                s4[h2, HR:MR, :] = jnp.broadcast_to(power, (16, CH)).astype(jnp.int32).astype(jnp.int16)
                mir(h2).start()

    @pl.when(jnp.logical_not(owner))
    def _():
        for h2 in range(2):
            rcopy(s4.at[0], r4.at[h2], q4s.at[0], q4r.at[h2], (mirror[h2][1], mirror[h2][0])).wait_recv()
        parts = []
        for h2 in range(2):
            power = r4[h2, HR:MR, :].astype(jnp.int32).astype(f32)[0:1]
            parts.append(r4[h2, 0:HR, :].astype(jnp.int32).astype(f32) * (jnp.exp2(power) * (1.0 / TOP)))
        out[0:HR, :] = jnp.concatenate([parts[0][:, :TR], parts[1][:, :TR]], axis=1)
        out[HR:TR, :] = jnp.concatenate([parts[0][:, TR:], parts[1][:, TR:]], axis=1)

    drain()


def shards(half, metric, survive):
    bf, f32, i16 = jnp.bfloat16, jnp.float32, jnp.int16
    rows = half.reshape(CH, half.shape[-1])
    perm = jnp.asarray(perm_matrix(), bf)
    vm, dma = pltpu.VMEM, pltpu.SemaphoreType.DMA
    scratch = [
        vm((NCH, CH, CH), bf), vm((48, CH), bf),
        vm((NCH, CH, CH), bf), vm((NCH, CH, CH), bf), vm((NCH, 96, CH), bf), vm((CH, CH), bf),
        vm((NCH, 2 * CH, CH), bf), vm((NCH, CH, 2 * CH), bf),
        vm((12, 8, CH), f32), vm((18, 8, CH), f32), vm((18, 8, CH), f32),
        vm((18, 2, 8, CH), f32), vm((18, 2, 8, CH), f32),
        vm((12, TR, CH), i16), vm((2, 12, TR, CH), i16), vm((2, 12, HR, CH), i16), vm((2, 12, TR, CH), i16),
        vm((3, TR, CH), f32),
        vm((3, TR, CH), i16), vm((2, 3, TR, CH), i16), vm((2, 3, HR, CH), i16), vm((2, 3, TR, CH), i16),
        vm((3, TR, CH), i16), vm((3, TR, CH), i16),
        vm((2, MR, CH), i16), vm((2, MR, CH), i16),
        dma((NCH, 6)), dma((NCH, 8)), dma((NCH,)), dma((NCH,)), dma((NCH, 2)),
        dma((8,)), dma((8,)), dma((NCH,)), dma((NCH,)), dma((12,)), dma((12,)),
        dma((12, 2)), dma((2, 12)), dma((2, 12)), dma((2, 12)),
        dma((3, 2)), dma((2, 3)), dma((2, 3)), dma((2, 3)),
        dma((3,)), dma((3,)), dma((2,)), dma((2,)), dma((NCH,)),
    ]
    return pl.pallas_call(
        kernel,
        out_shape=jax.ShapeDtypeStruct((TR, CH), f32),
        in_specs=[pl.BlockSpec(memory_space=pl.ANY), pl.BlockSpec(memory_space=pltpu.SMEM),
                  pl.BlockSpec(memory_space=pltpu.VMEM), pl.BlockSpec(memory_space=pltpu.VMEM)],
        out_specs=pl.BlockSpec(memory_space=pltpu.VMEM),
        scratch_shapes=scratch,
        compiler_params=pltpu.CompilerParams(collective_id=0, has_side_effects=True,
                                             vmem_limit_bytes=62 * 1024 * 1024),
    )(rows, survive, metric, perm)


def solution(mesh):
    placed = (P("aux", "orb", None), P("aux", None), P("aux", "orb", None))
    return jax.shard_map(shards, mesh=mesh, in_specs=placed, out_specs=P("orb", "aux"), check_vma=False)
```

```python
import jax
import jax.numpy as jnp
import numpy as np
from jax import lax
from jax.experimental import pallas as pl
from jax.experimental.pallas import tpu as pltpu
from jax.sharding import PartitionSpec as P

MESH = pl.DeviceIdType.MESH
CH = 384
NCH = 8
TR = 192
HR = 96
MR = 112
TOP = 32700.0
TINY = 1e-36
ORDER = ((2, 0), (2, 1), (1, 0), (3, 0), (1, 1), (3, 1), (0, 1))


def perm_matrix():
    m = np.zeros((CH, CH), np.float32)
    for d in range(8):
        for aux in range(16):
            for i in range(3):
                m[d * 48 + aux * 3 + i, aux * 24 + 3 * d + i] = 1.0
    return m


def spread(metric):
    f32, bf = jnp.float32, jnp.bfloat16

    def third(n):
        return jnp.floor((n.astype(f32) + 0.5) * (1.0 / 3.0))

    def iota(shape, dim):
        return lax.broadcasted_iota(jnp.int32, shape, dim)

    left = (third(iota((48, 16), 0)) == iota((48, 16), 1).astype(f32)).astype(f32).astype(bf)
    right = (third(iota((128, CH), 1)) == iota((128, CH), 0).astype(f32)).astype(f32).astype(bf)
    rows = jnp.dot(left, metric, preferred_element_type=f32).astype(bf)
    wide = jnp.dot(rows, right, preferred_element_type=f32)
    a, b = iota((48, CH), 0), iota((48, CH), 1)
    same = (a.astype(f32) - 3.0 * third(a)) == (b.astype(f32) - 3.0 * third(b))
    return jnp.where(same, wide, 0.0).astype(bf)


def kernel(half, survive, metric, perm, out, block, kron, snd, rcv, m3, fb, ft, dvr, dv, cs, csi, rb, rbi,
           kbuf, s1f, s1n, r1f, r1n, s2f, s2n, r2f, r2n, s3, r3, s4, r4,
           lds, p1s, p1r, ks, kr, fs, fr, d1s, d1r, ds_, dr,
           q1fs, q1fr, q1ns, q1nr, q2fs, q2fr, q2ns, q2nr, q3s, q3r, q4s, q4r):
    f32 = jnp.float32
    aux = lax.axis_index("aux")
    orb = lax.axis_index("orb")
    z, c = aux // 2, aux % 2
    x, y = orb // 4, orb % 4
    me1 = x * (1 - c) + y * c
    me2 = y * (1 - c) + x * c
    sib = 2 * z + 1 - c

    def row_of(t, u):
        return t * (4 - 3 * c) + u * (1 + 3 * c)

    def ring1(o):
        return (aux, row_of((me1 + o) % 4, me2))

    def ring2(o):
        return (aux, row_of(me1, (me2 + o) % 4))

    def zdev(o, core):
        return (2 * ((z + o) % 4) + core, orb)

    pr = orb // 2
    mirror = [(2 * aux + h, pr) for h in range(2)]
    has_mirror = aux != pr

    def cut(q):
        return pl.ds(pl.multiple_of(q * CH, 128), CH)

    def load(q):
        return pltpu.make_async_copy(half.at[:, cut(q)], block.at[q], lds.at[q])

    for q in range(NCH):
        load(q).start()

    bar = pltpu.get_barrier_semaphore()
    for o in range(1, 8):
        pl.semaphore_signal(bar, inc=1, device_id=((aux + o) % 8, orb), device_id_type=MESH)
    for o in range(1, 4):
        pl.semaphore_signal(bar, inc=1, device_id=ring1(o), device_id_type=MESH)
        pl.semaphore_signal(bar, inc=1, device_id=ring2(o), device_id_type=MESH)

    kron[...] = spread(metric[...])

    @pl.when(has_mirror)
    def _():
        for o, a in mirror:
            pl.semaphore_signal(bar, inc=1, device_id=(a, o), device_id_type=MESH)

    def rcopy(src, dst, ss, rs, dev):
        return pltpu.make_async_remote_copy(src_ref=src, dst_ref=dst, send_sem=ss, recv_sem=rs,
                                            device_id=dev, device_id_type=MESH)

    def al48(v):
        return pl.ds(pl.multiple_of(v * 48, 16), 48)

    def krcopy(o):
        dst = m3.at[al48(aux)]
        return rcopy(kron, dst, ks.at[o], kr.at[o], ((aux + o) % 8, orb))

    def send(q, o, flip):
        dev = 2 * ((z + o) % 4) + (c + flip) % 2
        return rcopy(snd.at[q, al48(dev)], rcv.at[q, al48(aux)], p1s.at[q, 2 * o + flip], p1r.at[q, aux], (dev, orb))

    def arrival(q, a):
        return rcopy(rcv.at[q, al48(a)], rcv.at[q, al48(a)], p1s.at[q, 0], p1r.at[q, a], (sib, orb))

    def gate(q):
        flags = [jnp.full((1, 128), survive[0, 0, 3 * q + n].astype(f32)) for n in range(3)]
        return jnp.concatenate(flags, axis=1).astype(jnp.bfloat16)

    @pl.loop(0, NCH)
    def _(q):
        load(q).wait()
        kept = block[q] * gate(q)
        snd[q] = jnp.dot(perm[...], kept, preferred_element_type=f32).astype(jnp.bfloat16)
        rcv[q, al48(aux), :] = snd[q, al48(aux), :]

    @pl.when(has_mirror)
    def _():
        pl.semaphore_wait(bar, 15)

    @pl.when(jnp.logical_not(has_mirror))
    def _():
        pl.semaphore_wait(bar, 13)

    for o in range(1, 8):
        krcopy(o).start()
    m3[al48(aux), :] = kron[...]

    @pl.loop(0, NCH)
    def _(q):
        for o, flip in ORDER:
            send(q, o, flip).start()

    for o in range(1, 8):
        src = (aux + 8 - o) % 8
        rcopy(kron, m3.at[al48(src)], ks.at[o], kr.at[o], (sib, orb)).wait_recv()

    def fcopy(q):
        return rcopy(fb.at[q, pl.ds(0, CH)], fb.at[q, pl.ds(CH, CH)], fs.at[q], fr.at[q], (sib, orb))

    def table(n, val, at):
        val = jnp.maximum(val, TINY)
        lane = lax.broadcasted_iota(jnp.int32, val.shape, 1)
        inv = lax.rsqrt(val)
        csi[n, at, :] = inv
        cs[n, at, :] = val * inv
        for h in range(2):
            part = jnp.where((lane >= TR) == (h == 1), val, TINY)
            top = jnp.broadcast_to(jnp.max(part, axis=1, keepdims=True), val.shape)
            tinv = lax.rsqrt(top)
            rbi[n, h, at, :] = tinv * TOP
            rb[n, h, at, :] = top * tinv * (1.0 / TOP)

    def tables(first, terms):
        for n, val in enumerate(terms):
            table(first + n, val, slice(None))

    def gather(level, dev):
        base = 4 * level
        for o in range(1, 4):
            rcopy(dv.at[base], dv.at[base + 4 - o], ds_.at[base + o], dr.at[base + 4 - o], dev(o)).start()

    def gathered(level, dev):
        base = 4 * level
        for o in range(1, 4):
            rcopy(dv.at[base], dv.at[base + o], ds_.at[base + o], dr.at[base + o], dev(o)).wait_recv()
        return [dv[base + o] for o in range(4)]

    def ring_terms(d):
        return [d[0], d[3], d[1], d[0] + d[3], d[0] + d[1], d[3] + d[2], d[1] + d[2]]

    def dcopy(q, o):
        return rcopy(dvr.at[0, q], dvr.at[4 - o, q], d1s.at[o, q], d1r.at[4 - o, q], ring1(o))

    def enc(val, n, h, p, q):
        inv = csi[n, pl.ds(q, 1), :] * rbi[n, h, pl.ds(p, 1), :]
        return jnp.round(val * inv).astype(jnp.int32).astype(jnp.int16)

    def dec(val, n, h, p, q):
        sc = cs[n, pl.ds(q, 1), :] * rb[n, h, pl.ds(p, 1), :]
        return val.astype(jnp.int32).astype(f32) * sc

    def where(t, u, m):
        r = row_of(t, u)
        p = r // 2
        k = (p + c) % 2 + 2 * m
        return r % 2, p, (p + k) % 8, k + p // 4 <= 4

    tp, tm, tf = (me1 + 1) % 4, (me1 + 3) % 4, (me1 + 2) % 4

    def pair_of(k, j):
        g = (k - j) // 5
        return j + g * (k - j), k - g * (k - j)

    def place(p, q, h):
        a, b = p // 2, 2 * (p % 2) + h
        t, u = a * (1 - c) + b * c, b * (1 - c) + a * c
        return u * 3 + ((q - p + 8) % 8) // 2, (t - me1 + 4) % 4

    def each(k, body):
        @pl.loop(0, k + 1)
        def _(j):
            p, q = pair_of(k, j)

            @pl.when(q % 2 == c)
            def _():
                body(p, q)

    def far1(i, half_at):
        rows = pl.ds(half_at * HR, HR)
        dst = 0 if half_at == 0 else 1
        return rcopy(s1f.at[i, rows], r1f.at[dst, i], q1fs.at[i, half_at], q1fr.at[dst, i],
                     ring1(1 if half_at == 0 else 3))

    def near1(i, way, dev):
        return rcopy(s1n.at[way, i], r1n.at[way, i], q1ns.at[way, i], q1nr.at[way, i], dev)

    def pair(k):
        fcopy(k).wait_recv()
        both = fb[k]
        ft[k] = both.T
        wide = both.astype(f32)
        norm = jnp.sum(wide * wide, axis=0, keepdims=True)
        dvr[0, k] = norm
        for o in range(1, 4):
            dcopy(k, o).start()
        table(0, norm, pl.ds(k, 1))

    def compute(k):
        def body(p, q):
            tile = jnp.dot(ft[p], fb[q], preferred_element_type=f32)
            for h in range(2):
                i, role = place(p, q, h)
                part = tile[h * TR:(h + 1) * TR]

                @pl.when(role == 2)
                def _():
                    s1f[i] = enc(part, 0, h, p, q)
                    far1(i, 0).start()
                    far1(i, 1).start()

                @pl.when(role != 2)
                def _():
                    kbuf[(role + 1) // 2, i] = part

        each(k, body)

    def norms(k):
        for o in range(1, 4):
            rcopy(dvr.at[0, k], dvr.at[o, k], d1s.at[o, k], d1r.at[o, k], ring1(o)).wait_recv()
        d = [dvr[o, k] for o in range(4)]
        for n, val in enumerate(ring_terms(d)):
            if n:
                table(n, val, pl.ds(k, 1))
        dv[4, pl.ds(k, 1), :] = d[0] + d[1] + d[2] + d[3]

    def pass_on(k):
        def body(p, q):
            for h in range(2):
                i, role = place(p, q, h)

                @pl.when(role % 2 == 1)
                def _():
                    way = role // 2
                    pltpu.make_async_remote_copy(
                        src_ref=s1f.at[i, pl.ds(0, HR)], dst_ref=r1f.at[way, i], send_sem=q1fs.at[i, 0],
                        recv_sem=q1fr.at[way, i], device_id=ring1(1), device_id_type=MESH).wait_recv()
                    rows = pl.ds(pl.multiple_of(way * HR, 32), HR)
                    kbuf[1 + way, i, rows, :] = kbuf[1 + way, i, rows, :] + dec(r1f[way, i], 1 + way, h, p, q)
                    s1n[way, i] = enc(kbuf[1 + way, i], 3 + way, h, p, q)
                    near1(i, way, ring1(role)).start()

        each(k, body)

    def collect(k):
        def body(p, q):
            for h in range(2):
                i, role = place(p, q, h)

                @pl.when(role == 0)
                def _():
                    near1(i, 0, ring1(1)).wait_recv()
                    near1(i, 1, ring1(1)).wait_recv()
                    kbuf[0, i] = kbuf[0, i] + dec(r1n[0, i], 5, h, p, q) + dec(r1n[1, i], 6, h, p, q)

        each(k, body)

    @pl.loop(0, NCH)
    def _(k):
        for o in range(1, 8):
            arrival(k, (aux + o) % 8).wait_recv()
        fb[k, 0:CH, :] = jnp.dot(m3[...], rcv[k], preferred_element_type=f32).astype(jnp.bfloat16)
        fcopy(k).start()

        @pl.when(k > 0)
        def _():
            norms(k - 1)
            pass_on(k - 1)

        @pl.when(k > 1)
        def _():
            collect(k - 2)

        pair(k)
        compute(k)

    norms(NCH - 1)
    gather(1, ring2)
    pass_on(NCH - 1)
    collect(NCH - 2)
    d1 = gathered(1, ring2)
    tables(7, ring_terms(d1))
    dv[8] = d1[0] + d1[1] + d1[2] + d1[3]

    def zline(o):
        return zdev(o, c)

    gather(2, zline)
    collect(NCH - 1)

    def own1(u, m, then):
        h, p, q, ok = where(me1, u, m)

        @pl.when(ok)
        def _():
            then(kbuf[0, u * 3 + m], h, p, q)

    def far2(m, half_at):
        rows = pl.ds(half_at * HR, HR)
        dst = 0 if half_at == 0 else 1
        return rcopy(s2f.at[m, rows], r2f.at[dst, m], q2fs.at[m, half_at], q2fr.at[dst, m],
                     ring2(1 if half_at == 0 else 3))

    def near2(m, way):
        return rcopy(s2n.at[way, m], r2n.at[way, m], q2ns.at[way, m], q2nr.at[way, m],
                     ring2(1 if way == 0 else 3))

    uf, up, um = (me2 + 2) % 4, (me2 + 1) % 4, (me2 + 3) % 4

    @pl.loop(0, 3)
    def _(m):
        def then(tile, h, p, q):
            s2f[m] = enc(tile, 7, h, p, q)
            far2(m, 0).start()
            far2(m, 1).start()

        own1(uf, m, then)

    for way, u in ((0, up), (1, um)):
        @pl.loop(0, 3)
        def _(m):
            def then(tile, h, p, q):
                far2(m, way).wait_recv()
                add = dec(r2f[way, m], 8 + way, h, p, q)
                low, high = tile[:HR], tile[HR:]
                if way == 0:
                    low = low + add
                else:
                    high = high + add
                s2n[way, m, 0:HR, :] = enc(low, 10 + way, h, p, q)
                s2n[way, m, HR:TR, :] = enc(high, 10 + way, h, p, q)
                near2(m, way).start()

            own1(u, m, then)

    d2 = gathered(2, zline)
    tables(14, d2)

    def last(m, o):
        return rcopy(s3.at[m], r3.at[o - 1], q3s.at[m], q3r.at[o - 1], zdev(4 - o, c))

    @pl.loop(0, 3)
    def _(m):
        def then(tile, h, p, q):
            near2(m, 0).wait_recv()
            near2(m, 1).wait_recv()
            tile = tile + dec(r2n[0, m], 12, h, p, q) + dec(r2n[1, m], 13, h, p, q)
            kbuf[0, me2 * 3 + m] = tile
            o = (z + 4 - q // 2) % 4

            @pl.when(o > 0)
            def _():
                s3[m] = enc(tile, 14, h, p, q)
                last(m, o).start()

        own1(me2, m, then)

    def mir(h):
        return rcopy(s4.at[h], r4.at[orb % 2], q4s.at[h], q4r.at[orb % 2], (mirror[h][1], mirror[h][0]))

    kk = (aux + 8 - pr) % 8
    owner = kk + pr // 4 <= 4

    @pl.when(owner)
    def _():
        h = orb % 2
        m = kk // 2
        tile = kbuf[0, me2 * 3 + m]
        for o in range(1, 4):
            rcopy(s3.at[0], r3.at[o - 1], q3s.at[0], q3r.at[o - 1], zdev(o, c)).wait_recv()
            tile = tile + dec(r3[o - 1], 14 + o, h, pr, aux)
        out[...] = tile

        @pl.when(has_mirror)
        def _():
            turned = tile.T
            for h2 in range(2):
                part = turned[h2 * TR:(h2 + 1) * TR]
                flat = jnp.concatenate([part[:HR], part[HR:]], axis=1)
                top = jnp.max(jnp.abs(flat), axis=0, keepdims=True)
                power = jnp.ceil(jnp.log2(jnp.maximum(top, TINY)))
                s4[h2, 0:HR, :] = jnp.round(flat * (jnp.exp2(-power) * TOP)).astype(jnp.int32).astype(jnp.int16)
                s4[h2, HR:MR, :] = jnp.broadcast_to(power, (16, CH)).astype(jnp.int32).astype(jnp.int16)
                mir(h2).start()

    @pl.when(jnp.logical_not(owner))
    def _():
        for h2 in range(2):
            rcopy(s4.at[0], r4.at[h2], q4s.at[0], q4r.at[h2], (mirror[h2][1], mirror[h2][0])).wait_recv()
        parts = []
        for h2 in range(2):
            power = r4[h2, HR:MR, :].astype(jnp.int32).astype(f32)[0:1]
            parts.append(r4[h2, 0:HR, :].astype(jnp.int32).astype(f32) * (jnp.exp2(power) * (1.0 / TOP)))
        out[0:HR, :] = jnp.concatenate([parts[0][:, :TR], parts[1][:, :TR]], axis=1)
        out[HR:TR, :] = jnp.concatenate([parts[0][:, TR:], parts[1][:, TR:]], axis=1)

    for o in range(1, 8):
        krcopy(o).wait_send()

    @pl.loop(0, NCH)
    def _(q):
        for o, flip in ORDER:
            send(q, o, flip).wait_send()
        fcopy(q).wait_send()
        for o in range(1, 4):
            dcopy(q, o).wait_send()

    for level, dev in ((1, ring2), (2, zline)):
        for o in range(1, 4):
            rcopy(dv.at[4 * level], dv.at[4 * level], ds_.at[4 * level + o], dr.at[4 * level], dev(o)).wait_send()

    @pl.loop(0, 12)
    def _(j):
        u, m = j // 3, j % 3

        @pl.when(where(tf, u, m)[3])
        def _():
            far1(j, 0).wait_send()
            far1(j, 1).wait_send()

        for way, t in ((0, tp), (1, tm)):
            @pl.when(where(t, u, m)[3])
            def _():
                near1(j, way, ring1(1)).wait_send()

    @pl.loop(0, 3)
    def _(m):
        @pl.when(where(me1, uf, m)[3])
        def _():
            far2(m, 0).wait_send()
            far2(m, 1).wait_send()

        for way, u in ((0, up), (1, um)):
            @pl.when(where(me1, u, m)[3])
            def _():
                near2(m, way).wait_send()

        _, _, q, ok = where(me1, me2, m)
        o = (z + 4 - q // 2) % 4

        @pl.when(jnp.logical_and(ok, o > 0))
        def _():
            last(m, o).wait_send()

    @pl.when(jnp.logical_and(owner, has_mirror))
    def _():
        for h2 in range(2):
            mir(h2).wait_send()


def shards(half, metric, survive):
    bf, f32, i16 = jnp.bfloat16, jnp.float32, jnp.int16
    rows = half.reshape(CH, half.shape[-1])
    perm = jnp.asarray(perm_matrix(), bf)
    vm, dma = pltpu.VMEM, pltpu.SemaphoreType.DMA
    scratch = [
        vm((NCH, CH, CH), bf), vm((48, CH), bf),
        vm((NCH, CH, CH), bf), vm((NCH, CH, CH), bf), vm((CH, CH), bf),
        vm((NCH, 2 * CH, CH), bf), vm((NCH, CH, 2 * CH), bf),
        vm((4, NCH, 1, CH), f32), vm((12, 8, CH), f32), vm((18, 8, CH), f32), vm((18, 8, CH), f32),
        vm((18, 2, 8, CH), f32), vm((18, 2, 8, CH), f32),
        vm((3, 12, TR, CH), f32),
        vm((12, TR, CH), i16), vm((2, 12, TR, CH), i16), vm((2, 12, HR, CH), i16), vm((2, 12, TR, CH), i16),
        vm((3, TR, CH), i16), vm((2, 3, TR, CH), i16), vm((2, 3, HR, CH), i16), vm((2, 3, TR, CH), i16),
        vm((3, TR, CH), i16), vm((3, TR, CH), i16),
        vm((2, MR, CH), i16), vm((2, MR, CH), i16),
        dma((NCH,)), dma((NCH, 8)), dma((NCH, 8)), dma((8,)), dma((8,)), dma((NCH,)), dma((NCH,)),
        dma((4, NCH)), dma((4, NCH)), dma((12,)), dma((12,)),
        dma((12, 2)), dma((2, 12)), dma((2, 12)), dma((2, 12)),
        dma((3, 2)), dma((2, 3)), dma((2, 3)), dma((2, 3)),
        dma((3,)), dma((3,)), dma((2,)), dma((2,)),
    ]
    return pl.pallas_call(
        kernel,
        out_shape=jax.ShapeDtypeStruct((TR, CH), f32),
        in_specs=[pl.BlockSpec(memory_space=pl.ANY), pl.BlockSpec(memory_space=pltpu.SMEM),
                  pl.BlockSpec(memory_space=pltpu.VMEM), pl.BlockSpec(memory_space=pltpu.VMEM)],
        out_specs=pl.BlockSpec(memory_space=pltpu.VMEM),
        scratch_shapes=scratch,
        compiler_params=pltpu.CompilerParams(collective_id=0, has_side_effects=True,
                                             vmem_limit_bytes=62 * 1024 * 1024),
    )(rows, survive, metric, perm)


def solution(mesh):
    placed = (P("aux", "orb", None), P("aux", None), P("aux", "orb", None))
    return jax.shard_map(shards, mesh=mesh, in_specs=placed, out_specs=P("orb", "aux"), check_vma=False)
```

```python
import jax
import jax.numpy as jnp
import numpy as np
from jax import lax
from jax.experimental import pallas as pl
from jax.experimental.pallas import tpu as pltpu
from jax.sharding import PartitionSpec as P

MESH = pl.DeviceIdType.MESH
CH = 384
NCH = 8
TR = 192
HR = 96
MR = 112
TOP = 32700.0
TINY = 1e-36
ORDER = ((2, 0), (2, 1), (1, 0), (3, 0), (1, 1), (3, 1), (0, 1))


def perm_matrix():
    m = np.zeros((CH, CH), np.float32)
    for d in range(8):
        for aux in range(16):
            for i in range(3):
                m[d * 48 + aux * 3 + i, aux * 24 + 3 * d + i] = 1.0
    return m


def spread(metric):
    f32, bf = jnp.float32, jnp.bfloat16

    def third(n):
        return jnp.floor((n.astype(f32) + 0.5) * (1.0 / 3.0))

    def iota(shape, dim):
        return lax.broadcasted_iota(jnp.int32, shape, dim)

    left = (third(iota((48, 16), 0)) == iota((48, 16), 1).astype(f32)).astype(f32).astype(bf)
    right = (third(iota((128, CH), 1)) == iota((128, CH), 0).astype(f32)).astype(f32).astype(bf)
    rows = jnp.dot(left, metric, preferred_element_type=f32).astype(bf)
    wide = jnp.dot(rows, right, preferred_element_type=f32)
    a, b = iota((48, CH), 0), iota((48, CH), 1)
    same = (a.astype(f32) - 3.0 * third(a)) == (b.astype(f32) - 3.0 * third(b))
    return jnp.where(same, wide, 0.0).astype(bf)


def kernel(half, survive, metric, perm, out, block, kron, snd, rcv, m3, fb, ft, dvr, dv, cs1, csi1, rb1, rbi1, cs, csi, rb, rbi,
           kbuf, s1f, s1n, r1f, r1n, s2f, s2n, r2f, r2n, s3, r3, s4, r4,
           lds, p1s, p1r, ks, kr, fs, fr, d1s, d1r, ds_, dr,
           q1fs, q1fr, q1ns, q1nr, q2fs, q2fr, q2ns, q2nr, q3s, q3r, q4s, q4r):
    f32 = jnp.float32
    aux = lax.axis_index("aux")
    orb = lax.axis_index("orb")
    z, c = aux // 2, aux % 2
    x, y = orb // 4, orb % 4
    me1 = x * (1 - c) + y * c
    me2 = y * (1 - c) + x * c
    sib = 2 * z + 1 - c

    def row_of(t, u):
        return t * (4 - 3 * c) + u * (1 + 3 * c)

    def ring1(o):
        return (aux, row_of((me1 + o) % 4, me2))

    def ring2(o):
        return (aux, row_of(me1, (me2 + o) % 4))

    def zdev(o, core):
        return (2 * ((z + o) % 4) + core, orb)

    pr = orb // 2
    mirror = [(2 * aux + h, pr) for h in range(2)]
    has_mirror = aux != pr

    def cut(q):
        return pl.ds(pl.multiple_of(q * CH, 128), CH)

    def load(q):
        return pltpu.make_async_copy(half.at[:, cut(q)], block.at[q], lds.at[q])

    for q in range(NCH):
        load(q).start()

    bar = pltpu.get_barrier_semaphore()
    for o in range(1, 8):
        pl.semaphore_signal(bar, inc=1, device_id=((aux + o) % 8, orb), device_id_type=MESH)
    for o in range(1, 4):
        pl.semaphore_signal(bar, inc=1, device_id=ring1(o), device_id_type=MESH)
        pl.semaphore_signal(bar, inc=1, device_id=ring2(o), device_id_type=MESH)

    kron[...] = spread(metric[...])

    @pl.when(has_mirror)
    def _():
        for o, a in mirror:
            pl.semaphore_signal(bar, inc=1, device_id=(a, o), device_id_type=MESH)

    def rcopy(src, dst, ss, rs, dev):
        return pltpu.make_async_remote_copy(src_ref=src, dst_ref=dst, send_sem=ss, recv_sem=rs,
                                            device_id=dev, device_id_type=MESH)

    def al48(v):
        return pl.ds(pl.multiple_of(v * 48, 16), 48)

    def krcopy(o):
        dst = m3.at[al48(aux)]
        return rcopy(kron, dst, ks.at[o], kr.at[o], ((aux + o) % 8, orb))

    def send(q, o, flip):
        dev = 2 * ((z + o) % 4) + (c + flip) % 2
        return rcopy(snd.at[q, al48(dev)], rcv.at[q, al48(aux)], p1s.at[q, 2 * o + flip], p1r.at[q, aux], (dev, orb))

    def arrival(q, a):
        return rcopy(rcv.at[q, al48(a)], rcv.at[q, al48(a)], p1s.at[q, 0], p1r.at[q, a], (sib, orb))

    def gate(q):
        flags = [jnp.full((1, 128), survive[0, 0, 3 * q + n].astype(f32)) for n in range(3)]
        return jnp.concatenate(flags, axis=1).astype(jnp.bfloat16)

    @pl.loop(0, NCH)
    def _(q):
        load(q).wait()
        kept = block[q] * gate(q)
        snd[q] = jnp.dot(perm[...], kept, preferred_element_type=f32).astype(jnp.bfloat16)
        rcv[q, al48(aux), :] = snd[q, al48(aux), :]

    @pl.when(has_mirror)
    def _():
        pl.semaphore_wait(bar, 15)

    @pl.when(jnp.logical_not(has_mirror))
    def _():
        pl.semaphore_wait(bar, 13)

    for o in range(1, 8):
        krcopy(o).start()
    m3[al48(aux), :] = kron[...]

    @pl.loop(0, NCH)
    def _(q):
        for o, flip in ORDER:
            send(q, o, flip).start()

    for o in range(1, 8):
        src = (aux + 8 - o) % 8
        rcopy(kron, m3.at[al48(src)], ks.at[o], kr.at[o], (sib, orb)).wait_recv()

    def fcopy(q):
        return rcopy(fb.at[q, pl.ds(0, CH)], fb.at[q, pl.ds(CH, CH)], fs.at[q], fr.at[q], (sib, orb))

    def scales(val):
        val = jnp.maximum(val, TINY)
        lane = lax.broadcasted_iota(jnp.int32, val.shape, 1)
        inv = lax.rsqrt(val)
        yield val * inv, inv
        for h in range(2):
            part = jnp.where((lane >= TR) == (h == 1), val, TINY)
            top = jnp.broadcast_to(jnp.max(part, axis=1, keepdims=True), val.shape)
            tinv = lax.rsqrt(top)
            yield top * tinv * (1.0 / TOP), tinv * TOP

    def tables1(k, rows, val):
        for n, (sc, inv) in enumerate(scales(val)):
            if n == 0:
                cs1[k, rows, :], csi1[k, rows, :] = sc, inv
            else:
                rb1[n - 1, k, rows, :], rbi1[n - 1, k, rows, :] = sc, inv

    def tables(first, terms):
        for i, val in enumerate(terms):
            for n, (sc, inv) in enumerate(scales(val)):
                if n == 0:
                    cs[first + i], csi[first + i] = sc, inv
                else:
                    rb[first + i, n - 1], rbi[first + i, n - 1] = sc, inv

    def gather(level, dev):
        base = 4 * level
        for o in range(1, 4):
            rcopy(dv.at[base], dv.at[base + 4 - o], ds_.at[base + o], dr.at[base + 4 - o], dev(o)).start()

    def gathered(level, dev):
        base = 4 * level
        for o in range(1, 4):
            rcopy(dv.at[base], dv.at[base + o], ds_.at[base + o], dr.at[base + o], dev(o)).wait_recv()
        return [dv[base + o] for o in range(4)]

    def ring_terms(d):
        return [d[0], d[3], d[1], d[0] + d[3], d[0] + d[1], d[3] + d[2], d[1] + d[2]]

    def dcopy(q, o):
        return rcopy(dvr.at[0, q], dvr.at[4 - o, q], d1s.at[o, q], d1r.at[4 - o, q], ring1(o))

    def enc1(val, n, h, p, q):
        inv = csi1[q, pl.ds(n, 1), :] * rbi1[h, p, pl.ds(n, 1), :]
        return jnp.round(val * inv).astype(jnp.int32).astype(jnp.int16)

    def dec1(val, n, h, p, q):
        sc = cs1[q, pl.ds(n, 1), :] * rb1[h, p, pl.ds(n, 1), :]
        return val.astype(jnp.int32).astype(f32) * sc

    def enc(val, n, h, p, q):
        inv = csi[n, pl.ds(q, 1), :] * rbi[n, h, pl.ds(p, 1), :]
        return jnp.round(val * inv).astype(jnp.int32).astype(jnp.int16)

    def dec(val, n, h, p, q):
        sc = cs[n, pl.ds(q, 1), :] * rb[n, h, pl.ds(p, 1), :]
        return val.astype(jnp.int32).astype(f32) * sc

    def where(t, u, m):
        r = row_of(t, u)
        p = r // 2
        k = (p + c) % 2 + 2 * m
        return r % 2, p, (p + k) % 8, k + p // 4 <= 4

    tp, tm, tf = (me1 + 1) % 4, (me1 + 3) % 4, (me1 + 2) % 4

    def pair_of(k, j):
        g = (k - j) // 5
        return j + g * (k - j), k - g * (k - j)

    def place(p, q, h):
        a, b = p // 2, 2 * (p % 2) + h
        t, u = a * (1 - c) + b * c, b * (1 - c) + a * c
        return u * 3 + ((q - p + 8) % 8) // 2, (t - me1 + 4) % 4

    def each(k, body):
        @pl.loop(0, k + 1)
        def _(j):
            p, q = pair_of(k, j)

            @pl.when(q % 2 == c)
            def _():
                body(p, q)

    def far1(i, half_at):
        rows = pl.ds(half_at * HR, HR)
        dst = 0 if half_at == 0 else 1
        return rcopy(s1f.at[i, rows], r1f.at[dst, i], q1fs.at[i, half_at], q1fr.at[dst, i],
                     ring1(1 if half_at == 0 else 3))

    def near1(i, way, dev):
        return rcopy(s1n.at[way, i], r1n.at[way, i], q1ns.at[way, i], q1nr.at[way, i], dev)

    def pair(k):
        fcopy(k).wait_recv()
        both = fb[k]
        ft[k] = both.T
        wide = both.astype(f32)
        norm = jnp.sum(wide * wide, axis=0, keepdims=True)
        dvr[0, k] = norm
        for o in range(1, 4):
            dcopy(k, o).start()
        tables1(k, pl.ds(0, 1), norm)

    def compute(k):
        def body(p, q):
            tile = jnp.dot(ft[p], fb[q], preferred_element_type=f32)
            for h in range(2):
                i, role = place(p, q, h)
                part = tile[h * TR:(h + 1) * TR]

                @pl.when(role == 2)
                def _():
                    s1f[i] = enc1(part, 0, h, p, q)
                    far1(i, 0).start()
                    far1(i, 1).start()

                @pl.when(role != 2)
                def _():
                    kbuf[(role + 1) // 2, i] = part

        each(k, body)

    def norms(k):
        for o in range(1, 4):
            rcopy(dvr.at[0, k], dvr.at[o, k], d1s.at[o, k], d1r.at[o, k], ring1(o)).wait_recv()
        d = [dvr[o, k] for o in range(4)]
        whole = d[0] + d[1] + d[2] + d[3]
        tables1(k, slice(None), jnp.concatenate(ring_terms(d) + [whole], axis=0))
        dv[4, pl.ds(k, 1), :] = whole

    def pass_on(k):
        def body(p, q):
            for h in range(2):
                i, role = place(p, q, h)

                @pl.when(role % 2 == 1)
                def _():
                    way = role // 2
                    pltpu.make_async_remote_copy(
                        src_ref=s1f.at[i, pl.ds(0, HR)], dst_ref=r1f.at[way, i], send_sem=q1fs.at[i, 0],
                        recv_sem=q1fr.at[way, i], device_id=ring1(1), device_id_type=MESH).wait_recv()
                    rows = pl.ds(pl.multiple_of(way * HR, 32), HR)
                    kbuf[1 + way, i, rows, :] = kbuf[1 + way, i, rows, :] + dec1(r1f[way, i], 1 + way, h, p, q)
                    s1n[way, i] = enc1(kbuf[1 + way, i], 3 + way, h, p, q)
                    near1(i, way, ring1(role)).start()

        each(k, body)

    def collect(k):
        def body(p, q):
            for h in range(2):
                i, role = place(p, q, h)

                @pl.when(role == 0)
                def _():
                    near1(i, 0, ring1(1)).wait_recv()
                    near1(i, 1, ring1(1)).wait_recv()
                    kbuf[0, i] = kbuf[0, i] + dec1(r1n[0, i], 5, h, p, q) + dec1(r1n[1, i], 6, h, p, q)

        each(k, body)

    @pl.loop(0, NCH)
    def _(k):
        for o in range(1, 8):
            arrival(k, (aux + o) % 8).wait_recv()
        fb[k, 0:CH, :] = jnp.dot(m3[...], rcv[k], preferred_element_type=f32).astype(jnp.bfloat16)
        fcopy(k).start()

        @pl.when(k > 1)
        def _():
            norms(k - 2)
            pass_on(k - 2)

        @pl.when(k > 2)
        def _():
            collect(k - 3)

        pair(k)
        compute(k)

    norms(NCH - 2)
    norms(NCH - 1)
    gather(1, ring2)
    pass_on(NCH - 2)
    collect(NCH - 3)
    pass_on(NCH - 1)
    collect(NCH - 2)
    d1 = gathered(1, ring2)
    tables(0, ring_terms(d1))
    dv[8] = d1[0] + d1[1] + d1[2] + d1[3]

    def zline(o):
        return zdev(o, c)

    gather(2, zline)
    collect(NCH - 1)

    def own1(u, m, then):
        h, p, q, ok = where(me1, u, m)

        @pl.when(ok)
        def _():
            then(kbuf[0, u * 3 + m], h, p, q)

    def far2(m, half_at):
        rows = pl.ds(half_at * HR, HR)
        dst = 0 if half_at == 0 else 1
        return rcopy(s2f.at[m, rows], r2f.at[dst, m], q2fs.at[m, half_at], q2fr.at[dst, m],
                     ring2(1 if half_at == 0 else 3))

    def near2(m, way):
        return rcopy(s2n.at[way, m], r2n.at[way, m], q2ns.at[way, m], q2nr.at[way, m],
                     ring2(1 if way == 0 else 3))

    uf, up, um = (me2 + 2) % 4, (me2 + 1) % 4, (me2 + 3) % 4

    @pl.loop(0, 3)
    def _(m):
        def then(tile, h, p, q):
            s2f[m] = enc(tile, 0, h, p, q)
            far2(m, 0).start()
            far2(m, 1).start()

        own1(uf, m, then)

    for way, u in ((0, up), (1, um)):
        @pl.loop(0, 3)
        def _(m):
            def then(tile, h, p, q):
                far2(m, way).wait_recv()
                add = dec(r2f[way, m], 1 + way, h, p, q)
                low, high = tile[:HR], tile[HR:]
                if way == 0:
                    low = low + add
                else:
                    high = high + add
                s2n[way, m, 0:HR, :] = enc(low, 3 + way, h, p, q)
                s2n[way, m, HR:TR, :] = enc(high, 3 + way, h, p, q)
                near2(m, way).start()

            own1(u, m, then)

    d2 = gathered(2, zline)
    tables(7, d2)

    def last(m, o):
        return rcopy(s3.at[m], r3.at[o - 1], q3s.at[m], q3r.at[o - 1], zdev(4 - o, c))

    @pl.loop(0, 3)
    def _(m):
        def then(tile, h, p, q):
            near2(m, 0).wait_recv()
            near2(m, 1).wait_recv()
            tile = tile + dec(r2n[0, m], 5, h, p, q) + dec(r2n[1, m], 6, h, p, q)
            kbuf[0, me2 * 3 + m] = tile
            o = (z + 4 - q // 2) % 4

            @pl.when(o > 0)
            def _():
                s3[m] = enc(tile, 7, h, p, q)
                last(m, o).start()

        own1(me2, m, then)

    def mir(h):
        return rcopy(s4.at[h], r4.at[orb % 2], q4s.at[h], q4r.at[orb % 2], (mirror[h][1], mirror[h][0]))

    kk = (aux + 8 - pr) % 8
    owner = kk + pr // 4 <= 4

    @pl.when(owner)
    def _():
        h = orb % 2
        m = kk // 2
        tile = kbuf[0, me2 * 3 + m]
        for o in range(1, 4):
            rcopy(s3.at[0], r3.at[o - 1], q3s.at[0], q3r.at[o - 1], zdev(o, c)).wait_recv()
            tile = tile + dec(r3[o - 1], 7 + o, h, pr, aux)
        out[...] = tile

        @pl.when(has_mirror)
        def _():
            turned = tile.T
            for h2 in range(2):
                part = turned[h2 * TR:(h2 + 1) * TR]
                flat = jnp.concatenate([part[:HR], part[HR:]], axis=1)
                top = jnp.max(jnp.abs(flat), axis=0, keepdims=True)
                power = jnp.ceil(jnp.log2(jnp.maximum(top, TINY)))
                s4[h2, 0:HR, :] = jnp.round(flat * (jnp.exp2(-power) * TOP)).astype(jnp.int32).astype(jnp.int16)
                s4[h2, HR:MR, :] = jnp.broadcast_to(power, (16, CH)).astype(jnp.int32).astype(jnp.int16)
                mir(h2).start()

    @pl.when(jnp.logical_not(owner))
    def _():
        for h2 in range(2):
            rcopy(s4.at[0], r4.at[h2], q4s.at[0], q4r.at[h2], (mirror[h2][1], mirror[h2][0])).wait_recv()
        parts = []
        for h2 in range(2):
            power = r4[h2, HR:MR, :].astype(jnp.int32).astype(f32)[0:1]
            parts.append(r4[h2, 0:HR, :].astype(jnp.int32).astype(f32) * (jnp.exp2(power) * (1.0 / TOP)))
        out[0:HR, :] = jnp.concatenate([parts[0][:, :TR], parts[1][:, :TR]], axis=1)
        out[HR:TR, :] = jnp.concatenate([parts[0][:, TR:], parts[1][:, TR:]], axis=1)

    for o in range(1, 8):
        krcopy(o).wait_send()

    @pl.loop(0, NCH)
    def _(q):
        for o, flip in ORDER:
            send(q, o, flip).wait_send()
        fcopy(q).wait_send()
        for o in range(1, 4):
            dcopy(q, o).wait_send()

    for level, dev in ((1, ring2), (2, zline)):
        for o in range(1, 4):
            rcopy(dv.at[4 * level], dv.at[4 * level], ds_.at[4 * level + o], dr.at[4 * level], dev(o)).wait_send()

    @pl.loop(0, 12)
    def _(j):
        u, m = j // 3, j % 3

        @pl.when(where(tf, u, m)[3])
        def _():
            far1(j, 0).wait_send()
            far1(j, 1).wait_send()

        for way, t in ((0, tp), (1, tm)):
            @pl.when(where(t, u, m)[3])
            def _():
                near1(j, way, ring1(1)).wait_send()

    @pl.loop(0, 3)
    def _(m):
        @pl.when(where(me1, uf, m)[3])
        def _():
            far2(m, 0).wait_send()
            far2(m, 1).wait_send()

        for way, u in ((0, up), (1, um)):
            @pl.when(where(me1, u, m)[3])
            def _():
                near2(m, way).wait_send()

        _, _, q, ok = where(me1, me2, m)
        o = (z + 4 - q // 2) % 4

        @pl.when(jnp.logical_and(ok, o > 0))
        def _():
            last(m, o).wait_send()

    @pl.when(jnp.logical_and(owner, has_mirror))
    def _():
        for h2 in range(2):
            mir(h2).wait_send()


def shards(half, metric, survive):
    bf, f32, i16 = jnp.bfloat16, jnp.float32, jnp.int16
    rows = half.reshape(CH, half.shape[-1])
    perm = jnp.asarray(perm_matrix(), bf)
    vm, dma = pltpu.VMEM, pltpu.SemaphoreType.DMA
    scratch = [
        vm((NCH, CH, CH), bf), vm((48, CH), bf),
        vm((NCH, CH, CH), bf), vm((NCH, CH, CH), bf), vm((CH, CH), bf),
        vm((NCH, 2 * CH, CH), bf), vm((NCH, CH, 2 * CH), bf),
        vm((4, NCH, 1, CH), f32), vm((12, 8, CH), f32),
        vm((NCH, 8, CH), f32), vm((NCH, 8, CH), f32), vm((2, NCH, 8, CH), f32), vm((2, NCH, 8, CH), f32),
        vm((11, 8, CH), f32), vm((11, 8, CH), f32), vm((11, 2, 8, CH), f32), vm((11, 2, 8, CH), f32),
        vm((3, 12, TR, CH), f32),
        vm((12, TR, CH), i16), vm((2, 12, TR, CH), i16), vm((2, 12, HR, CH), i16), vm((2, 12, TR, CH), i16),
        vm((3, TR, CH), i16), vm((2, 3, TR, CH), i16), vm((2, 3, HR, CH), i16), vm((2, 3, TR, CH), i16),
        vm((3, TR, CH), i16), vm((3, TR, CH), i16),
        vm((2, MR, CH), i16), vm((2, MR, CH), i16),
        dma((NCH,)), dma((NCH, 8)), dma((NCH, 8)), dma((8,)), dma((8,)), dma((NCH,)), dma((NCH,)),
        dma((4, NCH)), dma((4, NCH)), dma((12,)), dma((12,)),
        dma((12, 2)), dma((2, 12)), dma((2, 12)), dma((2, 12)),
        dma((3, 2)), dma((2, 3)), dma((2, 3)), dma((2, 3)),
        dma((3,)), dma((3,)), dma((2,)), dma((2,)),
    ]
    return pl.pallas_call(
        kernel,
        out_shape=jax.ShapeDtypeStruct((TR, CH), f32),
        in_specs=[pl.BlockSpec(memory_space=pl.ANY), pl.BlockSpec(memory_space=pltpu.SMEM),
                  pl.BlockSpec(memory_space=pltpu.VMEM), pl.BlockSpec(memory_space=pltpu.VMEM)],
        out_specs=pl.BlockSpec(memory_space=pltpu.VMEM),
        scratch_shapes=scratch,
        compiler_params=pltpu.CompilerParams(collective_id=0, has_side_effects=True,
                                             vmem_limit_bytes=62 * 1024 * 1024),
    )(rows, survive, metric, perm)


def solution(mesh):
    placed = (P("aux", "orb", None), P("aux", None), P("aux", "orb", None))
    return jax.shard_map(shards, mesh=mesh, in_specs=placed, out_specs=P("orb", "aux"), check_vma=False)
```

```python
import jax
import jax.numpy as jnp
from jax import lax
from jax.experimental import pallas as pl
from jax.experimental.pallas import tpu as pltpu
from jax.sharding import PartitionSpec as P

MESH = pl.DeviceIdType.MESH
CH = 384
NCH = 8
TR = 192
HR = 96
MR = 112
TOP = 32700.0
TINY = 1e-36
ORDER = ((2, 0), (2, 1), (1, 0), (3, 0), (1, 1), (3, 1), (0, 1))


def third(n):
    return jnp.floor((n + 0.5) * (1.0 / 3.0))


def iota(shape, dim):
    return lax.broadcasted_iota(jnp.int32, shape, dim).astype(jnp.float32)


def sorting():
    row, col = iota((CH, CH), 0), iota((CH, CH), 1)
    d = jnp.floor((row + 0.5) * (1.0 / 48.0))
    rest = row - 48.0 * d
    aux = third(rest)
    return jnp.where(col == 21.0 * aux + 3.0 * d + rest, 1.0, 0.0).astype(jnp.bfloat16)


def spread(metric):
    f32, bf = jnp.float32, jnp.bfloat16
    left = jnp.where(third(iota((CH, 128), 0)) == iota((CH, 128), 1), 1.0, 0.0).astype(bf)
    right = jnp.where(third(iota((128, CH), 1)) == iota((128, CH), 0), 1.0, 0.0).astype(bf)
    rows = jnp.dot(left, metric, preferred_element_type=f32).astype(bf)
    wide = jnp.dot(rows, right, preferred_element_type=f32)
    a, b = iota((CH, CH), 0), iota((CH, CH), 1)
    return jnp.where(a - 3.0 * third(a) == b - 3.0 * third(b), wide, 0.0).astype(bf)


def kernel(half, survive, metric, out, block, perm, whole, snd, rcv, m3, fb, ft, dvr, dv, cs1, csi1, rb1, rbi1, cs, csi, rb, rbi,
           kbuf, s1f, s1n, r1f, r1n, s2f, s2n, r2f, r2n, s3, r3, fin, s4, r4,
           lds, p1s, p1r, ks, kr, fs, fr, d1s, d1r, ds_, dr,
           q1fs, q1fr, q1ns, q1nr, q2fs, q2fr, q2ns, q2nr, q3s, q3r, q4s, q4r):
    f32 = jnp.float32
    aux = lax.axis_index("aux")
    orb = lax.axis_index("orb")
    z, c = aux // 2, aux % 2
    x, y = orb // 4, orb % 4
    me1 = x * (1 - c) + y * c
    me2 = y * (1 - c) + x * c
    sib = 2 * z + 1 - c

    def row_of(t, u):
        return t * (4 - 3 * c) + u * (1 + 3 * c)

    def ring1(o):
        return (aux, row_of((me1 + o) % 4, me2))

    def ring2(o):
        return (aux, row_of(me1, (me2 + o) % 4))

    def zdev(o, core):
        return (2 * ((z + o) % 4) + core, orb)

    pr = orb // 2
    mirror = [(2 * aux + h, pr) for h in range(2)]
    has_mirror = aux != pr

    def cut(q):
        return pl.ds(pl.multiple_of(q * CH, 128), CH)

    def load(q):
        return pltpu.make_async_copy(half.at[:, cut(q)], block.at[q], lds.at[q])

    for q in range(NCH):
        load(q).start()

    bar = pltpu.get_barrier_semaphore()
    for o in range(1, 8):
        pl.semaphore_signal(bar, inc=1, device_id=((aux + o) % 8, orb), device_id_type=MESH)
    for o in range(1, 4):
        pl.semaphore_signal(bar, inc=1, device_id=ring1(o), device_id_type=MESH)
        pl.semaphore_signal(bar, inc=1, device_id=ring2(o), device_id_type=MESH)

    def rcopy(src, dst, ss, rs, dev):
        return pltpu.make_async_remote_copy(src_ref=src, dst_ref=dst, send_sem=ss, recv_sem=rs,
                                            device_id=dev, device_id_type=MESH)

    def al48(v):
        return pl.ds(pl.multiple_of(v * 48, 16), 48)

    def mcopy(o):
        rows = pl.ds(pl.multiple_of(aux * 16, 16), 16)
        return rcopy(metric, whole.at[rows], ks.at[o], kr.at[o], ((aux + o) % 8, orb))

    def send(q, o, flip):
        dev = 2 * ((z + o) % 4) + (c + flip) % 2
        return rcopy(snd.at[q, al48(dev)], rcv.at[q, al48(aux)], p1s.at[q, 2 * o + flip], p1r.at[q, aux], (dev, orb))

    def arrival(q, a):
        return rcopy(rcv.at[q, al48(a)], rcv.at[q, al48(a)], p1s.at[q, 0], p1r.at[q, a], (sib, orb))

    def gate(q):
        flags = [jnp.full((1, 128), survive[0, 0, 3 * q + n].astype(f32)) for n in range(3)]
        return jnp.concatenate(flags, axis=1).astype(jnp.bfloat16)

    def sort(q):
        load(q).wait()
        kept = block[q] * gate(q)
        snd[q] = jnp.dot(perm[...], kept, preferred_element_type=f32).astype(jnp.bfloat16)
        rcv[q, al48(aux), :] = snd[q, al48(aux), :]

    def sends(q):
        for o, flip in ORDER:
            send(q, o, flip).start()

    perm[...] = sorting()
    sort(0)
    pl.semaphore_wait(bar, 13)
    for o in range(1, 8):
        mcopy(o).start()
    sends(0)
    whole[pl.ds(pl.multiple_of(aux * 16, 16), 16), :] = metric[...]

    @pl.loop(1, NCH)
    def _(q):
        sort(q)
        sends(q)

    for o in range(1, 8):
        rows = pl.ds(pl.multiple_of((aux + 8 - o) % 8 * 16, 16), 16)
        rcopy(metric, whole.at[rows], ks.at[o], kr.at[o], (sib, orb)).wait_recv()
    m3[...] = spread(whole[...])

    def fcopy(q):
        return rcopy(fb.at[q, pl.ds(0, CH)], fb.at[q, pl.ds(CH, CH)], fs.at[q], fr.at[q], (sib, orb))

    def scales(val):
        val = jnp.maximum(val, TINY)
        lane = lax.broadcasted_iota(jnp.int32, val.shape, 1)
        inv = lax.rsqrt(val)
        yield val * inv, inv
        for h in range(2):
            part = jnp.where((lane >= TR) == (h == 1), val, TINY)
            top = jnp.broadcast_to(jnp.max(part, axis=1, keepdims=True), val.shape)
            tinv = lax.rsqrt(top)
            yield top * tinv * (1.0 / TOP), tinv * TOP

    def tables1(k, rows, val):
        for n, (sc, inv) in enumerate(scales(val)):
            if n == 0:
                cs1[k, rows, :], csi1[k, rows, :] = sc, inv
            else:
                rb1[n - 1, k, rows, :], rbi1[n - 1, k, rows, :] = sc, inv

    def tables(first, terms):
        for i, val in enumerate(terms):
            for n, (sc, inv) in enumerate(scales(val)):
                if n == 0:
                    cs[first + i], csi[first + i] = sc, inv
                else:
                    rb[first + i, n - 1], rbi[first + i, n - 1] = sc, inv

    def gather(level, dev):
        base = 4 * level
        for o in range(1, 4):
            rcopy(dv.at[base], dv.at[base + 4 - o], ds_.at[base + o], dr.at[base + 4 - o], dev(o)).start()

    def gathered(level, dev):
        base = 4 * level
        for o in range(1, 4):
            rcopy(dv.at[base], dv.at[base + o], ds_.at[base + o], dr.at[base + o], dev(o)).wait_recv()
        return [dv[base + o] for o in range(4)]

    def ring_terms(d):
        return [d[0], d[3], d[1], d[0] + d[3], d[0] + d[1], d[3] + d[2], d[1] + d[2]]

    def dcopy(q, o):
        return rcopy(dvr.at[0, q], dvr.at[4 - o, q], d1s.at[o, q], d1r.at[4 - o, q], ring1(o))

    def enc1(val, n, h, p, q):
        inv = csi1[q, pl.ds(n, 1), :] * rbi1[h, p, pl.ds(n, 1), :]
        return jnp.round(val * inv).astype(jnp.int32).astype(jnp.int16)

    def dec1(val, n, h, p, q):
        sc = cs1[q, pl.ds(n, 1), :] * rb1[h, p, pl.ds(n, 1), :]
        return val.astype(jnp.int32).astype(f32) * sc

    def enc(val, n, h, p, q):
        inv = csi[n, pl.ds(q, 1), :] * rbi[n, h, pl.ds(p, 1), :]
        return jnp.round(val * inv).astype(jnp.int32).astype(jnp.int16)

    def dec(val, n, h, p, q):
        sc = cs[n, pl.ds(q, 1), :] * rb[n, h, pl.ds(p, 1), :]
        return val.astype(jnp.int32).astype(f32) * sc

    def held(p, k):
        return jnp.logical_or(k < 4, jnp.logical_and(k == 4, p % 2 == p // 4))

    def where(t, u, m):
        r = row_of(t, u)
        p = r // 2
        k = c + 2 * m
        return r % 2, p, (p + k) % 8, held(p, k)

    tp, tm, tf = (me1 + 1) % 4, (me1 + 3) % 4, (me1 + 2) % 4

    def pair_of(k, j):
        g = (k - j + j % 2) // 5
        return j + g * (k - j), k - g * (k - j)

    def place(p, q, h):
        a, b = p // 2, 2 * (p % 2) + h
        t, u = a * (1 - c) + b * c, b * (1 - c) + a * c
        return u * 3 + ((q - p + 8) % 8) // 2, (t - me1 + 4) % 4

    def each(k, body):
        @pl.loop(0, k + 1)
        def _(j):
            p, q = pair_of(k, j)

            @pl.when((p + q) % 2 == c)
            def _():
                body(p, q)

    def far1(i, half_at):
        rows = pl.ds(half_at * HR, HR)
        dst = 0 if half_at == 0 else 1
        return rcopy(s1f.at[i, rows], r1f.at[dst, i], q1fs.at[i, half_at], q1fr.at[dst, i],
                     ring1(1 if half_at == 0 else 3))

    def near1(i, way, dev):
        return rcopy(s1n.at[way, i], r1n.at[way, i], q1ns.at[way, i], q1nr.at[way, i], dev)

    def pair(k):
        fcopy(k).wait_recv()
        both = fb[k]
        ft[k] = both.T
        wide = both.astype(f32)
        norm = jnp.sum(wide * wide, axis=0, keepdims=True)
        dvr[0, k] = norm
        for o in range(1, 4):
            dcopy(k, o).start()
        tables1(k, pl.ds(0, 1), norm)

    def compute(k):
        def body(p, q):
            tile = jnp.dot(ft[p], fb[q], preferred_element_type=f32)
            for h in range(2):
                i, role = place(p, q, h)
                part = tile[h * TR:(h + 1) * TR]

                @pl.when(role == 2)
                def _():
                    s1f[i] = enc1(part, 0, h, p, q)
                    far1(i, 0).start()
                    far1(i, 1).start()

                @pl.when(role != 2)
                def _():
                    kbuf[(role + 1) // 2, i] = part

        each(k, body)

    def norms(k):
        for o in range(1, 4):
            rcopy(dvr.at[0, k], dvr.at[o, k], d1s.at[o, k], d1r.at[o, k], ring1(o)).wait_recv()
        d = [dvr[o, k] for o in range(4)]
        whole = d[0] + d[1] + d[2] + d[3]
        tables1(k, slice(None), jnp.concatenate(ring_terms(d) + [whole], axis=0))
        dv[4, pl.ds(k, 1), :] = whole

    def pass_on(k):
        def body(p, q):
            for h in range(2):
                i, role = place(p, q, h)

                @pl.when(role % 2 == 1)
                def _():
                    way = role // 2
                    pltpu.make_async_remote_copy(
                        src_ref=s1f.at[i, pl.ds(0, HR)], dst_ref=r1f.at[way, i], send_sem=q1fs.at[i, 0],
                        recv_sem=q1fr.at[way, i], device_id=ring1(1), device_id_type=MESH).wait_recv()
                    rows = pl.ds(pl.multiple_of(way * HR, 32), HR)
                    kbuf[1 + way, i, rows, :] = kbuf[1 + way, i, rows, :] + dec1(r1f[way, i], 1 + way, h, p, q)
                    s1n[way, i] = enc1(kbuf[1 + way, i], 3 + way, h, p, q)
                    near1(i, way, ring1(role)).start()

        each(k, body)

    def collect(k):
        def body(p, q):
            for h in range(2):
                i, role = place(p, q, h)

                @pl.when(role == 0)
                def _():
                    near1(i, 0, ring1(1)).wait_recv()
                    near1(i, 1, ring1(1)).wait_recv()
                    kbuf[0, i] = kbuf[0, i] + dec1(r1n[0, i], 5, h, p, q) + dec1(r1n[1, i], 6, h, p, q)

        each(k, body)

    @pl.loop(0, NCH)
    def _(k):
        for o in range(1, 8):
            arrival(k, (aux + o) % 8).wait_recv()
        fb[k, 0:CH, :] = jnp.dot(m3[...], rcv[k], preferred_element_type=f32).astype(jnp.bfloat16)
        fcopy(k).start()

        @pl.when(k > 0)
        def _():
            compute(k - 1)

        @pl.when(k > 1)
        def _():
            norms(k - 2)
            pass_on(k - 2)

        @pl.when(k > 2)
        def _():
            collect(k - 3)

        pair(k)

    compute(NCH - 1)
    norms(NCH - 2)
    norms(NCH - 1)
    gather(1, ring2)
    pass_on(NCH - 2)
    collect(NCH - 3)
    pass_on(NCH - 1)
    collect(NCH - 2)
    d1 = gathered(1, ring2)
    tables(0, ring_terms(d1))
    dv[8] = d1[0] + d1[1] + d1[2] + d1[3]

    def zline(o):
        return zdev(o, c)

    gather(2, zline)
    collect(NCH - 1)

    def own1(u, m, then):
        h, p, q, ok = where(me1, u, m)

        @pl.when(ok)
        def _():
            then(kbuf[0, u * 3 + m], h, p, q)

    def far2(m, half_at):
        rows = pl.ds(half_at * HR, HR)
        dst = 0 if half_at == 0 else 1
        return rcopy(s2f.at[m, rows], r2f.at[dst, m], q2fs.at[m, half_at], q2fr.at[dst, m],
                     ring2(1 if half_at == 0 else 3))

    def near2(m, way):
        return rcopy(s2n.at[way, m], r2n.at[way, m], q2ns.at[way, m], q2nr.at[way, m],
                     ring2(1 if way == 0 else 3))

    uf, up, um = (me2 + 2) % 4, (me2 + 1) % 4, (me2 + 3) % 4

    @pl.loop(0, 3)
    def _(m):
        def then(tile, h, p, q):
            s2f[m] = enc(tile, 0, h, p, q)
            far2(m, 0).start()
            far2(m, 1).start()

        own1(uf, m, then)

    for way, u in ((0, up), (1, um)):
        @pl.loop(0, 3)
        def _(m):
            def then(tile, h, p, q):
                far2(m, way).wait_recv()
                add = dec(r2f[way, m], 1 + way, h, p, q)
                low, high = tile[:HR], tile[HR:]
                if way == 0:
                    low = low + add
                else:
                    high = high + add
                s2n[way, m, 0:HR, :] = enc(low, 3 + way, h, p, q)
                s2n[way, m, HR:TR, :] = enc(high, 3 + way, h, p, q)
                near2(m, way).start()

            own1(u, m, then)

    d2 = gathered(2, zline)
    tables(7, d2)

    def last(m, o, q):
        return rcopy(s3.at[m], r3.at[o], q3s.at[m], q3r.at[o], zdev(4 - o, q % 2))

    def stays(o, q):
        return jnp.logical_and(o == 0, q % 2 == c)

    @pl.loop(0, 3)
    def _(m):
        def then(tile, h, p, q):
            near2(m, 0).wait_recv()
            near2(m, 1).wait_recv()
            tile = tile + dec(r2n[0, m], 5, h, p, q) + dec(r2n[1, m], 6, h, p, q)
            o = (z + 4 - q // 2) % 4

            @pl.when(stays(o, q))
            def _():
                fin[...] = tile

            @pl.when(jnp.logical_not(stays(o, q)))
            def _():
                s3[m] = enc(tile, 7, h, p, q)
                last(m, o, q).start()

        own1(me2, m, then)

    def mir(h):
        return rcopy(s4.at[h], r4.at[orb % 2], q4s.at[h], q4r.at[orb % 2], (mirror[h][1], mirror[h][0]))

    kk = (aux + 8 - pr) % 8
    owner = held(pr, kk)

    def got(o):
        rcopy(s3.at[0], r3.at[o], q3s.at[0], q3r.at[o], zdev(o, c)).wait_recv()
        return dec(r3[o], 7 + o, orb % 2, pr, aux)

    @pl.when(owner)
    def _():
        @pl.when(pr % 2 == 1)
        def _():
            fin[...] = got(0)

        tile = fin[...] + got(1) + got(2) + got(3)
        out[...] = tile

        @pl.when(has_mirror)
        def _():
            turned = tile.T
            for h2 in range(2):
                part = turned[h2 * TR:(h2 + 1) * TR]
                flat = jnp.concatenate([part[:HR], part[HR:]], axis=1)
                top = jnp.max(jnp.abs(flat), axis=0, keepdims=True)
                power = jnp.ceil(jnp.log2(jnp.maximum(top, TINY)))
                s4[h2, 0:HR, :] = jnp.round(flat * (jnp.exp2(-power) * TOP)).astype(jnp.int32).astype(jnp.int16)
                s4[h2, HR:MR, :] = jnp.broadcast_to(power, (16, CH)).astype(jnp.int32).astype(jnp.int16)
                mir(h2).start()

    @pl.when(jnp.logical_not(owner))
    def _():
        for h2 in range(2):
            rcopy(s4.at[0], r4.at[h2], q4s.at[0], q4r.at[h2], (mirror[h2][1], mirror[h2][0])).wait_recv()
        parts = []
        for h2 in range(2):
            power = r4[h2, HR:MR, :].astype(jnp.int32).astype(f32)[0:1]
            parts.append(r4[h2, 0:HR, :].astype(jnp.int32).astype(f32) * (jnp.exp2(power) * (1.0 / TOP)))
        out[0:HR, :] = jnp.concatenate([parts[0][:, :TR], parts[1][:, :TR]], axis=1)
        out[HR:TR, :] = jnp.concatenate([parts[0][:, TR:], parts[1][:, TR:]], axis=1)

    for o in range(1, 8):
        mcopy(o).wait_send()

    @pl.loop(0, NCH)
    def _(q):
        for o, flip in ORDER:
            send(q, o, flip).wait_send()
        fcopy(q).wait_send()
        for o in range(1, 4):
            dcopy(q, o).wait_send()

    for level, dev in ((1, ring2), (2, zline)):
        for o in range(1, 4):
            rcopy(dv.at[4 * level], dv.at[4 * level], ds_.at[4 * level + o], dr.at[4 * level], dev(o)).wait_send()

    @pl.loop(0, 12)
    def _(j):
        u, m = j // 3, j % 3

        @pl.when(where(tf, u, m)[3])
        def _():
            far1(j, 0).wait_send()
            far1(j, 1).wait_send()

        for way, t in ((0, tp), (1, tm)):
            @pl.when(where(t, u, m)[3])
            def _():
                near1(j, way, ring1(1)).wait_send()

    @pl.loop(0, 3)
    def _(m):
        @pl.when(where(me1, uf, m)[3])
        def _():
            far2(m, 0).wait_send()
            far2(m, 1).wait_send()

        for way, u in ((0, up), (1, um)):
            @pl.when(where(me1, u, m)[3])
            def _():
                near2(m, way).wait_send()

        _, _, q, ok = where(me1, me2, m)
        o = (z + 4 - q // 2) % 4

        @pl.when(jnp.logical_and(ok, jnp.logical_not(stays(o, q))))
        def _():
            last(m, o, q).wait_send()

    @pl.when(jnp.logical_and(owner, has_mirror))
    def _():
        for h2 in range(2):
            mir(h2).wait_send()


def shards(half, metric, survive):
    bf, f32, i16 = jnp.bfloat16, jnp.float32, jnp.int16
    rows = half.reshape(CH, half.shape[-1])
    vm, dma = pltpu.VMEM, pltpu.SemaphoreType.DMA
    scratch = [
        vm((NCH, CH, CH), bf), vm((CH, CH), bf), vm((128, 128), bf),
        vm((NCH, CH, CH), bf), vm((NCH, CH, CH), bf), vm((CH, CH), bf),
        vm((NCH, 2 * CH, CH), bf), vm((NCH, CH, 2 * CH), bf),
        vm((4, NCH, 1, CH), f32), vm((12, 8, CH), f32),
        vm((NCH, 8, CH), f32), vm((NCH, 8, CH), f32), vm((2, NCH, 8, CH), f32), vm((2, NCH, 8, CH), f32),
        vm((11, 8, CH), f32), vm((11, 8, CH), f32), vm((11, 2, 8, CH), f32), vm((11, 2, 8, CH), f32),
        vm((3, 12, TR, CH), f32),
        vm((12, TR, CH), i16), vm((2, 12, TR, CH), i16), vm((2, 12, HR, CH), i16), vm((2, 12, TR, CH), i16),
        vm((3, TR, CH), i16), vm((2, 3, TR, CH), i16), vm((2, 3, HR, CH), i16), vm((2, 3, TR, CH), i16),
        vm((3, TR, CH), i16), vm((4, TR, CH), i16), vm((TR, CH), f32),
        vm((2, MR, CH), i16), vm((2, MR, CH), i16),
        dma((NCH,)), dma((NCH, 8)), dma((NCH, 8)), dma((8,)), dma((8,)), dma((NCH,)), dma((NCH,)),
        dma((4, NCH)), dma((4, NCH)), dma((12,)), dma((12,)),
        dma((12, 2)), dma((2, 12)), dma((2, 12)), dma((2, 12)),
        dma((3, 2)), dma((2, 3)), dma((2, 3)), dma((2, 3)),
        dma((3,)), dma((4,)), dma((2,)), dma((2,)),
    ]
    return pl.pallas_call(
        kernel,
        out_shape=jax.ShapeDtypeStruct((TR, CH), f32),
        in_specs=[pl.BlockSpec(memory_space=pl.ANY), pl.BlockSpec(memory_space=pltpu.SMEM),
                  pl.BlockSpec(memory_space=pltpu.VMEM)],
        out_specs=pl.BlockSpec(memory_space=pltpu.VMEM),
        scratch_shapes=scratch,
        compiler_params=pltpu.CompilerParams(collective_id=0, has_side_effects=True,
                                             vmem_limit_bytes=62 * 1024 * 1024),
    )(rows, survive, metric)


def solution(mesh):
    placed = (P("aux", "orb", None), P("aux", None), P("aux", "orb", None))
    return jax.shard_map(shards, mesh=mesh, in_specs=placed, out_specs=P("orb", "aux"), check_vma=False)
```

```python
import jax
import jax.numpy as jnp
from jax import lax
from jax.experimental import pallas as pl
from jax.experimental.pallas import tpu as pltpu
from jax.sharding import PartitionSpec as P

MESH = pl.DeviceIdType.MESH
CH = 384
NCH = 8
TR = 192
HR = 96
MR = 112
TOP = 32700.0
TINY = 1e-36
ORDER = ((2, 0), (2, 1), (1, 0), (3, 0), (1, 1), (3, 1), (0, 1))


def third(n):
    return jnp.floor((n + 0.5) * (1.0 / 3.0))


def iota(shape, dim):
    return lax.broadcasted_iota(jnp.int32, shape, dim).astype(jnp.float32)


def sorting():
    row, col = iota((CH, CH), 0), iota((CH, CH), 1)
    d = jnp.floor((row + 0.5) * (1.0 / 48.0))
    rest = row - 48.0 * d
    aux = third(rest)
    return jnp.where(col == 21.0 * aux + 3.0 * d + rest, 1.0, 0.0).astype(jnp.bfloat16)


def spread(metric):
    f32, bf = jnp.float32, jnp.bfloat16
    left = jnp.where(third(iota((CH, 128), 0)) == iota((CH, 128), 1), 1.0, 0.0).astype(bf)
    right = jnp.where(third(iota((128, CH), 1)) == iota((128, CH), 0), 1.0, 0.0).astype(bf)
    rows = jnp.dot(left, metric, preferred_element_type=f32).astype(bf)
    wide = jnp.dot(rows, right, preferred_element_type=f32)
    a, b = iota((CH, CH), 0), iota((CH, CH), 1)
    return jnp.where(a - 3.0 * third(a) == b - 3.0 * third(b), wide, 0.0).astype(bf)


def kernel(half, survive, metric, out, block, perm, whole, snd, rcv, m3, fb, ft, dvr, dv, cs1, csi1, rb1, rbi1, cs, csi, rb, rbi,
           kbuf, s1, r1, s2, r2, s3, r3, fin, s4, r4,
           lds, p1s, p1r, ks, kr, fs, fr, d1s, d1r, ds_, dr, q1s, q1r, q2s, q2r, q3s, q3r, q4s, q4r):
    f32 = jnp.float32
    aux = lax.axis_index("aux")
    orb = lax.axis_index("orb")
    z, c = aux // 2, aux % 2
    x, y = orb // 4, orb % 4
    me1 = x * (1 - c) + y * c
    me2 = y * (1 - c) + x * c
    sib = 2 * z + 1 - c

    def row_of(t, u):
        return t * (4 - 3 * c) + u * (1 + 3 * c)

    def ring1(o):
        return (aux, row_of((me1 + o) % 4, me2))

    def ring2(o):
        return (aux, row_of(me1, (me2 + o) % 4))

    def zdev(o, core):
        return (2 * ((z + o) % 4) + core, orb)

    pr = orb // 2
    mirror = [(2 * aux + h, pr) for h in range(2)]
    has_mirror = aux != pr

    def cut(q):
        return pl.ds(pl.multiple_of(q * CH, 128), CH)

    def load(q):
        return pltpu.make_async_copy(half.at[:, cut(q)], block.at[q], lds.at[q])

    for q in range(NCH):
        load(q).start()

    bar = pltpu.get_barrier_semaphore()
    for o in range(1, 8):
        pl.semaphore_signal(bar, inc=1, device_id=((aux + o) % 8, orb), device_id_type=MESH)
    for o in range(1, 4):
        pl.semaphore_signal(bar, inc=1, device_id=ring1(o), device_id_type=MESH)
        pl.semaphore_signal(bar, inc=1, device_id=ring2(o), device_id_type=MESH)

    def rcopy(src, dst, ss, rs, dev):
        return pltpu.make_async_remote_copy(src_ref=src, dst_ref=dst, send_sem=ss, recv_sem=rs,
                                            device_id=dev, device_id_type=MESH)

    def al48(v):
        return pl.ds(pl.multiple_of(v * 48, 16), 48)

    def mcopy(o):
        rows = pl.ds(pl.multiple_of(aux * 16, 16), 16)
        return rcopy(metric, whole.at[rows], ks.at[o], kr.at[o], ((aux + o) % 8, orb))

    def send(q, o, flip):
        dev = 2 * ((z + o) % 4) + (c + flip) % 2
        return rcopy(snd.at[q, al48(dev)], rcv.at[q, al48(aux)], p1s.at[q, 2 * o + flip], p1r.at[q, aux], (dev, orb))

    def arrival(q, a):
        return rcopy(rcv.at[q, al48(a)], rcv.at[q, al48(a)], p1s.at[q, 0], p1r.at[q, a], (sib, orb))

    def gate(q):
        flags = [jnp.full((1, 128), survive[0, 0, 3 * q + n].astype(f32)) for n in range(3)]
        return jnp.concatenate(flags, axis=1).astype(jnp.bfloat16)

    def sort(q):
        load(q).wait()
        kept = block[q] * gate(q)
        snd[q] = jnp.dot(perm[...], kept, preferred_element_type=f32).astype(jnp.bfloat16)
        rcv[q, al48(aux), :] = snd[q, al48(aux), :]

    def sends(q):
        for o, flip in ORDER:
            send(q, o, flip).start()

    perm[...] = sorting()
    sort(0)
    pl.semaphore_wait(bar, 13)
    for o in range(1, 8):
        mcopy(o).start()
    sends(0)
    whole[pl.ds(pl.multiple_of(aux * 16, 16), 16), :] = metric[...]

    @pl.loop(1, NCH)
    def _(q):
        sort(q)
        sends(q)

    for o in range(1, 8):
        rows = pl.ds(pl.multiple_of((aux + 8 - o) % 8 * 16, 16), 16)
        rcopy(metric, whole.at[rows], ks.at[o], kr.at[o], (sib, orb)).wait_recv()
    m3[...] = spread(whole[...])

    def fcopy(q):
        return rcopy(fb.at[q, pl.ds(0, CH)], fb.at[q, pl.ds(CH, CH)], fs.at[q], fr.at[q], (sib, orb))

    def scales(val):
        val = jnp.maximum(val, TINY)
        lane = lax.broadcasted_iota(jnp.int32, val.shape, 1)
        inv = lax.rsqrt(val)
        yield val * inv, inv
        for h in range(2):
            part = jnp.where((lane >= TR) == (h == 1), val, TINY)
            top = jnp.broadcast_to(jnp.max(part, axis=1, keepdims=True), val.shape)
            tinv = lax.rsqrt(top)
            yield top * tinv * (1.0 / TOP), tinv * TOP

    def tables1(k, rows, val):
        for n, (sc, inv) in enumerate(scales(val)):
            if n == 0:
                cs1[k, rows, :], csi1[k, rows, :] = sc, inv
            else:
                rb1[n - 1, k, rows, :], rbi1[n - 1, k, rows, :] = sc, inv

    def tables(first, terms):
        for i, val in enumerate(terms):
            for n, (sc, inv) in enumerate(scales(val)):
                if n == 0:
                    cs[first + i], csi[first + i] = sc, inv
                else:
                    rb[first + i, n - 1], rbi[first + i, n - 1] = sc, inv

    def gather(level, dev):
        base = 4 * level
        for o in range(1, 4):
            rcopy(dv.at[base], dv.at[base + 4 - o], ds_.at[base + o], dr.at[base + 4 - o], dev(o)).start()

    def gathered(level, dev):
        base = 4 * level
        for o in range(1, 4):
            rcopy(dv.at[base], dv.at[base + o], ds_.at[base + o], dr.at[base + o], dev(o)).wait_recv()
        return [dv[base + o] for o in range(4)]

    def dcopy(q, o):
        return rcopy(dvr.at[0, q], dvr.at[4 - o, q], d1s.at[o, q], d1r.at[4 - o, q], ring1(o))

    def enc1(val, n, h, p, q):
        inv = csi1[q, pl.ds(n, 1), :] * rbi1[h, p, pl.ds(n, 1), :]
        return jnp.round(val * inv).astype(jnp.int32).astype(jnp.int16)

    def dec1(val, n, h, p, q):
        sc = cs1[q, pl.ds(n, 1), :] * rb1[h, p, pl.ds(n, 1), :]
        return val.astype(jnp.int32).astype(f32) * sc

    def enc(val, n, h, p, q):
        inv = csi[n, pl.ds(q, 1), :] * rbi[n, h, pl.ds(p, 1), :]
        return jnp.round(val * inv).astype(jnp.int32).astype(jnp.int16)

    def dec(val, n, h, p, q):
        sc = cs[n, pl.ds(q, 1), :] * rb[n, h, pl.ds(p, 1), :]
        return val.astype(jnp.int32).astype(f32) * sc

    def held(p, k):
        return jnp.logical_or(k < 4, jnp.logical_and(k == 4, p % 2 == p // 4))

    def where(t, u, m):
        r = row_of(t, u)
        p = r // 2
        k = c + 2 * m
        return r % 2, p, (p + k) % 8, held(p, k)

    def pair_of(k, j):
        g = (k - j + j % 2) // 5
        return j + g * (k - j), k - g * (k - j)

    def place(p, q, h):
        a, b = p // 2, 2 * (p % 2) + h
        t, u = a * (1 - c) + b * c, b * (1 - c) + a * c
        return u * 3 + ((q - p + 8) % 8) // 2, (t - me1 + 4) % 4

    def each(k, body):
        @pl.loop(0, k + 1)
        def _(j):
            p, q = pair_of(k, j)

            @pl.when((p + q) % 2 == c)
            def _():
                body(p, q)

    def tile1(role, i):
        return rcopy(s1.at[role - 1, i], r1.at[3 - role, i], q1s.at[role - 1, i], q1r.at[3 - role, i], ring1(role))

    def tile2(role, m):
        return rcopy(s2.at[role - 1, m], r2.at[3 - role, m], q2s.at[role - 1, m], q2r.at[3 - role, m], ring2(role))

    def pair(k):
        fcopy(k).wait_recv()
        both = fb[k]
        ft[k] = both.T
        wide = both.astype(f32)
        norm = jnp.sum(wide * wide, axis=0, keepdims=True)
        dvr[0, k] = norm
        for o in range(1, 4):
            dcopy(k, o).start()
        tables1(k, pl.ds(0, 1), norm)

    def compute(k):
        def body(p, q):
            tile = jnp.dot(ft[p], fb[q], preferred_element_type=f32)
            for h in range(2):
                i, role = place(p, q, h)
                part = tile[h * TR:(h + 1) * TR]

                @pl.when(role == 0)
                def _():
                    kbuf[i] = part

                @pl.when(role > 0)
                def _():
                    s1[role - 1, i] = enc1(part, 0, h, p, q)
                    tile1(role, i).start()

        each(k, body)

    def norms(k):
        for o in range(1, 4):
            rcopy(dvr.at[0, k], dvr.at[o, k], d1s.at[o, k], d1r.at[o, k], ring1(o)).wait_recv()
        d = [dvr[o, k] for o in range(4)]
        tables1(k, slice(None), jnp.concatenate(d + d, axis=0))
        dv[4, pl.ds(k, 1), :] = d[0] + d[1] + d[2] + d[3]

    @pl.loop(0, NCH)
    def _(k):
        for o in range(1, 8):
            arrival(k, (aux + o) % 8).wait_recv()
        fb[k, 0:CH, :] = jnp.dot(m3[...], rcv[k], preferred_element_type=f32).astype(jnp.bfloat16)
        fcopy(k).start()

        @pl.when(k > 0)
        def _():
            compute(k - 1)

        pair(k)

    compute(NCH - 1)

    @pl.loop(0, NCH)
    def _(k):
        norms(k)

    gather(1, ring2)

    def total1(u, m, then):
        h, p, q, ok = where(me1, u, m)
        i = u * 3 + m

        @pl.when(ok)
        def _():
            tile = kbuf[i]
            for o in range(1, 4):
                rcopy(s1.at[0, i], r1.at[o - 1, i], q1s.at[0, i], q1r.at[o - 1, i], ring1(1)).wait_recv()
                tile = tile + dec1(r1[o - 1, i], o, h, p, q)
            then(tile, h, p, q)

    d1 = gathered(1, ring2)
    tables(0, d1)
    dv[8] = d1[0] + d1[1] + d1[2] + d1[3]

    def zline(o):
        return zdev(o, c)

    gather(2, zline)
    for role in (2, 1, 3):
        @pl.loop(0, 3)
        def _(m):
            def then(tile, h, p, q):
                s2[role - 1, m] = enc(tile, 0, h, p, q)
                tile2(role, m).start()

            total1((me2 + role) % 4, m, then)

    @pl.loop(0, 3)
    def _(m):
        def then(tile, h, p, q):
            kbuf[m] = tile

        total1(me2, m, then)

    d2 = gathered(2, zline)
    tables(4, d2)

    def last(m, o, q):
        return rcopy(s3.at[m], r3.at[o], q3s.at[m], q3r.at[o], zdev(4 - o, q % 2))

    def stays(o, q):
        return jnp.logical_and(o == 0, q % 2 == c)

    @pl.loop(0, 3)
    def _(m):
        h, p, q, ok = where(me1, me2, m)

        @pl.when(ok)
        def _():
            tile = kbuf[m]
            for n in range(1, 4):
                rcopy(s2.at[0, m], r2.at[n - 1, m], q2s.at[0, m], q2r.at[n - 1, m], ring2(1)).wait_recv()
                tile = tile + dec(r2[n - 1, m], n, h, p, q)
            o = (z + 4 - q // 2) % 4

            @pl.when(stays(o, q))
            def _():
                fin[...] = tile

            @pl.when(jnp.logical_not(stays(o, q)))
            def _():
                s3[m] = enc(tile, 4, h, p, q)
                last(m, o, q).start()

    def mir(h):
        return rcopy(s4.at[h], r4.at[orb % 2], q4s.at[h], q4r.at[orb % 2], (mirror[h][1], mirror[h][0]))

    kk = (aux + 8 - pr) % 8
    owner = held(pr, kk)

    def got(o):
        rcopy(s3.at[0], r3.at[o], q3s.at[0], q3r.at[o], zdev(o, c)).wait_recv()
        return dec(r3[o], 4 + o, orb % 2, pr, aux)

    @pl.when(owner)
    def _():
        @pl.when(pr % 2 == 1)
        def _():
            fin[...] = got(0)

        tile = fin[...] + got(1) + got(2) + got(3)
        out[...] = tile

        @pl.when(has_mirror)
        def _():
            turned = tile.T
            for h2 in range(2):
                part = turned[h2 * TR:(h2 + 1) * TR]
                flat = jnp.concatenate([part[:HR], part[HR:]], axis=1)
                top = jnp.max(jnp.abs(flat), axis=0, keepdims=True)
                power = jnp.ceil(jnp.log2(jnp.maximum(top, TINY)))
                s4[h2, 0:HR, :] = jnp.round(flat * (jnp.exp2(-power) * TOP)).astype(jnp.int32).astype(jnp.int16)
                s4[h2, HR:MR, :] = jnp.broadcast_to(power, (16, CH)).astype(jnp.int32).astype(jnp.int16)
                mir(h2).start()

    @pl.when(jnp.logical_not(owner))
    def _():
        for h2 in range(2):
            rcopy(s4.at[0], r4.at[h2], q4s.at[0], q4r.at[h2], (mirror[h2][1], mirror[h2][0])).wait_recv()
        parts = []
        for h2 in range(2):
            power = r4[h2, HR:MR, :].astype(jnp.int32).astype(f32)[0:1]
            parts.append(r4[h2, 0:HR, :].astype(jnp.int32).astype(f32) * (jnp.exp2(power) * (1.0 / TOP)))
        out[0:HR, :] = jnp.concatenate([parts[0][:, :TR], parts[1][:, :TR]], axis=1)
        out[HR:TR, :] = jnp.concatenate([parts[0][:, TR:], parts[1][:, TR:]], axis=1)

    for o in range(1, 8):
        mcopy(o).wait_send()

    @pl.loop(0, NCH)
    def _(q):
        for o, flip in ORDER:
            send(q, o, flip).wait_send()
        fcopy(q).wait_send()
        for o in range(1, 4):
            dcopy(q, o).wait_send()

    for level, dev in ((1, ring2), (2, zline)):
        for o in range(1, 4):
            rcopy(dv.at[4 * level], dv.at[4 * level], ds_.at[4 * level + o], dr.at[4 * level], dev(o)).wait_send()

    for role in range(1, 4):
        @pl.loop(0, 12)
        def _(j):
            @pl.when(where((me1 + role) % 4, j // 3, j % 3)[3])
            def _():
                tile1(role, j).wait_send()

        @pl.loop(0, 3)
        def _(m):
            @pl.when(where(me1, (me2 + role) % 4, m)[3])
            def _():
                tile2(role, m).wait_send()

    @pl.loop(0, 3)
    def _(m):
        _, _, q, ok = where(me1, me2, m)
        o = (z + 4 - q // 2) % 4

        @pl.when(jnp.logical_and(ok, jnp.logical_not(stays(o, q))))
        def _():
            last(m, o, q).wait_send()

    @pl.when(jnp.logical_and(owner, has_mirror))
    def _():
        for h2 in range(2):
            mir(h2).wait_send()


def shards(half, metric, survive):
    bf, f32, i16 = jnp.bfloat16, jnp.float32, jnp.int16
    rows = half.reshape(CH, half.shape[-1])
    vm, dma = pltpu.VMEM, pltpu.SemaphoreType.DMA
    scratch = [
        vm((NCH, CH, CH), bf), vm((CH, CH), bf), vm((128, 128), bf),
        vm((NCH, CH, CH), bf), vm((NCH, CH, CH), bf), vm((CH, CH), bf),
        vm((NCH, 2 * CH, CH), bf), vm((NCH, CH, 2 * CH), bf),
        vm((4, NCH, 1, CH), f32), vm((12, 8, CH), f32),
        vm((NCH, 8, CH), f32), vm((NCH, 8, CH), f32), vm((2, NCH, 8, CH), f32), vm((2, NCH, 8, CH), f32),
        vm((8, 8, CH), f32), vm((8, 8, CH), f32), vm((8, 2, 8, CH), f32), vm((8, 2, 8, CH), f32),
        vm((12, TR, CH), f32), vm((3, 12, TR, CH), i16), vm((3, 12, TR, CH), i16),
        vm((3, 3, TR, CH), i16), vm((3, 3, TR, CH), i16),
        vm((3, TR, CH), i16), vm((4, TR, CH), i16), vm((TR, CH), f32),
        vm((2, MR, CH), i16), vm((2, MR, CH), i16),
        dma((NCH,)), dma((NCH, 8)), dma((NCH, 8)), dma((8,)), dma((8,)), dma((NCH,)), dma((NCH,)),
        dma((4, NCH)), dma((4, NCH)), dma((12,)), dma((12,)),
        dma((3, 12)), dma((3, 12)), dma((3, 3)), dma((3, 3)),
        dma((3,)), dma((4,)), dma((2,)), dma((2,)),
    ]
    return pl.pallas_call(
        kernel,
        out_shape=jax.ShapeDtypeStruct((TR, CH), f32),
        in_specs=[pl.BlockSpec(memory_space=pl.ANY), pl.BlockSpec(memory_space=pltpu.SMEM),
                  pl.BlockSpec(memory_space=pltpu.VMEM)],
        out_specs=pl.BlockSpec(memory_space=pltpu.VMEM),
        scratch_shapes=scratch,
        compiler_params=pltpu.CompilerParams(collective_id=0, has_side_effects=True,
                                             vmem_limit_bytes=62 * 1024 * 1024),
    )(rows, survive, metric)


def solution(mesh):
    placed = (P("aux", "orb", None), P("aux", None), P("aux", "orb", None))
    return jax.shard_map(shards, mesh=mesh, in_specs=placed, out_specs=P("orb", "aux"), check_vma=False)
```

```python
import jax
import jax.numpy as jnp
from jax import lax
from jax.experimental import pallas as pl
from jax.experimental.pallas import tpu as pltpu
from jax.sharding import PartitionSpec as P

MESH = pl.DeviceIdType.MESH
CH = 384
NCH = 8
TR = 192
HR = 96
TOP = 32700.0
TINY = 1e-36
ORDER = ((2, 0), (2, 1), (1, 0), (3, 0), (1, 1), (3, 1), (0, 1))


def third(n):
    return jnp.floor((n + 0.5) * (1.0 / 3.0))


def iota(shape, dim):
    return lax.broadcasted_iota(jnp.int32, shape, dim).astype(jnp.float32)


def sorting():
    row, col = iota((CH, CH), 0), iota((CH, CH), 1)
    d = jnp.floor((row + 0.5) * (1.0 / 48.0))
    rest = row - 48.0 * d
    aux = third(rest)
    return jnp.where(col == 21.0 * aux + 3.0 * d + rest, 1.0, 0.0).astype(jnp.bfloat16)


def spread(metric):
    f32, bf = jnp.float32, jnp.bfloat16
    left = jnp.where(third(iota((CH, 128), 0)) == iota((CH, 128), 1), 1.0, 0.0).astype(bf)
    right = jnp.where(third(iota((128, CH), 1)) == iota((128, CH), 0), 1.0, 0.0).astype(bf)
    rows = jnp.dot(left, metric, preferred_element_type=f32).astype(bf)
    wide = jnp.dot(rows, right, preferred_element_type=f32)
    a, b = iota((CH, CH), 0), iota((CH, CH), 1)
    return jnp.where(a - 3.0 * third(a) == b - 3.0 * third(b), wide, 0.0).astype(bf)


def kernel(half, survive, metric, out, block, perm, whole, snd, rcv, m3, fb, ft, dvr, dv, cs1, csi1, rb1, rbi1, cs, csi, rb, rbi,
           kbuf, s1, r1, s2, r2, s3, r3, s4, r4,
           lds, p1s, p1r, ks, kr, fs, fr, d1s, d1r, ds_, dr, q1s, q1r, q2s, q2r, q3s, q3r, q4s, q4r):
    f32 = jnp.float32
    aux = lax.axis_index("aux")
    orb = lax.axis_index("orb")
    z, c = aux // 2, aux % 2
    x, y = orb // 4, orb % 4
    me1 = x * (1 - c) + y * c
    me2 = y * (1 - c) + x * c
    sib = 2 * z + 1 - c

    def row_of(t, u):
        return t * (4 - 3 * c) + u * (1 + 3 * c)

    def ring1(o):
        return (aux, row_of((me1 + o) % 4, me2))

    def ring2(o):
        return (aux, row_of(me1, (me2 + o) % 4))

    def zdev(o, core):
        return (2 * ((z + o) % 4) + core, orb)

    pr = orb // 2
    def cut(q):
        return pl.ds(pl.multiple_of(q * CH, 128), CH)

    def load(q):
        return pltpu.make_async_copy(half.at[:, cut(q)], block.at[q], lds.at[q])

    for q in range(NCH):
        load(q).start()

    bar = pltpu.get_barrier_semaphore()
    for o in range(1, 8):
        pl.semaphore_signal(bar, inc=1, device_id=((aux + o) % 8, orb), device_id_type=MESH)
    for o in range(1, 4):
        pl.semaphore_signal(bar, inc=1, device_id=ring1(o), device_id_type=MESH)
        pl.semaphore_signal(bar, inc=1, device_id=ring2(o), device_id_type=MESH)

    def rcopy(src, dst, ss, rs, dev):
        return pltpu.make_async_remote_copy(src_ref=src, dst_ref=dst, send_sem=ss, recv_sem=rs,
                                            device_id=dev, device_id_type=MESH)

    def al48(v):
        return pl.ds(pl.multiple_of(v * 48, 16), 48)

    def mcopy(o):
        rows = pl.ds(pl.multiple_of(aux * 16, 16), 16)
        return rcopy(metric, whole.at[rows], ks.at[o], kr.at[o], ((aux + o) % 8, orb))

    def send(q, o, flip):
        dev = 2 * ((z + o) % 4) + (c + flip) % 2
        return rcopy(snd.at[q, al48(dev)], rcv.at[q, al48(aux)], p1s.at[q, 2 * o + flip], p1r.at[q, aux], (dev, orb))

    def arrival(q, a):
        return rcopy(rcv.at[q, al48(a)], rcv.at[q, al48(a)], p1s.at[q, 0], p1r.at[q, a], (sib, orb))

    def gate(q):
        flags = [jnp.full((1, 128), survive[0, 0, 3 * q + n].astype(f32)) for n in range(3)]
        return jnp.concatenate(flags, axis=1).astype(jnp.bfloat16)

    def sort(q):
        load(q).wait()
        kept = block[q] * gate(q)
        snd[q] = jnp.dot(perm[...], kept, preferred_element_type=f32).astype(jnp.bfloat16)
        rcv[q, al48(aux), :] = snd[q, al48(aux), :]

    def sends(q):
        for o, flip in ORDER:
            send(q, o, flip).start()

    perm[...] = sorting()
    sort(0)
    pl.semaphore_wait(bar, 13)
    for o in range(1, 8):
        mcopy(o).start()
    sends(0)
    whole[pl.ds(pl.multiple_of(aux * 16, 16), 16), :] = metric[...]

    @pl.loop(1, NCH)
    def _(q):
        sort(q)
        sends(q)

    for o in range(1, 8):
        rows = pl.ds(pl.multiple_of((aux + 8 - o) % 8 * 16, 16), 16)
        rcopy(metric, whole.at[rows], ks.at[o], kr.at[o], (sib, orb)).wait_recv()
    m3[...] = spread(whole[...])

    def fcopy(q):
        return rcopy(fb.at[q, pl.ds(0, CH)], fb.at[q, pl.ds(CH, CH)], fs.at[q], fr.at[q], (sib, orb))

    def scales(val):
        val = jnp.maximum(val, TINY)
        lane = lax.broadcasted_iota(jnp.int32, val.shape, 1)
        inv = lax.rsqrt(val)
        yield val * inv, inv
        for h in range(2):
            part = jnp.where((lane >= TR) == (h == 1), val, TINY)
            top = jnp.broadcast_to(jnp.max(part, axis=1, keepdims=True), val.shape)
            tinv = lax.rsqrt(top)
            yield top * tinv * (1.0 / TOP), tinv * TOP

    def tables1(k, rows, val):
        for n, (sc, inv) in enumerate(scales(val)):
            if n == 0:
                cs1[k, rows, :], csi1[k, rows, :] = sc, inv
            else:
                rb1[n - 1, k, rows, :], rbi1[n - 1, k, rows, :] = sc, inv

    def tables(first, terms):
        for i, val in enumerate(terms):
            for n, (sc, inv) in enumerate(scales(val)):
                if n == 0:
                    cs[first + i], csi[first + i] = sc, inv
                else:
                    rb[first + i, n - 1], rbi[first + i, n - 1] = sc, inv

    def gather(level, dev):
        base = 4 * level
        for o in range(1, 4):
            rcopy(dv.at[base], dv.at[base + 4 - o], ds_.at[base + o], dr.at[base + 4 - o], dev(o)).start()

    def gathered(level, dev):
        base = 4 * level
        for o in range(1, 4):
            rcopy(dv.at[base], dv.at[base + o], ds_.at[base + o], dr.at[base + o], dev(o)).wait_recv()
        return [dv[base + o] for o in range(4)]

    def dcopy(q, o):
        return rcopy(dvr.at[0, q], dvr.at[4 - o, q], d1s.at[o, q], d1r.at[4 - o, q], ring1(o))

    def enc1(val, n, h, p, q):
        inv = csi1[q, pl.ds(n, 1), :] * rbi1[h, p, pl.ds(n, 1), :]
        return jnp.round(val * inv).astype(jnp.int32).astype(jnp.int16)

    def dec1(val, n, h, p, q):
        sc = cs1[q, pl.ds(n, 1), :] * rb1[h, p, pl.ds(n, 1), :]
        return val.astype(jnp.int32).astype(f32) * sc

    def enc(val, n, h, p, q):
        inv = csi[n, pl.ds(q, 1), :] * rbi[n, h, pl.ds(p, 1), :]
        return jnp.round(val * inv).astype(jnp.int32).astype(jnp.int16)

    def dec(val, n, h, p, q):
        sc = cs[n, pl.ds(q, 1), :] * rb[n, h, pl.ds(p, 1), :]
        return val.astype(jnp.int32).astype(f32) * sc

    def where(t, i):
        p = 2 * (i // 4) + t // 2
        q = 2 * (i % 4) + (i // 4 + c) % 2
        return t % 2, p, q, q >= p

    def slot(u, m):
        return m * 4 + (u - m + 4) % 4

    def source(p, q, h):
        core = (p // 2 + q) % 2
        t, u = 2 * (p % 2) + h, (p // 2 + q // 2) % 4
        return t * (4 - 3 * core) + u * (1 + 3 * core), core

    def place(p, q, h):
        return (p // 2) * 4 + q // 2, (2 * (p % 2) + h - me1 + 4) % 4

    def each(k, body):
        @pl.loop(0, k + 1)
        def _(j):
            @pl.when((j // 2 + k) % 2 == c)
            def _():
                body(j, k)

    def tile1(role, i):
        return rcopy(s1.at[role - 1, i], r1.at[3 - role, i], q1s.at[role - 1, i], q1r.at[3 - role, i], ring1(role))

    def tile2(role, m):
        return rcopy(s2.at[role - 1, m], r2.at[3 - role, m], q2s.at[role - 1, m], q2r.at[3 - role, m], ring2(role))

    def pair(k):
        fcopy(k).wait_recv()
        both = fb[k]
        ft[k] = both.T
        wide = both.astype(f32)
        norm = jnp.sum(wide * wide, axis=0, keepdims=True)
        dvr[0, k] = norm
        for o in range(1, 4):
            dcopy(k, o).start()
        tables1(k, pl.ds(0, 1), norm)

    def compute(k):
        def body(p, q):
            tile = jnp.dot(ft[p], fb[q], preferred_element_type=f32)
            for h in range(2):
                i, role = place(p, q, h)
                part = tile[h * TR:(h + 1) * TR]

                @pl.when(role == 0)
                def _():
                    kbuf[i] = part

                @pl.when(role > 0)
                def _():
                    s1[role - 1, i] = enc1(part, 0, h, p, q)
                    tile1(role, i).start()

        each(k, body)

    def norms(k):
        for o in range(1, 4):
            rcopy(dvr.at[0, k], dvr.at[o, k], d1s.at[o, k], d1r.at[o, k], ring1(o)).wait_recv()
        d = [dvr[o, k] for o in range(4)]
        tables1(k, slice(None), jnp.concatenate(d + d, axis=0))
        dv[4, pl.ds(k, 1), :] = d[0] + d[1] + d[2] + d[3]

    @pl.loop(0, NCH)
    def _(k):
        for o in range(1, 8):
            arrival(k, (aux + o) % 8).wait_recv()
        fb[k, 0:CH, :] = jnp.dot(m3[...], rcv[k], preferred_element_type=f32).astype(jnp.bfloat16)
        fcopy(k).start()

        @pl.when(k > 0)
        def _():
            compute(k - 1)

        pair(k)

    compute(NCH - 1)

    @pl.loop(0, NCH)
    def _(k):
        norms(k)

    gather(1, ring2)

    def total1(u, m, then):
        i = slot(u, m)
        h, p, q, ok = where(me1, i)

        @pl.when(ok)
        def _():
            tile = kbuf[i]
            for o in range(1, 4):
                rcopy(s1.at[0, i], r1.at[o - 1, i], q1s.at[0, i], q1r.at[o - 1, i], ring1(1)).wait_recv()
                tile = tile + dec1(r1[o - 1, i], o, h, p, q)
            then(tile, h, p, q)

    d1 = gathered(1, ring2)
    tables(0, d1)
    dv[8] = d1[0] + d1[1] + d1[2] + d1[3]

    def zline(o):
        return zdev(o, c)

    gather(2, zline)
    for role in (2, 1, 3):
        @pl.loop(0, 4)
        def _(m):
            def then(tile, h, p, q):
                s2[role - 1, m] = enc(tile, 0, h, p, q)
                tile2(role, m).start()

            total1((me2 + role) % 4, m, then)

    @pl.loop(0, 4)
    def _(m):
        def then(tile, h, p, q):
            kbuf[m] = tile

        total1(me2, m, then)

    d2 = gathered(2, zline)
    tables(4, d2)

    def last(m, h, p, q):
        return rcopy(s3.at[m], r3.at[z], q3s.at[m], q3r.at[z], (q, 2 * p + h))

    def turned(m, n, h, p, q):
        return rcopy(s4.at[m, n], r4.at[h, z], q4s.at[m, n], q4r.at[h, z], (p, 2 * q + n))

    def this(a, o):
        return jnp.logical_and(aux == a, orb == o)

    @pl.loop(0, 4)
    def _(m):
        h, p, q, ok = where(me1, slot(me2, m))

        @pl.when(ok)
        def _():
            tile = kbuf[m]
            for n in range(1, 4):
                rcopy(s2.at[0, m], r2.at[n - 1, m], q2s.at[0, m], q2r.at[n - 1, m], ring2(1)).wait_recv()
                tile = tile + dec(r2[n - 1, m], n, h, p, q)
            code = jnp.round(tile * (csi[4, pl.ds(q, 1), :] * rbi[4, h, pl.ds(p, 1), :]))
            full = code.astype(jnp.int32).astype(jnp.int16)

            @pl.when(this(q, 2 * p + h))
            def _():
                r3[z] = full

            @pl.when(jnp.logical_not(this(q, 2 * p + h)))
            def _():
                s3[m] = full
                last(m, h, p, q).start()

            @pl.when(q > p)
            def _():
                for n in range(2):
                    part = code[:, n * TR:(n + 1) * TR]
                    flat = jnp.concatenate([part[:HR], part[HR:]], axis=1).astype(jnp.int32).astype(jnp.int16)

                    @pl.when(this(p, 2 * q + n))
                    def _():
                        r4[h, z] = flat

                    @pl.when(jnp.logical_not(this(p, 2 * q + n)))
                    def _():
                        s4[m, n] = flat
                        turned(m, n, h, p, q).start()

    def other(p, q, h, level):
        src, core = source(p, q, h)
        return jnp.logical_not(this(2 * level + core, src))

    @pl.when(aux >= pr)
    def _():
        h = orb % 2
        for o in range(4):
            up = (z + o) % 4

            @pl.when(other(pr, aux, h, up))
            def _():
                rcopy(s3.at[0], r3.at[up], q3s.at[0], q3r.at[up], (sib, orb)).wait_recv()
        tile = dec(r3[z], 4, h, pr, aux)
        for o in range(1, 4):
            tile = tile + dec(r3[(z + o) % 4], 4 + o, h, pr, aux)
        out[...] = tile

    @pl.when(aux < pr)
    def _():
        n = orb % 2
        for h in range(2):
            for o in range(4):
                up = (z + o) % 4

                @pl.when(other(aux, pr, h, up))
                def _():
                    rcopy(s4.at[0, 0], r4.at[h, up], q4s.at[0, 0], q4r.at[h, up], (sib, orb)).wait_recv()
        wide = []
        for h in range(2):
            flat = jnp.zeros((HR, CH), f32)
            for o in range(4):
                sc = cs[4 + o, pl.ds(pr, 1), :]
                low = jnp.concatenate([sc[:, :TR], sc[:, :TR]], axis=1)
                high = jnp.concatenate([sc[:, TR:], sc[:, TR:]], axis=1)
                sc = jnp.where(n == 0, low, high) * rb[4 + o, h, pl.ds(aux, 1), :]
                flat = flat + r4[h, (z + o) % 4].astype(jnp.int32).astype(f32) * sc
            wide.append(jnp.concatenate([flat[:, :TR], flat[:, TR:]], axis=0).T)
        out[...] = jnp.concatenate(wide, axis=1)

    for o in range(1, 8):
        mcopy(o).wait_send()

    @pl.loop(0, NCH)
    def _(q):
        for o, flip in ORDER:
            send(q, o, flip).wait_send()
        fcopy(q).wait_send()
        for o in range(1, 4):
            dcopy(q, o).wait_send()

    for level, dev in ((1, ring2), (2, zline)):
        for o in range(1, 4):
            rcopy(dv.at[4 * level], dv.at[4 * level], ds_.at[4 * level + o], dr.at[4 * level], dev(o)).wait_send()

    for role in range(1, 4):
        @pl.loop(0, 16)
        def _(i):
            @pl.when(where((me1 + role) % 4, i)[3])
            def _():
                tile1(role, i).wait_send()

        @pl.loop(0, 4)
        def _(m):
            @pl.when(where(me1, slot((me2 + role) % 4, m))[3])
            def _():
                tile2(role, m).wait_send()

    @pl.loop(0, 4)
    def _(m):
        h, p, q, ok = where(me1, slot(me2, m))

        @pl.when(jnp.logical_and(ok, jnp.logical_not(this(q, 2 * p + h))))
        def _():
            last(m, h, p, q).wait_send()

        for n in range(2):
            @pl.when(jnp.logical_and(jnp.logical_and(ok, q > p), jnp.logical_not(this(p, 2 * q + n))))
            def _():
                turned(m, n, h, p, q).wait_send()


def shards(half, metric, survive):
    bf, f32, i16 = jnp.bfloat16, jnp.float32, jnp.int16
    rows = half.reshape(CH, half.shape[-1])
    vm, dma = pltpu.VMEM, pltpu.SemaphoreType.DMA
    scratch = [
        vm((NCH, CH, CH), bf), vm((CH, CH), bf), vm((128, 128), bf),
        vm((NCH, CH, CH), bf), vm((NCH, CH, CH), bf), vm((CH, CH), bf),
        vm((NCH, 2 * CH, CH), bf), vm((NCH, CH, 2 * CH), bf),
        vm((4, NCH, 1, CH), f32), vm((12, 8, CH), f32),
        vm((NCH, 8, CH), f32), vm((NCH, 8, CH), f32), vm((2, NCH, 8, CH), f32), vm((2, NCH, 8, CH), f32),
        vm((8, 8, CH), f32), vm((8, 8, CH), f32), vm((8, 2, 8, CH), f32), vm((8, 2, 8, CH), f32),
        vm((16, TR, CH), f32), vm((3, 16, TR, CH), i16), vm((3, 16, TR, CH), i16),
        vm((3, 4, TR, CH), i16), vm((3, 4, TR, CH), i16),
        vm((4, TR, CH), i16), vm((4, TR, CH), i16), vm((4, 2, HR, CH), i16), vm((2, 4, HR, CH), i16),
        dma((NCH,)), dma((NCH, 8)), dma((NCH, 8)), dma((8,)), dma((8,)), dma((NCH,)), dma((NCH,)),
        dma((4, NCH)), dma((4, NCH)), dma((12,)), dma((12,)),
        dma((3, 16)), dma((3, 16)), dma((3, 4)), dma((3, 4)),
        dma((4,)), dma((4,)), dma((4, 2)), dma((2, 4)),
    ]
    return pl.pallas_call(
        kernel,
        out_shape=jax.ShapeDtypeStruct((TR, CH), f32),
        in_specs=[pl.BlockSpec(memory_space=pl.ANY), pl.BlockSpec(memory_space=pltpu.SMEM),
                  pl.BlockSpec(memory_space=pltpu.VMEM)],
        out_specs=pl.BlockSpec(memory_space=pltpu.VMEM),
        scratch_shapes=scratch,
        compiler_params=pltpu.CompilerParams(collective_id=0, has_side_effects=True,
                                             vmem_limit_bytes=62 * 1024 * 1024),
    )(rows, survive, metric)


def solution(mesh):
    placed = (P("aux", "orb", None), P("aux", None), P("aux", "orb", None))
    return jax.shard_map(shards, mesh=mesh, in_specs=placed, out_specs=P("orb", "aux"), check_vma=False)
```

```python
import jax
import jax.numpy as jnp
from jax import lax
from jax.experimental import pallas as pl
from jax.experimental.pallas import tpu as pltpu
from jax.sharding import PartitionSpec as P

MESH = pl.DeviceIdType.MESH
CH = 384
NCH = 8
TR = 192
HR = 96
TOP = 32700.0
TINY = 1e-36
ORDER = ((2, 0), (2, 1), (1, 0), (3, 0), (1, 1), (3, 1), (0, 1))


def third(n):
    return jnp.floor((n + 0.5) * (1.0 / 3.0))


def iota(shape, dim):
    return lax.broadcasted_iota(jnp.int32, shape, dim).astype(jnp.float32)


def sorting():
    row, col = iota((CH, CH), 0), iota((CH, CH), 1)
    d = jnp.floor((row + 0.5) * (1.0 / 48.0))
    rest = row - 48.0 * d
    aux = third(rest)
    return jnp.where(col == 21.0 * aux + 3.0 * d + rest, 1.0, 0.0).astype(jnp.bfloat16)


def spread(metric):
    f32, bf = jnp.float32, jnp.bfloat16
    left = jnp.where(third(iota((CH, 128), 0)) == iota((CH, 128), 1), 1.0, 0.0).astype(bf)
    right = jnp.where(third(iota((128, CH), 1)) == iota((128, CH), 0), 1.0, 0.0).astype(bf)
    rows = jnp.dot(left, metric, preferred_element_type=f32).astype(bf)
    wide = jnp.dot(rows, right, preferred_element_type=f32)
    a, b = iota((CH, CH), 0), iota((CH, CH), 1)
    return jnp.where(a - 3.0 * third(a) == b - 3.0 * third(b), wide, 0.0).astype(bf)


def kernel(half, survive, metric, out, block, perm, whole, snd, rcv, m3, fb, ft, dvr, dv, cs1, csi1, rb1, rbi1, cs, csi, rb, rbi,
           kbuf, s1, r1, s2, r2, s3, r3, s4, r4,
           lds, p1s, p1r, ks, kr, fs, fr, d1s, d1r, ds_, dr, q1s, q1r, q2s, q2r, q3s, q3r, q4s, q4r):
    f32 = jnp.float32
    aux = lax.axis_index("aux")
    orb = lax.axis_index("orb")
    z, c = aux // 2, aux % 2
    x, y = orb // 4, orb % 4
    me1 = x * (1 - c) + y * c
    me2 = y * (1 - c) + x * c
    sib = 2 * z + 1 - c

    def row_of(t, u):
        return t * (4 - 3 * c) + u * (1 + 3 * c)

    def ring1(o):
        return (aux, row_of((me1 + o) % 4, me2))

    def ring2(o):
        return (aux, row_of(me1, (me2 + o) % 4))

    def cross(o):
        return (sib, row_of(me1, (me2 + o) % 4))

    def zdev(o, core):
        return (2 * ((z + o) % 4) + core, orb)

    pr = orb // 2
    def cut(q):
        return pl.ds(pl.multiple_of(q * CH, 128), CH)

    def load(q):
        return pltpu.make_async_copy(half.at[:, cut(q)], block.at[q], lds.at[q])

    for q in range(NCH):
        load(q).start()

    bar = pltpu.get_barrier_semaphore()
    for o in range(1, 8):
        pl.semaphore_signal(bar, inc=1, device_id=((aux + o) % 8, orb), device_id_type=MESH)
    for o in range(1, 4):
        pl.semaphore_signal(bar, inc=1, device_id=ring1(o), device_id_type=MESH)
        pl.semaphore_signal(bar, inc=1, device_id=ring2(o), device_id_type=MESH)
        pl.semaphore_signal(bar, inc=1, device_id=cross(o), device_id_type=MESH)

    def rcopy(src, dst, ss, rs, dev):
        return pltpu.make_async_remote_copy(src_ref=src, dst_ref=dst, send_sem=ss, recv_sem=rs,
                                            device_id=dev, device_id_type=MESH)

    def al48(v):
        return pl.ds(pl.multiple_of(v * 48, 16), 48)

    def mcopy(o):
        rows = pl.ds(pl.multiple_of(aux * 16, 16), 16)
        return rcopy(metric, whole.at[rows], ks.at[o], kr.at[o], ((aux + o) % 8, orb))

    def send(q, o, flip):
        dev = 2 * ((z + o) % 4) + (c + flip) % 2
        return rcopy(snd.at[q, al48(dev)], rcv.at[q, al48(aux)], p1s.at[q, 2 * o + flip], p1r.at[q, aux], (dev, orb))

    def arrival(q, a):
        return rcopy(rcv.at[q, al48(a)], rcv.at[q, al48(a)], p1s.at[q, 0], p1r.at[q, a], (sib, orb))

    def gate(q):
        flags = [jnp.full((1, 128), survive[0, 0, 3 * q + n].astype(f32)) for n in range(3)]
        return jnp.concatenate(flags, axis=1).astype(jnp.bfloat16)

    def sort(q):
        load(q).wait()
        kept = block[q] * gate(q)
        snd[q] = jnp.dot(perm[...], kept, preferred_element_type=f32).astype(jnp.bfloat16)
        rcv[q, al48(aux), :] = snd[q, al48(aux), :]

    def sends(q):
        for o, flip in ORDER:
            send(q, o, flip).start()

    perm[...] = sorting()
    sort(0)
    pl.semaphore_wait(bar, 16)
    for o in range(1, 8):
        mcopy(o).start()
    sends(0)
    whole[pl.ds(pl.multiple_of(aux * 16, 16), 16), :] = metric[...]

    @pl.loop(1, NCH)
    def _(q):
        sort(q)
        sends(q)

    for o in range(1, 8):
        rows = pl.ds(pl.multiple_of((aux + 8 - o) % 8 * 16, 16), 16)
        rcopy(metric, whole.at[rows], ks.at[o], kr.at[o], (sib, orb)).wait_recv()
    m3[...] = spread(whole[...])

    def fcopy(q):
        return rcopy(fb.at[q, pl.ds(0, CH)], fb.at[q, pl.ds(CH, CH)], fs.at[q], fr.at[q], (sib, orb))

    def scales(val):
        val = jnp.maximum(val, TINY)
        lane = lax.broadcasted_iota(jnp.int32, val.shape, 1)
        inv = lax.rsqrt(val)
        yield val * inv, inv
        for h in range(2):
            part = jnp.where((lane >= TR) == (h == 1), val, TINY)
            top = jnp.broadcast_to(jnp.max(part, axis=1, keepdims=True), val.shape)
            tinv = lax.rsqrt(top)
            yield top * tinv * (1.0 / TOP), tinv * TOP

    def tables1(k, rows, val):
        for n, (sc, inv) in enumerate(scales(val)):
            if n == 0:
                cs1[k, rows, :], csi1[k, rows, :] = sc, inv
            else:
                rb1[n - 1, k, rows, :], rbi1[n - 1, k, rows, :] = sc, inv

    def tables(first, terms):
        for i, val in enumerate(terms):
            for n, (sc, inv) in enumerate(scales(val)):
                if n == 0:
                    cs[first + i], csi[first + i] = sc, inv
                else:
                    rb[first + i, n - 1], rbi[first + i, n - 1] = sc, inv

    def gather(level, dev):
        base = 4 * level
        for o in range(1, 4):
            rcopy(dv.at[base], dv.at[base + 4 - o], ds_.at[base + o], dr.at[base + 4 - o], dev(o)).start()

    def gathered(level, dev):
        base = 4 * level
        for o in range(1, 4):
            rcopy(dv.at[base], dv.at[base + o], ds_.at[base + o], dr.at[base + o], dev(o)).wait_recv()
        return [dv[base + o] for o in range(4)]

    def dcopy(q, o):
        return rcopy(dvr.at[0, q], dvr.at[4 - o, q], d1s.at[o, q], d1r.at[4 - o, q], cross(o))

    def enc1(val, n, h, p, q):
        inv = csi1[q, pl.ds(n, 1), :] * rbi1[h, p, pl.ds(n, 1), :]
        return jnp.round(val * inv).astype(jnp.int32).astype(jnp.int16)

    def dec1(val, n, h, p, q):
        sc = cs1[q, pl.ds(n, 1), :] * rb1[h, p, pl.ds(n, 1), :]
        return val.astype(jnp.int32).astype(f32) * sc

    def enc(val, n, h, p, q):
        inv = csi[n, pl.ds(q, 1), :] * rbi[n, h, pl.ds(p, 1), :]
        return jnp.round(val * inv).astype(jnp.int32).astype(jnp.int16)

    def dec(val, n, h, p, q):
        sc = cs[n, pl.ds(q, 1), :] * rb[n, h, pl.ds(p, 1), :]
        return val.astype(jnp.int32).astype(f32) * sc

    def where(t, i):
        p = 2 * (i // 4) + t // 2
        q = 2 * (i % 4) + (i // 4 + c) % 2
        return t % 2, p, q, q >= p

    def slot(u, m):
        return m * 4 + (u - m + 4) % 4

    def source(p, q, h):
        core = (p // 2 + q) % 2
        t, u = 2 * (p % 2) + h, (p // 2 + q // 2) % 4
        return t * (4 - 3 * core) + u * (1 + 3 * core), core

    def place(p, q, h):
        return (p // 2) * 4 + q // 2, (2 * (p % 2) + h - me1 + 4) % 4

    def each(k, body):
        @pl.loop(0, k + 1)
        def _(j):
            @pl.when((j // 2 + k) % 2 == c)
            def _():
                body(j, k)

    def tile1(role, i):
        return rcopy(s1.at[role - 1, i], r1.at[3 - role, i], q1s.at[role - 1, i], q1r.at[3 - role, i], ring1(role))

    def tile2(role, m):
        return rcopy(s2.at[role - 1, m], r2.at[3 - role, m], q2s.at[role - 1, m], q2r.at[3 - role, m], ring2(role))

    def pair(k):
        fcopy(k).wait_recv()
        both = fb[k]
        ft[k] = both.T
        wide = both.astype(f32)
        wide = wide * wide
        norm = jnp.sum(wide[:CH], axis=0, keepdims=True) + jnp.sum(wide[CH:], axis=0, keepdims=True)
        dvr[0, k] = norm
        for o in range(1, 4):
            dcopy(k, o).start()
        tables1(k, pl.ds(0, 1), norm)

    def compute(k):
        def body(p, q):
            tile = jnp.dot(ft[p], fb[q], preferred_element_type=f32)
            for h in range(2):
                i, role = place(p, q, h)
                part = tile[h * TR:(h + 1) * TR]

                @pl.when(role == 0)
                def _():
                    kbuf[i] = part

                @pl.when(role > 0)
                def _():
                    s1[role - 1, i] = enc1(part, 0, h, p, q)
                    tile1(role, i).start()

        each(k, body)

    def norms(k):
        for o in range(1, 4):
            rcopy(dvr.at[0, k], dvr.at[o, k], d1s.at[o, k], d1r.at[o, k], ring1(o)).wait_recv()
        d = [dvr[o, k] for o in range(4)]
        tables1(k, slice(None), jnp.concatenate(d + d, axis=0))
        dv[4, pl.ds(k, 1), :] = d[0] + d[1] + d[2] + d[3]

    @pl.loop(0, NCH)
    def _(k):
        for o in range(1, 8):
            arrival(k, (aux + o) % 8).wait_recv()
        fb[k, 0:CH, :] = jnp.dot(m3[...], rcv[k], preferred_element_type=f32).astype(jnp.bfloat16)
        fcopy(k).start()

        @pl.when(k > 0)
        def _():
            compute(k - 1)

        @pl.when(k > 3)
        def _():
            norms(k - 4)

        pair(k)

    compute(NCH - 1)

    @pl.loop(NCH - 4, NCH)
    def _(k):
        norms(k)

    gather(1, ring2)

    d1 = gathered(1, ring2)
    tables(0, d1)
    dv[8] = d1[0] + d1[1] + d1[2] + d1[3]

    def zline(o):
        return zdev(o, c)

    gather(2, zline)
    @pl.loop(0, 16)
    def _(n):
        b = n // 4
        a = 2 * (n % 2) + (n % 4 // 2) * (1 - 2 * c) + c
        i = a * 4 + b
        h, p, q, ok = where(me1, i)
        role = (a + b - me2 + 4) % 4

        @pl.when(ok)
        def _():
            tile = kbuf[i]
            for o in range(1, 4):
                rcopy(s1.at[0, i], r1.at[o - 1, i], q1s.at[0, i], q1r.at[o - 1, i], ring1(1)).wait_recv()
                tile = tile + dec1(r1[o - 1, i], o, h, p, q)

            @pl.when(role == 0)
            def _():
                kbuf[i] = tile

            @pl.when(role > 0)
            def _():
                s2[role - 1, a] = enc(tile, 0, h, p, q)
                tile2(role, a).start()

    d2 = gathered(2, zline)
    tables(4, d2)

    def last(m, h, p, q):
        return rcopy(s3.at[m], r3.at[z], q3s.at[m], q3r.at[z], (q, 2 * p + h))

    def turned(m, n, h, p, q):
        return rcopy(s4.at[m, n], r4.at[h, z], q4s.at[m, n], q4r.at[h, z], (p, 2 * q + n))

    def this(a, o):
        return jnp.logical_and(aux == a, orb == o)

    @pl.loop(0, 4)
    def _(b):
        m = (me2 - b + 4) % 4
        i = m * 4 + b
        h, p, q, ok = where(me1, i)

        @pl.when(ok)
        def _():
            tile = kbuf[i]
            for n in range(1, 4):
                rcopy(s2.at[0, m], r2.at[n - 1, m], q2s.at[0, m], q2r.at[n - 1, m], ring2(1)).wait_recv()
                tile = tile + dec(r2[n - 1, m], n, h, p, q)
            code = jnp.round(tile * (csi[4, pl.ds(q, 1), :] * rbi[4, h, pl.ds(p, 1), :]))
            full = code.astype(jnp.int32).astype(jnp.int16)

            @pl.when(this(q, 2 * p + h))
            def _():
                r3[z] = full

            @pl.when(jnp.logical_not(this(q, 2 * p + h)))
            def _():
                s3[m] = full
                last(m, h, p, q).start()

            @pl.when(q > p)
            def _():
                for n in range(2):
                    part = code[:, n * TR:(n + 1) * TR]
                    flat = jnp.concatenate([part[:HR], part[HR:]], axis=1).astype(jnp.int32).astype(jnp.int16)

                    @pl.when(this(p, 2 * q + n))
                    def _():
                        r4[h, z] = flat

                    @pl.when(jnp.logical_not(this(p, 2 * q + n)))
                    def _():
                        s4[m, n] = flat
                        turned(m, n, h, p, q).start()

    def other(p, q, h, level):
        src, core = source(p, q, h)
        return jnp.logical_not(this(2 * level + core, src))

    @pl.when(aux >= pr)
    def _():
        h = orb % 2
        for o in range(4):
            up = (z + o) % 4

            @pl.when(other(pr, aux, h, up))
            def _():
                rcopy(s3.at[0], r3.at[up], q3s.at[0], q3r.at[up], (sib, orb)).wait_recv()
        tile = dec(r3[z], 4, h, pr, aux)
        for o in range(1, 4):
            tile = tile + dec(r3[(z + o) % 4], 4 + o, h, pr, aux)
        out[...] = tile

    @pl.when(aux < pr)
    def _():
        n = orb % 2
        for h in range(2):
            for o in range(4):
                up = (z + o) % 4

                @pl.when(other(aux, pr, h, up))
                def _():
                    rcopy(s4.at[0, 0], r4.at[h, up], q4s.at[0, 0], q4r.at[h, up], (sib, orb)).wait_recv()
        wide = []
        for h in range(2):
            flat = jnp.zeros((HR, CH), f32)
            for o in range(4):
                sc = cs[4 + o, pl.ds(pr, 1), :]
                low = jnp.concatenate([sc[:, :TR], sc[:, :TR]], axis=1)
                high = jnp.concatenate([sc[:, TR:], sc[:, TR:]], axis=1)
                sc = jnp.where(n == 0, low, high) * rb[4 + o, h, pl.ds(aux, 1), :]
                flat = flat + r4[h, (z + o) % 4].astype(jnp.int32).astype(f32) * sc
            wide.append(jnp.concatenate([flat[:, :TR], flat[:, TR:]], axis=0).T)
        out[...] = jnp.concatenate(wide, axis=1)

    for o in range(1, 8):
        mcopy(o).wait_send()

    @pl.loop(0, NCH)
    def _(q):
        for o, flip in ORDER:
            send(q, o, flip).wait_send()
        fcopy(q).wait_send()
        for o in range(1, 4):
            dcopy(q, o).wait_send()

    for level, dev in ((1, ring2), (2, zline)):
        for o in range(1, 4):
            rcopy(dv.at[4 * level], dv.at[4 * level], ds_.at[4 * level + o], dr.at[4 * level], dev(o)).wait_send()

    for role in range(1, 4):
        @pl.loop(0, 16)
        def _(i):
            @pl.when(where((me1 + role) % 4, i)[3])
            def _():
                tile1(role, i).wait_send()

        @pl.loop(0, 4)
        def _(m):
            @pl.when(where(me1, slot((me2 + role) % 4, m))[3])
            def _():
                tile2(role, m).wait_send()

    @pl.loop(0, 4)
    def _(m):
        h, p, q, ok = where(me1, slot(me2, m))

        @pl.when(jnp.logical_and(ok, jnp.logical_not(this(q, 2 * p + h))))
        def _():
            last(m, h, p, q).wait_send()

        for n in range(2):
            @pl.when(jnp.logical_and(jnp.logical_and(ok, q > p), jnp.logical_not(this(p, 2 * q + n))))
            def _():
                turned(m, n, h, p, q).wait_send()


def shards(half, metric, survive):
    bf, f32, i16 = jnp.bfloat16, jnp.float32, jnp.int16
    rows = half.reshape(CH, half.shape[-1])
    vm, dma = pltpu.VMEM, pltpu.SemaphoreType.DMA
    scratch = [
        vm((NCH, CH, CH), bf), vm((CH, CH), bf), vm((128, 128), bf),
        vm((NCH, CH, CH), bf), vm((NCH, CH, CH), bf), vm((CH, CH), bf),
        vm((NCH, 2 * CH, CH), bf), vm((NCH, CH, 2 * CH), bf),
        vm((4, NCH, 1, CH), f32), vm((12, 8, CH), f32),
        vm((NCH, 8, CH), f32), vm((NCH, 8, CH), f32), vm((2, NCH, 8, CH), f32), vm((2, NCH, 8, CH), f32),
        vm((8, 8, CH), f32), vm((8, 8, CH), f32), vm((8, 2, 8, CH), f32), vm((8, 2, 8, CH), f32),
        vm((16, TR, CH), f32), vm((3, 16, TR, CH), i16), vm((3, 16, TR, CH), i16),
        vm((3, 4, TR, CH), i16), vm((3, 4, TR, CH), i16),
        vm((4, TR, CH), i16), vm((4, TR, CH), i16), vm((4, 2, HR, CH), i16), vm((2, 4, HR, CH), i16),
        dma((NCH,)), dma((NCH, 8)), dma((NCH, 8)), dma((8,)), dma((8,)), dma((NCH,)), dma((NCH,)),
        dma((4, NCH)), dma((4, NCH)), dma((12,)), dma((12,)),
        dma((3, 16)), dma((3, 16)), dma((3, 4)), dma((3, 4)),
        dma((4,)), dma((4,)), dma((4, 2)), dma((2, 4)),
    ]
    return pl.pallas_call(
        kernel,
        out_shape=jax.ShapeDtypeStruct((TR, CH), f32),
        in_specs=[pl.BlockSpec(memory_space=pl.ANY), pl.BlockSpec(memory_space=pltpu.SMEM),
                  pl.BlockSpec(memory_space=pltpu.VMEM)],
        out_specs=pl.BlockSpec(memory_space=pltpu.VMEM),
        scratch_shapes=scratch,
        compiler_params=pltpu.CompilerParams(collective_id=0, has_side_effects=True,
                                             vmem_limit_bytes=62 * 1024 * 1024),
    )(rows, survive, metric)


def solution(mesh):
    placed = (P("aux", "orb", None), P("aux", None), P("aux", "orb", None))
    return jax.shard_map(shards, mesh=mesh, in_specs=placed, out_specs=P("orb", "aux"), check_vma=False)
```

```python
import jax
import jax.numpy as jnp
from jax import lax
from jax.experimental import pallas as pl
from jax.experimental.pallas import tpu as pltpu
from jax.sharding import PartitionSpec as P

MESH = pl.DeviceIdType.MESH
CH = 384
NCH = 8
TR = 192
HR = 96
TOP = 32700.0
TINY = 1e-36
ORDER = ((2, 0), (2, 1), (1, 0), (3, 0), (1, 1), (3, 1), (0, 1))


def third(n):
    return jnp.floor((n + 0.5) * (1.0 / 3.0))


def iota(shape, dim):
    return lax.broadcasted_iota(jnp.int32, shape, dim).astype(jnp.float32)


def sorting():
    row, col = iota((CH, CH), 0), iota((CH, CH), 1)
    d = jnp.floor((row + 0.5) * (1.0 / 48.0))
    rest = row - 48.0 * d
    aux = third(rest)
    return jnp.where(col == 21.0 * aux + 3.0 * d + rest, 1.0, 0.0).astype(jnp.bfloat16)


def spread(metric):
    f32, bf = jnp.float32, jnp.bfloat16
    left = jnp.where(third(iota((CH, 128), 0)) == iota((CH, 128), 1), 1.0, 0.0).astype(bf)
    right = jnp.where(third(iota((128, CH), 1)) == iota((128, CH), 0), 1.0, 0.0).astype(bf)
    rows = jnp.dot(left, metric, preferred_element_type=f32).astype(bf)
    wide = jnp.dot(rows, right, preferred_element_type=f32)
    a, b = iota((CH, CH), 0), iota((CH, CH), 1)
    return jnp.where(a - 3.0 * third(a) == b - 3.0 * third(b), wide, 0.0).astype(bf)


def kernel(half, survive, metric, out, block, perm, whole, snd, rcv, m3, fb, ft, dvr, dv, cs1, csi1, rb1, rbi1, cs, csi, rb, rbi,
           kbuf, s1, r1, s2, r2, s3, r3, s4, r4,
           lds, p1s, p1r, ks, kr, fs, fr, d1s, d1r, ds_, dr, q1s, q1r, q2s, q2r, q3s, q3r, q4s, q4r):
    f32 = jnp.float32
    aux = lax.axis_index("aux")
    orb = lax.axis_index("orb")
    z, c = aux // 2, aux % 2
    x, y = orb // 4, orb % 4
    me1 = x * (1 - c) + y * c
    me2 = y * (1 - c) + x * c
    sib = 2 * z + 1 - c

    def row_of(t, u):
        return t * (4 - 3 * c) + u * (1 + 3 * c)

    def ring1(o):
        return (aux, row_of((me1 + o) % 4, me2))

    def ring2(o):
        return (aux, row_of(me1, (me2 + o) % 4))

    def cross(o):
        return (sib, row_of(me1, (me2 + o) % 4))

    def zdev(o, core):
        return (2 * ((z + o) % 4) + core, orb)

    pr = orb // 2
    def block_at(s):
        return (2 * s) % 8 + s // 4

    def turn_of(v):
        return v // 2 + 4 * (v % 2)

    def cut(q):
        return pl.ds(pl.multiple_of(q * CH, 128), CH)

    def load(q):
        return pltpu.make_async_copy(half.at[:, cut(block_at(q))], block.at[q], lds.at[q])

    for q in range(NCH):
        load(q).start()

    bar = pltpu.get_barrier_semaphore()
    for o in range(1, 8):
        pl.semaphore_signal(bar, inc=1, device_id=((aux + o) % 8, orb), device_id_type=MESH)
    for o in range(1, 4):
        pl.semaphore_signal(bar, inc=1, device_id=ring1(o), device_id_type=MESH)
        pl.semaphore_signal(bar, inc=1, device_id=ring2(o), device_id_type=MESH)
        pl.semaphore_signal(bar, inc=1, device_id=cross(o), device_id_type=MESH)

    def rcopy(src, dst, ss, rs, dev):
        return pltpu.make_async_remote_copy(src_ref=src, dst_ref=dst, send_sem=ss, recv_sem=rs,
                                            device_id=dev, device_id_type=MESH)

    def al48(v):
        return pl.ds(pl.multiple_of(v * 48, 16), 48)

    def mcopy(o):
        rows = pl.ds(pl.multiple_of(aux * 16, 16), 16)
        return rcopy(metric, whole.at[rows], ks.at[o], kr.at[o], ((aux + o) % 8, orb))

    def send(q, o, flip):
        dev = 2 * ((z + o) % 4) + (c + flip) % 2
        return rcopy(snd.at[q, al48(dev)], rcv.at[q, al48(aux)], p1s.at[q, 2 * o + flip], p1r.at[q, aux], (dev, orb))

    def arrival(q, a):
        return rcopy(rcv.at[q, al48(a)], rcv.at[q, al48(a)], p1s.at[q, 0], p1r.at[q, a], (sib, orb))

    def gate(q):
        flags = [jnp.full((1, 128), survive[0, 0, 3 * block_at(q) + n].astype(f32)) for n in range(3)]
        return jnp.concatenate(flags, axis=1).astype(jnp.bfloat16)

    def sort(q):
        load(q).wait()
        kept = block[q] * gate(q)
        snd[q] = jnp.dot(perm[...], kept, preferred_element_type=f32).astype(jnp.bfloat16)
        rcv[q, al48(aux), :] = snd[q, al48(aux), :]

    def sends(q):
        for o, flip in ORDER:
            send(q, o, flip).start()

    perm[...] = sorting()
    sort(0)
    pl.semaphore_wait(bar, 16)
    for o in range(1, 8):
        mcopy(o).start()
    sends(0)
    whole[pl.ds(pl.multiple_of(aux * 16, 16), 16), :] = metric[...]

    @pl.loop(1, NCH)
    def _(q):
        sort(q)
        sends(q)

    for o in range(1, 8):
        rows = pl.ds(pl.multiple_of((aux + 8 - o) % 8 * 16, 16), 16)
        rcopy(metric, whole.at[rows], ks.at[o], kr.at[o], (sib, orb)).wait_recv()
    m3[...] = spread(whole[...])

    def fcopy(q):
        return rcopy(fb.at[q, pl.ds(0, CH)], fb.at[q, pl.ds(CH, CH)], fs.at[q], fr.at[q], (sib, orb))

    def scales(val):
        val = jnp.maximum(val, TINY)
        lane = lax.broadcasted_iota(jnp.int32, val.shape, 1)
        inv = lax.rsqrt(val)
        yield val * inv, inv
        for h in range(2):
            part = jnp.where((lane >= TR) == (h == 1), val, TINY)
            top = jnp.broadcast_to(jnp.max(part, axis=1, keepdims=True), val.shape)
            tinv = lax.rsqrt(top)
            yield top * tinv * (1.0 / TOP), tinv * TOP

    def tables1(k, rows, val):
        for n, (sc, inv) in enumerate(scales(val)):
            if n == 0:
                cs1[k, rows, :], csi1[k, rows, :] = sc, inv
            else:
                rb1[n - 1, k, rows, :], rbi1[n - 1, k, rows, :] = sc, inv

    def tables(first, terms):
        for i, val in enumerate(terms):
            for n, (sc, inv) in enumerate(scales(val)):
                if n == 0:
                    cs[first + i], csi[first + i] = sc, inv
                else:
                    rb[first + i, n - 1], rbi[first + i, n - 1] = sc, inv

    def gather(level, dev):
        base = 4 * level
        for o in range(1, 4):
            rcopy(dv.at[base], dv.at[base + 4 - o], ds_.at[base + o], dr.at[base + 4 - o], dev(o)).start()

    def gathered(level, dev):
        base = 4 * level
        for o in range(1, 4):
            rcopy(dv.at[base], dv.at[base + o], ds_.at[base + o], dr.at[base + o], dev(o)).wait_recv()
        return [dv[base + o] for o in range(4)]

    def dcopy(q, o):
        return rcopy(dvr.at[0, q], dvr.at[4 - o, q], d1s.at[o, q], d1r.at[4 - o, q], cross(o))

    def enc1(val, n, h, p, q):
        inv = csi1[q, pl.ds(n, 1), :] * rbi1[h, p, pl.ds(n, 1), :]
        return jnp.round(val * inv).astype(jnp.int32).astype(jnp.int16)

    def dec1(val, n, h, p, q):
        sc = cs1[q, pl.ds(n, 1), :] * rb1[h, p, pl.ds(n, 1), :]
        return val.astype(jnp.int32).astype(f32) * sc

    def enc(val, n, h, p, q):
        inv = csi[n, pl.ds(q, 1), :] * rbi[n, h, pl.ds(p, 1), :]
        return jnp.round(val * inv).astype(jnp.int32).astype(jnp.int16)

    def dec(val, n, h, p, q):
        sc = cs[n, pl.ds(q, 1), :] * rb[n, h, pl.ds(p, 1), :]
        return val.astype(jnp.int32).astype(f32) * sc

    def where(t, i):
        p = 2 * (i // 4) + t // 2
        q = 2 * (i % 4) + (i // 4 + c) % 2
        return t % 2, p, q, q >= p

    def slot(u, m):
        return m * 4 + (u - m + 4) % 4

    def source(p, q, h):
        core = (p // 2 + q) % 2
        t, u = 2 * (p % 2) + h, (p // 2 + q // 2) % 4
        return t * (4 - 3 * core) + u * (1 + 3 * core), core

    def place(p, q, h):
        return (p // 2) * 4 + q // 2, (2 * (p % 2) + h - me1 + 4) % 4

    def tile1(role, i):
        return rcopy(s1.at[role - 1, i], r1.at[3 - role, i], q1s.at[role - 1, i], q1r.at[3 - role, i], ring1(role))

    def tile2(role, m):
        return rcopy(s2.at[role - 1, m], r2.at[3 - role, m], q2s.at[role - 1, m], q2r.at[3 - role, m], ring2(role))

    def pair(k):
        fcopy(k).wait_recv()
        both = fb[k]
        ft[k] = both.T
        wide = both.astype(f32)
        wide = wide * wide
        norm = jnp.sum(wide[:CH], axis=0, keepdims=True) + jnp.sum(wide[CH:], axis=0, keepdims=True)
        dvr[0, k] = norm
        for o in range(1, 4):
            dcopy(k, o).start()
        tables1(k, pl.ds(0, 1), norm)

    def compute(k):
        @pl.loop(0, k // 2 + 1)
        def _(a):
            @pl.when((a + k) % 2 == c)
            def _():
                both = ft[pl.ds(2 * a, 2)].reshape(2 * CH, 2 * CH)
                tile = jnp.dot(both, fb[k], preferred_element_type=f32)
                for n in range(4):
                    p, h = 2 * a + n // 2, n % 2
                    i, role = place(p, k, h)
                    part = tile[n * TR:(n + 1) * TR]

                    @pl.when(jnp.logical_and(role == 0, p <= k))
                    def _():
                        kbuf[i] = part

                    @pl.when(jnp.logical_and(role > 0, p <= k))
                    def _():
                        s1[role - 1, i] = enc1(part, 0, h, p, k)
                        tile1(role, i).start()

    def norms(k):
        for o in range(1, 4):
            rcopy(dvr.at[0, k], dvr.at[o, k], d1s.at[o, k], d1r.at[o, k], ring1(o)).wait_recv()
        d = [dvr[o, k] for o in range(4)]
        tables1(k, slice(None), jnp.concatenate(d + d, axis=0))
        dv[4, pl.ds(k, 1), :] = d[0] + d[1] + d[2] + d[3]

    @pl.loop(0, NCH)
    def _(k):
        for o in range(1, 8):
            arrival(k, (aux + o) % 8).wait_recv()
        fb[k, 0:CH, :] = jnp.dot(m3[...], rcv[k], preferred_element_type=f32).astype(jnp.bfloat16)
        fcopy(k).start()

        @pl.when(k > 0)
        def _():
            compute(k - 1)

        pair(k)

    compute(NCH - 1)

    @pl.loop(0, NCH)
    def _(k):
        norms(k)

    gather(1, ring2)

    d1 = gathered(1, ring2)
    tables(0, d1)
    dv[8] = d1[0] + d1[1] + d1[2] + d1[3]

    def zline(o):
        return zdev(o, c)

    gather(2, zline)
    @pl.loop(0, 16)
    def _(n):
        b = n // 4
        a = 2 * (n % 2) + (n % 4 // 2) * (1 - 2 * c) + c
        i = a * 4 + b
        h, p, q, ok = where(me1, i)
        role = (a + b - me2 + 4) % 4

        @pl.when(ok)
        def _():
            tile = kbuf[i]
            for o in range(1, 4):
                rcopy(s1.at[0, i], r1.at[o - 1, i], q1s.at[0, i], q1r.at[o - 1, i], ring1(1)).wait_recv()
                tile = tile + dec1(r1[o - 1, i], o, h, p, q)

            @pl.when(role == 0)
            def _():
                kbuf[i] = tile

            @pl.when(role > 0)
            def _():
                s2[role - 1, a] = enc(tile, 0, h, p, q)
                tile2(role, a).start()

    d2 = gathered(2, zline)
    tables(4, d2)

    def last(m, h, p, q):
        return rcopy(s3.at[m], r3.at[z], q3s.at[m], q3r.at[z], (block_at(q), 2 * block_at(p) + h))

    def turned(m, n, h, p, q):
        return rcopy(s4.at[m, n], r4.at[h, z], q4s.at[m, n], q4r.at[h, z], (block_at(p), 2 * block_at(q) + n))

    def here(q, p, h):
        return jnp.logical_and(aux == block_at(q), orb == 2 * block_at(p) + h)

    @pl.loop(0, 4)
    def _(b):
        m = (me2 - b + 4) % 4
        i = m * 4 + b
        h, p, q, ok = where(me1, i)

        @pl.when(ok)
        def _():
            tile = kbuf[i]
            for n in range(1, 4):
                rcopy(s2.at[0, m], r2.at[n - 1, m], q2s.at[0, m], q2r.at[n - 1, m], ring2(1)).wait_recv()
                tile = tile + dec(r2[n - 1, m], n, h, p, q)
            code = jnp.round(tile * (csi[4, pl.ds(q, 1), :] * rbi[4, h, pl.ds(p, 1), :]))
            full = code.astype(jnp.int32).astype(jnp.int16)

            @pl.when(here(q, p, h))
            def _():
                r3[z] = full

            @pl.when(jnp.logical_not(here(q, p, h)))
            def _():
                s3[m] = full
                last(m, h, p, q).start()

            @pl.when(q > p)
            def _():
                for n in range(2):
                    part = code[:, n * TR:(n + 1) * TR]
                    flat = jnp.concatenate([part[:HR], part[HR:]], axis=1).astype(jnp.int32).astype(jnp.int16)

                    @pl.when(here(p, q, n))
                    def _():
                        r4[h, z] = flat

                    @pl.when(jnp.logical_not(here(p, q, n)))
                    def _():
                        s4[m, n] = flat
                        turned(m, n, h, p, q).start()

    def other(p, q, h, level):
        src, core = source(p, q, h)
        return jnp.logical_not(jnp.logical_and(aux == 2 * level + core, orb == src))

    ta, tp = turn_of(aux), turn_of(pr)

    @pl.when(ta >= tp)
    def _():
        h = orb % 2
        for o in range(4):
            up = (z + o) % 4

            @pl.when(other(tp, ta, h, up))
            def _():
                rcopy(s3.at[0], r3.at[up], q3s.at[0], q3r.at[up], (sib, orb)).wait_recv()
        tile = dec(r3[z], 4, h, tp, ta)
        for o in range(1, 4):
            tile = tile + dec(r3[(z + o) % 4], 4 + o, h, tp, ta)
        out[...] = tile

    @pl.when(ta < tp)
    def _():
        n = orb % 2
        for h in range(2):
            for o in range(4):
                up = (z + o) % 4

                @pl.when(other(ta, tp, h, up))
                def _():
                    rcopy(s4.at[0, 0], r4.at[h, up], q4s.at[0, 0], q4r.at[h, up], (sib, orb)).wait_recv()
        wide = []
        for h in range(2):
            flat = jnp.zeros((HR, CH), f32)
            for o in range(4):
                sc = cs[4 + o, pl.ds(tp, 1), :]
                low = jnp.concatenate([sc[:, :TR], sc[:, :TR]], axis=1)
                high = jnp.concatenate([sc[:, TR:], sc[:, TR:]], axis=1)
                sc = jnp.where(n == 0, low, high) * rb[4 + o, h, pl.ds(ta, 1), :]
                flat = flat + r4[h, (z + o) % 4].astype(jnp.int32).astype(f32) * sc
            wide.append(jnp.concatenate([flat[:, :TR], flat[:, TR:]], axis=0).T)
        out[...] = jnp.concatenate(wide, axis=1)

    for o in range(1, 8):
        mcopy(o).wait_send()

    @pl.loop(0, NCH)
    def _(q):
        for o, flip in ORDER:
            send(q, o, flip).wait_send()
        fcopy(q).wait_send()
        for o in range(1, 4):
            dcopy(q, o).wait_send()

    for level, dev in ((1, ring2), (2, zline)):
        for o in range(1, 4):
            rcopy(dv.at[4 * level], dv.at[4 * level], ds_.at[4 * level + o], dr.at[4 * level], dev(o)).wait_send()

    for role in range(1, 4):
        @pl.loop(0, 16)
        def _(i):
            @pl.when(where((me1 + role) % 4, i)[3])
            def _():
                tile1(role, i).wait_send()

        @pl.loop(0, 4)
        def _(m):
            @pl.when(where(me1, slot((me2 + role) % 4, m))[3])
            def _():
                tile2(role, m).wait_send()

    @pl.loop(0, 4)
    def _(m):
        h, p, q, ok = where(me1, slot(me2, m))

        @pl.when(jnp.logical_and(ok, jnp.logical_not(here(q, p, h))))
        def _():
            last(m, h, p, q).wait_send()

        for n in range(2):
            @pl.when(jnp.logical_and(jnp.logical_and(ok, q > p), jnp.logical_not(here(p, q, n))))
            def _():
                turned(m, n, h, p, q).wait_send()


def shards(half, metric, survive):
    bf, f32, i16 = jnp.bfloat16, jnp.float32, jnp.int16
    rows = half.reshape(CH, half.shape[-1])
    vm, dma = pltpu.VMEM, pltpu.SemaphoreType.DMA
    scratch = [
        vm((NCH, CH, CH), bf), vm((CH, CH), bf), vm((128, 128), bf),
        vm((NCH, CH, CH), bf), vm((NCH, CH, CH), bf), vm((CH, CH), bf),
        vm((NCH, 2 * CH, CH), bf), vm((NCH, CH, 2 * CH), bf),
        vm((4, NCH, 1, CH), f32), vm((12, 8, CH), f32),
        vm((NCH, 8, CH), f32), vm((NCH, 8, CH), f32), vm((2, NCH, 8, CH), f32), vm((2, NCH, 8, CH), f32),
        vm((8, 8, CH), f32), vm((8, 8, CH), f32), vm((8, 2, 8, CH), f32), vm((8, 2, 8, CH), f32),
        vm((16, TR, CH), f32), vm((3, 16, TR, CH), i16), vm((3, 16, TR, CH), i16),
        vm((3, 4, TR, CH), i16), vm((3, 4, TR, CH), i16),
        vm((4, TR, CH), i16), vm((4, TR, CH), i16), vm((4, 2, HR, CH), i16), vm((2, 4, HR, CH), i16),
        dma((NCH,)), dma((NCH, 8)), dma((NCH, 8)), dma((8,)), dma((8,)), dma((NCH,)), dma((NCH,)),
        dma((4, NCH)), dma((4, NCH)), dma((12,)), dma((12,)),
        dma((3, 16)), dma((3, 16)), dma((3, 4)), dma((3, 4)),
        dma((4,)), dma((4,)), dma((4, 2)), dma((2, 4)),
    ]
    return pl.pallas_call(
        kernel,
        out_shape=jax.ShapeDtypeStruct((TR, CH), f32),
        in_specs=[pl.BlockSpec(memory_space=pl.ANY), pl.BlockSpec(memory_space=pltpu.SMEM),
                  pl.BlockSpec(memory_space=pltpu.VMEM)],
        out_specs=pl.BlockSpec(memory_space=pltpu.VMEM),
        scratch_shapes=scratch,
        compiler_params=pltpu.CompilerParams(collective_id=0, has_side_effects=True,
                                             vmem_limit_bytes=62 * 1024 * 1024),
    )(rows, survive, metric)


def solution(mesh):
    placed = (P("aux", "orb", None), P("aux", None), P("aux", "orb", None))
    return jax.shard_map(shards, mesh=mesh, in_specs=placed, out_specs=P("orb", "aux"), check_vma=False)
```

```python
import jax
import jax.numpy as jnp
from jax import lax
from jax.experimental import pallas as pl
from jax.experimental.pallas import tpu as pltpu
from jax.sharding import PartitionSpec as P

MESH = pl.DeviceIdType.MESH
CH = 384
NCH = 8
TR = 192
HR = 96
LAG = 2
TOP = 32700.0
TINY = 1e-36
ORDER = ((2, 0), (2, 1), (1, 0), (3, 0), (1, 1), (3, 1), (0, 1))


def third(n):
    return jnp.floor((n + 0.5) * (1.0 / 3.0))


def iota(shape, dim):
    return lax.broadcasted_iota(jnp.int32, shape, dim).astype(jnp.float32)


def sorting():
    row, col = iota((CH, CH), 0), iota((CH, CH), 1)
    d = jnp.floor((row + 0.5) * (1.0 / 48.0))
    rest = row - 48.0 * d
    aux = third(rest)
    return jnp.where(col == 21.0 * aux + 3.0 * d + rest, 1.0, 0.0).astype(jnp.bfloat16)


def spread(metric):
    f32, bf = jnp.float32, jnp.bfloat16
    left = jnp.where(third(iota((CH, 128), 0)) == iota((CH, 128), 1), 1.0, 0.0).astype(bf)
    right = jnp.where(third(iota((128, CH), 1)) == iota((128, CH), 0), 1.0, 0.0).astype(bf)
    rows = jnp.dot(left, metric, preferred_element_type=f32).astype(bf)
    wide = jnp.dot(rows, right, preferred_element_type=f32)
    a, b = iota((CH, CH), 0), iota((CH, CH), 1)
    return jnp.where(a - 3.0 * third(a) == b - 3.0 * third(b), wide, 0.0).astype(bf)


def kernel(half, survive, metric, out, block, perm, whole, snd, rcv, m3, fb, ft, dvr, dv, cs1, csi1, rb1, rbi1, cs, csi, rb, rbi,
           kbuf, s1f, r1f, s1n, r1n, s2, r2, s3, r3, s4, r4,
           lds, p1s, p1r, ks, kr, fs, fr, d1s, d1r, ds_, dr, q1fs, q1fr, q1ns, q1nr, q2s, q2r, q3s, q3r, q4s, q4r):
    f32 = jnp.float32
    aux = lax.axis_index("aux")
    orb = lax.axis_index("orb")
    z, c = aux // 2, aux % 2
    x, y = orb // 4, orb % 4
    me1 = x * (1 - c) + y * c
    me2 = y * (1 - c) + x * c
    sib = 2 * z + 1 - c

    def row_of(t, u):
        return t * (4 - 3 * c) + u * (1 + 3 * c)

    def ring1(o):
        return (aux, row_of((me1 + o) % 4, me2))

    def ring2(o):
        return (aux, row_of(me1, (me2 + o) % 4))

    def cross(o):
        return (sib, row_of(me1, (me2 + o) % 4))

    def zdev(o, core):
        return (2 * ((z + o) % 4) + core, orb)

    pr = orb // 2
    def cut(q):
        return pl.ds(pl.multiple_of(q * CH, 128), CH)

    def load(q):
        return pltpu.make_async_copy(half.at[:, cut(q)], block.at[q], lds.at[q])

    for q in range(NCH):
        load(q).start()

    bar = pltpu.get_barrier_semaphore()
    for o in range(1, 8):
        pl.semaphore_signal(bar, inc=1, device_id=((aux + o) % 8, orb), device_id_type=MESH)
    for o in range(1, 4):
        pl.semaphore_signal(bar, inc=1, device_id=ring1(o), device_id_type=MESH)
        pl.semaphore_signal(bar, inc=1, device_id=ring2(o), device_id_type=MESH)
        pl.semaphore_signal(bar, inc=1, device_id=cross(o), device_id_type=MESH)

    def rcopy(src, dst, ss, rs, dev):
        return pltpu.make_async_remote_copy(src_ref=src, dst_ref=dst, send_sem=ss, recv_sem=rs,
                                            device_id=dev, device_id_type=MESH)

    def al48(v):
        return pl.ds(pl.multiple_of(v * 48, 16), 48)

    def mcopy(o):
        rows = pl.ds(pl.multiple_of(aux * 16, 16), 16)
        return rcopy(metric, whole.at[rows], ks.at[o], kr.at[o], ((aux + o) % 8, orb))

    def send(q, o, flip):
        dev = 2 * ((z + o) % 4) + (c + flip) % 2
        return rcopy(snd.at[q, al48(dev)], rcv.at[q, al48(aux)], p1s.at[q, 2 * o + flip], p1r.at[q, aux], (dev, orb))

    def arrival(q, a):
        return rcopy(rcv.at[q, al48(a)], rcv.at[q, al48(a)], p1s.at[q, 0], p1r.at[q, a], (sib, orb))

    def gate(q):
        flags = [jnp.full((1, 128), survive[0, 0, 3 * q + n].astype(f32)) for n in range(3)]
        return jnp.concatenate(flags, axis=1).astype(jnp.bfloat16)

    def sort(q):
        load(q).wait()
        kept = block[q] * gate(q)
        snd[q] = jnp.dot(perm[...], kept, preferred_element_type=f32).astype(jnp.bfloat16)
        rcv[q, al48(aux), :] = snd[q, al48(aux), :]

    def sends(q):
        for o, flip in ORDER:
            send(q, o, flip).start()

    perm[...] = sorting()
    sort(0)
    pl.semaphore_wait(bar, 16)
    for o in range(1, 8):
        mcopy(o).start()
    sends(0)
    whole[pl.ds(pl.multiple_of(aux * 16, 16), 16), :] = metric[...]

    @pl.loop(1, NCH)
    def _(q):
        sort(q)
        sends(q)

    for o in range(1, 8):
        rows = pl.ds(pl.multiple_of((aux + 8 - o) % 8 * 16, 16), 16)
        rcopy(metric, whole.at[rows], ks.at[o], kr.at[o], (sib, orb)).wait_recv()
    m3[...] = spread(whole[...])

    def fcopy(q):
        return rcopy(fb.at[q, pl.ds(0, CH)], fb.at[q, pl.ds(CH, CH)], fs.at[q], fr.at[q], (sib, orb))

    def scales(val):
        val = jnp.maximum(val, TINY)
        lane = lax.broadcasted_iota(jnp.int32, val.shape, 1)
        inv = lax.rsqrt(val)
        yield val * inv, inv
        for h in range(2):
            part = jnp.where((lane >= TR) == (h == 1), val, TINY)
            top = jnp.broadcast_to(jnp.max(part, axis=1, keepdims=True), val.shape)
            tinv = lax.rsqrt(top)
            yield top * tinv * (1.0 / TOP), tinv * TOP

    def tables1(k, rows, val):
        for n, (sc, inv) in enumerate(scales(val)):
            if n == 0:
                cs1[k, rows, :], csi1[k, rows, :] = sc, inv
            else:
                rb1[n - 1, k, rows, :], rbi1[n - 1, k, rows, :] = sc, inv

    def tables(first, terms):
        for i, val in enumerate(terms):
            for n, (sc, inv) in enumerate(scales(val)):
                if n == 0:
                    cs[first + i], csi[first + i] = sc, inv
                else:
                    rb[first + i, n - 1], rbi[first + i, n - 1] = sc, inv

    def gather(level, dev):
        base = 4 * level
        for o in range(1, 4):
            rcopy(dv.at[base], dv.at[base + 4 - o], ds_.at[base + o], dr.at[base + 4 - o], dev(o)).start()

    def gathered(level, dev):
        base = 4 * level
        for o in range(1, 4):
            rcopy(dv.at[base], dv.at[base + o], ds_.at[base + o], dr.at[base + o], dev(o)).wait_recv()
        return [dv[base + o] for o in range(4)]

    def dcopy(q, o):
        return rcopy(dvr.at[0, q], dvr.at[4 - o, q], d1s.at[o, q], d1r.at[4 - o, q], cross(o))

    def enc1(val, n, h, p, q):
        inv = csi1[q, pl.ds(n, 1), :] * rbi1[h, p, pl.ds(n, 1), :]
        return jnp.round(val * inv).astype(jnp.int32).astype(jnp.int16)

    def dec1(val, n, h, p, q):
        sc = cs1[q, pl.ds(n, 1), :] * rb1[h, p, pl.ds(n, 1), :]
        return val.astype(jnp.int32).astype(f32) * sc

    def enc(val, n, h, p, q):
        inv = csi[n, pl.ds(q, 1), :] * rbi[n, h, pl.ds(p, 1), :]
        return jnp.round(val * inv).astype(jnp.int32).astype(jnp.int16)

    def dec(val, n, h, p, q):
        sc = cs[n, pl.ds(q, 1), :] * rb[n, h, pl.ds(p, 1), :]
        return val.astype(jnp.int32).astype(f32) * sc

    def where(t, i):
        p = 2 * (i // 4) + t // 2
        q = 2 * (i % 4) + (i // 4 + c) % 2
        return t % 2, p, q, q >= p

    def slot(u, m):
        return m * 4 + (u - m + 4) % 4

    def source(p, q, h):
        core = (p // 2 + q) % 2
        t, u = 2 * (p % 2) + h, (p // 2 + q // 2) % 4
        return t * (4 - 3 * core) + u * (1 + 3 * core), core

    def place(p, q, h):
        return (p // 2) * 4 + q // 2, (2 * (p % 2) + h - me1 + 4) % 4

    def far(i, n):
        return rcopy(s1f.at[i, pl.ds(n * HR, HR)], r1f.at[n, i], q1fs.at[i, n], q1fr.at[n, i], ring1(1 + 2 * n))

    def near(i, way, dev):
        return rcopy(s1n.at[way, i], r1n.at[way, i], q1ns.at[way, i], q1nr.at[way, i], dev)

    def tile2(role, m):
        return rcopy(s2.at[role - 1, m], r2.at[3 - role, m], q2s.at[role - 1, m], q2r.at[3 - role, m], ring2(role))

    def pair(k):
        fcopy(k).wait_recv()
        both = fb[k]
        ft[k] = both.T
        wide = both.astype(f32)
        wide = wide * wide
        norm = jnp.sum(wide[:CH], axis=0, keepdims=True) + jnp.sum(wide[CH:], axis=0, keepdims=True)
        dvr[0, k] = norm
        for o in range(1, 4):
            dcopy(k, o).start()
        tables1(k, pl.ds(0, 1), norm)

    def each(k, body):
        @pl.loop(0, k + 1)
        def _(p):
            @pl.when((p // 2 + k) % 2 == c)
            def _():
                body(p)

    def compute(k):
        def body(p):
            tile = jnp.dot(ft[p], fb[k], preferred_element_type=f32)
            for h in range(2):
                i, role = place(p, k, h)
                part = tile[h * TR:(h + 1) * TR]

                @pl.when(role == 2)
                def _():
                    s1f[i] = enc1(part, 0, h, p, k)
                    far(i, 0).start()
                    far(i, 1).start()

                @pl.when(role != 2)
                def _():
                    kbuf[(role + 1) // 2, i] = part

        each(k, body)

    def pass_on(k):
        def body(p):
            for h in range(2):
                i, role = place(p, k, h)

                @pl.when(role % 2 == 1)
                def _():
                    way = role // 2
                    rcopy(s1f.at[i, pl.ds(0, HR)], r1f.at[way, i], q1fs.at[i, 0], q1fr.at[way, i], ring1(1)).wait_recv()
                    rows = pl.ds(pl.multiple_of(way * HR, 32), HR)
                    kbuf[1 + way, i, rows, :] = kbuf[1 + way, i, rows, :] + dec1(r1f[way, i], 1 + way, h, p, k)
                    s1n[way, i] = enc1(kbuf[1 + way, i], 3 + way, h, p, k)
                    near(i, way, ring1(role)).start()

        each(k, body)

    def norms(k):
        for o in range(1, 4):
            rcopy(dvr.at[0, k], dvr.at[o, k], d1s.at[o, k], d1r.at[o, k], ring1(o)).wait_recv()
        d = [dvr[o, k] for o in range(4)]
        terms = [d[0], d[3], d[1], d[0] + d[3], d[0] + d[1], d[3] + d[2], d[1] + d[2], d[0]]
        tables1(k, slice(None), jnp.concatenate(terms, axis=0))
        dv[4, pl.ds(k, 1), :] = d[0] + d[1] + d[2] + d[3]

    @pl.loop(0, NCH)
    def _(k):
        for o in range(1, 8):
            arrival(k, (aux + o) % 8).wait_recv()
        fb[k, 0:CH, :] = jnp.dot(m3[...], rcv[k], preferred_element_type=f32).astype(jnp.bfloat16)
        fcopy(k).start()

        @pl.when(k > 0)
        def _():
            compute(k - 1)

        @pl.when(k >= LAG)
        def _():
            norms(k - LAG)
            pass_on(k - LAG)

        pair(k)

    compute(NCH - 1)

    @pl.loop(NCH - LAG, NCH)
    def _(k):
        norms(k)

    gather(1, ring2)

    @pl.loop(NCH - LAG, NCH)
    def _(k):
        pass_on(k)


    d1 = gathered(1, ring2)
    tables(0, d1)
    dv[8] = d1[0] + d1[1] + d1[2] + d1[3]

    def zline(o):
        return zdev(o, c)

    gather(2, zline)
    @pl.loop(0, 16)
    def _(n):
        b = n // 4
        a = 2 * (n % 2) + (n % 4 // 2) * (1 - 2 * c) + c
        i = a * 4 + b
        h, p, q, ok = where(me1, i)
        role = (a + b - me2 + 4) % 4

        @pl.when(ok)
        def _():
            near(i, 0, ring1(1)).wait_recv()
            near(i, 1, ring1(1)).wait_recv()
            tile = kbuf[0, i] + dec1(r1n[0, i], 5, h, p, q) + dec1(r1n[1, i], 6, h, p, q)

            @pl.when(role == 0)
            def _():
                kbuf[0, i] = tile

            @pl.when(role > 0)
            def _():
                s2[role - 1, a] = enc(tile, 0, h, p, q)
                tile2(role, a).start()

    d2 = gathered(2, zline)
    tables(4, d2)

    def last(m, h, p, q):
        return rcopy(s3.at[m], r3.at[z], q3s.at[m], q3r.at[z], (q, 2 * p + h))

    def turned(m, n, h, p, q):
        return rcopy(s4.at[m, n], r4.at[h, z], q4s.at[m, n], q4r.at[h, z], (p, 2 * q + n))

    def here(q, p, h):
        return jnp.logical_and(aux == q, orb == 2 * p + h)

    @pl.loop(0, 4)
    def _(b):
        m = (me2 - b + 4) % 4
        i = m * 4 + b
        h, p, q, ok = where(me1, i)

        @pl.when(ok)
        def _():
            tile = kbuf[0, i]
            for n in range(1, 4):
                rcopy(s2.at[0, m], r2.at[n - 1, m], q2s.at[0, m], q2r.at[n - 1, m], ring2(1)).wait_recv()
                tile = tile + dec(r2[n - 1, m], n, h, p, q)
            code = jnp.round(tile * (csi[4, pl.ds(q, 1), :] * rbi[4, h, pl.ds(p, 1), :]))
            full = code.astype(jnp.int32).astype(jnp.int16)

            @pl.when(here(q, p, h))
            def _():
                r3[z] = full

            @pl.when(jnp.logical_not(here(q, p, h)))
            def _():
                s3[m] = full
                last(m, h, p, q).start()

            @pl.when(q > p)
            def _():
                for n in range(2):
                    part = code[:, n * TR:(n + 1) * TR]
                    flat = jnp.concatenate([part[:HR], part[HR:]], axis=1).astype(jnp.int32).astype(jnp.int16)

                    @pl.when(here(p, q, n))
                    def _():
                        r4[h, z] = flat

                    @pl.when(jnp.logical_not(here(p, q, n)))
                    def _():
                        s4[m, n] = flat
                        turned(m, n, h, p, q).start()

    def other(p, q, h, level):
        src, core = source(p, q, h)
        return jnp.logical_not(jnp.logical_and(aux == 2 * level + core, orb == src))

    @pl.when(aux >= pr)
    def _():
        h = orb % 2
        for o in range(4):
            up = (z + o) % 4

            @pl.when(other(pr, aux, h, up))
            def _():
                rcopy(s3.at[0], r3.at[up], q3s.at[0], q3r.at[up], (sib, orb)).wait_recv()
        tile = dec(r3[z], 4, h, pr, aux)
        for o in range(1, 4):
            tile = tile + dec(r3[(z + o) % 4], 4 + o, h, pr, aux)
        out[...] = tile

    @pl.when(aux < pr)
    def _():
        n = orb % 2
        for h in range(2):
            for o in range(4):
                up = (z + o) % 4

                @pl.when(other(aux, pr, h, up))
                def _():
                    rcopy(s4.at[0, 0], r4.at[h, up], q4s.at[0, 0], q4r.at[h, up], (sib, orb)).wait_recv()
        wide = []
        for h in range(2):
            flat = jnp.zeros((HR, CH), f32)
            for o in range(4):
                sc = cs[4 + o, pl.ds(pr, 1), :]
                low = jnp.concatenate([sc[:, :TR], sc[:, :TR]], axis=1)
                high = jnp.concatenate([sc[:, TR:], sc[:, TR:]], axis=1)
                sc = jnp.where(n == 0, low, high) * rb[4 + o, h, pl.ds(aux, 1), :]
                flat = flat + r4[h, (z + o) % 4].astype(jnp.int32).astype(f32) * sc
            wide.append(jnp.concatenate([flat[:, :TR], flat[:, TR:]], axis=0).T)
        out[...] = jnp.concatenate(wide, axis=1)

    for o in range(1, 8):
        mcopy(o).wait_send()

    @pl.loop(0, NCH)
    def _(q):
        for o, flip in ORDER:
            send(q, o, flip).wait_send()
        fcopy(q).wait_send()
        for o in range(1, 4):
            dcopy(q, o).wait_send()

    for level, dev in ((1, ring2), (2, zline)):
        for o in range(1, 4):
            rcopy(dv.at[4 * level], dv.at[4 * level], ds_.at[4 * level + o], dr.at[4 * level], dev(o)).wait_send()

    for role in range(1, 4):
        @pl.loop(0, 16)
        def _(i):
            @pl.when(where((me1 + role) % 4, i)[3])
            def _():
                if role == 2:
                    far(i, 0).wait_send()
                    far(i, 1).wait_send()
                else:
                    near(i, role // 2, ring1(1)).wait_send()

        @pl.loop(0, 4)
        def _(m):
            @pl.when(where(me1, slot((me2 + role) % 4, m))[3])
            def _():
                tile2(role, m).wait_send()

    @pl.loop(0, 4)
    def _(m):
        h, p, q, ok = where(me1, slot(me2, m))

        @pl.when(jnp.logical_and(ok, jnp.logical_not(here(q, p, h))))
        def _():
            last(m, h, p, q).wait_send()

        for n in range(2):
            @pl.when(jnp.logical_and(jnp.logical_and(ok, q > p), jnp.logical_not(here(p, q, n))))
            def _():
                turned(m, n, h, p, q).wait_send()


def shards(half, metric, survive):
    bf, f32, i16 = jnp.bfloat16, jnp.float32, jnp.int16
    rows = half.reshape(CH, half.shape[-1])
    vm, dma = pltpu.VMEM, pltpu.SemaphoreType.DMA
    scratch = [
        vm((NCH, CH, CH), bf), vm((CH, CH), bf), vm((128, 128), bf),
        vm((NCH, CH, CH), bf), vm((NCH, CH, CH), bf), vm((CH, CH), bf),
        vm((NCH, 2 * CH, CH), bf), vm((NCH, CH, 2 * CH), bf),
        vm((4, NCH, 1, CH), f32), vm((12, 8, CH), f32),
        vm((NCH, 8, CH), f32), vm((NCH, 8, CH), f32), vm((2, NCH, 8, CH), f32), vm((2, NCH, 8, CH), f32),
        vm((8, 8, CH), f32), vm((8, 8, CH), f32), vm((8, 2, 8, CH), f32), vm((8, 2, 8, CH), f32),
        vm((3, 16, TR, CH), f32),
        vm((16, TR, CH), i16), vm((2, 16, HR, CH), i16), vm((2, 16, TR, CH), i16), vm((2, 16, TR, CH), i16),
        vm((3, 4, TR, CH), i16), vm((3, 4, TR, CH), i16),
        vm((4, TR, CH), i16), vm((4, TR, CH), i16), vm((4, 2, HR, CH), i16), vm((2, 4, HR, CH), i16),
        dma((NCH,)), dma((NCH, 8)), dma((NCH, 8)), dma((8,)), dma((8,)), dma((NCH,)), dma((NCH,)),
        dma((4, NCH)), dma((4, NCH)), dma((12,)), dma((12,)),
        dma((16, 2)), dma((2, 16)), dma((2, 16)), dma((2, 16)), dma((3, 4)), dma((3, 4)),
        dma((4,)), dma((4,)), dma((4, 2)), dma((2, 4)),
    ]
    return pl.pallas_call(
        kernel,
        out_shape=jax.ShapeDtypeStruct((TR, CH), f32),
        in_specs=[pl.BlockSpec(memory_space=pl.ANY), pl.BlockSpec(memory_space=pltpu.SMEM),
                  pl.BlockSpec(memory_space=pltpu.VMEM)],
        out_specs=pl.BlockSpec(memory_space=pltpu.VMEM),
        scratch_shapes=scratch,
        compiler_params=pltpu.CompilerParams(collective_id=0, has_side_effects=True,
                                             vmem_limit_bytes=62 * 1024 * 1024),
    )(rows, survive, metric)


def solution(mesh):
    placed = (P("aux", "orb", None), P("aux", None), P("aux", "orb", None))
    return jax.shard_map(shards, mesh=mesh, in_specs=placed, out_specs=P("orb", "aux"), check_vma=False)
```

```python
import jax
import jax.numpy as jnp
from jax import lax
from jax.experimental import pallas as pl
from jax.experimental.pallas import tpu as pltpu
from jax.sharding import PartitionSpec as P

MESH = pl.DeviceIdType.MESH
CH = 384
NCH = 8
TR = 192
HR = 96
LAG = 2
TOP = 32700.0
TINY = 1e-36
ORDER = ((2, 0), (2, 1), (1, 0), (3, 0), (1, 1), (3, 1), (0, 1))


def third(n):
    return jnp.floor((n + 0.5) * (1.0 / 3.0))


def iota(shape, dim):
    return lax.broadcasted_iota(jnp.int32, shape, dim).astype(jnp.float32)


def sorting():
    row, col = iota((CH, CH), 0), iota((CH, CH), 1)
    d = jnp.floor((row + 0.5) * (1.0 / 48.0))
    rest = row - 48.0 * d
    aux = third(rest)
    return jnp.where(col == 21.0 * aux + 3.0 * d + rest, 1.0, 0.0).astype(jnp.bfloat16)


def spread(metric):
    f32, bf = jnp.float32, jnp.bfloat16
    left = jnp.where(third(iota((CH, 128), 0)) == iota((CH, 128), 1), 1.0, 0.0).astype(bf)
    right = jnp.where(third(iota((128, CH), 1)) == iota((128, CH), 0), 1.0, 0.0).astype(bf)
    rows = jnp.dot(left, metric, preferred_element_type=f32).astype(bf)
    wide = jnp.dot(rows, right, preferred_element_type=f32)
    a, b = iota((CH, CH), 0), iota((CH, CH), 1)
    return jnp.where(a - 3.0 * third(a) == b - 3.0 * third(b), wide, 0.0).astype(bf)


def kernel(half, survive, metric, out, block, perm, whole, snd, rcv, m3, fb, ft, dvr, dv, dvx, cs1, csi1, rb1, rbi1, cs, csi, rb, rbi,
           kbuf, s1f, r1f, s1n, r1n, s2, r2, s3, r3, s4, r4,
           lds, p1s, p1r, ks, kr, fs, fr, d1s, d1r, ds_, dr, dxs, dxr, q1fs, q1fr, q1ns, q1nr, q2s, q2r, q3s, q3r, q4s, q4r):
    f32 = jnp.float32
    aux = lax.axis_index("aux")
    orb = lax.axis_index("orb")
    z, c = aux // 2, aux % 2
    x, y = orb // 4, orb % 4
    me1 = x * (1 - c) + y * c
    me2 = z
    me3 = y * (1 - c) + x * c
    sib = 2 * z + 1 - c

    def row_of(t, u):
        return t * (4 - 3 * c) + u * (1 + 3 * c)

    def ring1(o):
        return (aux, row_of((me1 + o) % 4, me3))

    def ring2(o):
        return (2 * ((z + o) % 4) + c, orb)

    def line3(o):
        return (aux, row_of(me1, (me3 + o) % 4))

    def cross(o):
        return (sib, row_of(me1, (me3 + o) % 4))

    pr = orb // 2
    def cut(q):
        return pl.ds(pl.multiple_of(q * CH, 128), CH)

    def load(q):
        return pltpu.make_async_copy(half.at[:, cut(q)], block.at[q], lds.at[q])

    for q in range(NCH):
        load(q).start()

    bar = pltpu.get_barrier_semaphore()
    for o in range(1, 8):
        pl.semaphore_signal(bar, inc=1, device_id=((aux + o) % 8, orb), device_id_type=MESH)
    for o in range(1, 4):
        pl.semaphore_signal(bar, inc=1, device_id=ring1(o), device_id_type=MESH)
        pl.semaphore_signal(bar, inc=1, device_id=line3(o), device_id_type=MESH)
        pl.semaphore_signal(bar, inc=1, device_id=cross(o), device_id_type=MESH)

    def rcopy(src, dst, ss, rs, dev):
        return pltpu.make_async_remote_copy(src_ref=src, dst_ref=dst, send_sem=ss, recv_sem=rs,
                                            device_id=dev, device_id_type=MESH)

    def al48(v):
        return pl.ds(pl.multiple_of(v * 48, 16), 48)

    def mcopy(o):
        rows = pl.ds(pl.multiple_of(aux * 16, 16), 16)
        return rcopy(metric, whole.at[rows], ks.at[o], kr.at[o], ((aux + o) % 8, orb))

    def send(q, o, flip):
        dev = 2 * ((z + o) % 4) + (c + flip) % 2
        return rcopy(snd.at[q, al48(dev)], rcv.at[q, al48(aux)], p1s.at[q, 2 * o + flip], p1r.at[q, aux], (dev, orb))

    def arrival(q, a):
        return rcopy(rcv.at[q, al48(a)], rcv.at[q, al48(a)], p1s.at[q, 0], p1r.at[q, a], (sib, orb))

    def gate(q):
        flags = [jnp.full((1, 128), survive[0, 0, 3 * q + n].astype(f32)) for n in range(3)]
        return jnp.concatenate(flags, axis=1).astype(jnp.bfloat16)

    def sort(q):
        load(q).wait()
        kept = block[q] * gate(q)
        snd[q] = jnp.dot(perm[...], kept, preferred_element_type=f32).astype(jnp.bfloat16)
        rcv[q, al48(aux), :] = snd[q, al48(aux), :]

    def sends(q):
        for o, flip in ORDER:
            send(q, o, flip).start()

    perm[...] = sorting()
    sort(0)
    pl.semaphore_wait(bar, 16)
    for o in range(1, 8):
        mcopy(o).start()
    sends(0)
    whole[pl.ds(pl.multiple_of(aux * 16, 16), 16), :] = metric[...]

    @pl.loop(1, NCH)
    def _(q):
        sort(q)
        sends(q)

    for o in range(1, 8):
        rows = pl.ds(pl.multiple_of((aux + 8 - o) % 8 * 16, 16), 16)
        rcopy(metric, whole.at[rows], ks.at[o], kr.at[o], (sib, orb)).wait_recv()
    m3[...] = spread(whole[...])

    def fcopy(q):
        return rcopy(fb.at[q, pl.ds(0, CH)], fb.at[q, pl.ds(CH, CH)], fs.at[q], fr.at[q], (sib, orb))

    def scales(val):
        val = jnp.maximum(val, TINY)
        lane = lax.broadcasted_iota(jnp.int32, val.shape, 1)
        inv = lax.rsqrt(val)
        yield val * inv, inv
        for h in range(2):
            part = jnp.where((lane >= TR) == (h == 1), val, TINY)
            top = jnp.broadcast_to(jnp.max(part, axis=1, keepdims=True), val.shape)
            tinv = lax.rsqrt(top)
            yield top * tinv * (1.0 / TOP), tinv * TOP

    def tables1(k, rows, val):
        for n, (sc, inv) in enumerate(scales(val)):
            if n == 0:
                cs1[k, rows, :], csi1[k, rows, :] = sc, inv
            else:
                rb1[n - 1, k, rows, :], rbi1[n - 1, k, rows, :] = sc, inv

    def tables(first, terms):
        for i, val in enumerate(terms):
            for n, (sc, inv) in enumerate(scales(val)):
                if n == 0:
                    cs[first + i], csi[first + i] = sc, inv
                else:
                    rb[first + i, n - 1], rbi[first + i, n - 1] = sc, inv

    def gather(level, dev):
        base = 4 * level
        for o in range(1, 4):
            rcopy(dv.at[base], dv.at[base + 4 - o], ds_.at[base + o], dr.at[base + 4 - o], dev(o)).start()

    def gathered(level, dev):
        base = 4 * level
        for o in range(1, 4):
            rcopy(dv.at[base], dv.at[base + o], ds_.at[base + o], dr.at[base + o], dev(o)).wait_recv()
        return [dv[base + o] for o in range(4)]

    def dcopy(q, o):
        return rcopy(dvr.at[0, q], dvr.at[4 - o, q], d1s.at[o, q], d1r.at[4 - o, q], cross(o))

    def enc1(val, n, h, p, q):
        inv = csi1[q, pl.ds(n, 1), :] * rbi1[h, p, pl.ds(n, 1), :]
        return jnp.round(val * inv).astype(jnp.int32).astype(jnp.int16)

    def dec1(val, n, h, p, q):
        sc = cs1[q, pl.ds(n, 1), :] * rb1[h, p, pl.ds(n, 1), :]
        return val.astype(jnp.int32).astype(f32) * sc

    def enc(val, n, h, p, q):
        inv = csi[n, pl.ds(q, 1), :] * rbi[n, h, pl.ds(p, 1), :]
        return jnp.round(val * inv).astype(jnp.int32).astype(jnp.int16)

    def dec(val, n, h, p, q):
        sc = cs[n, pl.ds(q, 1), :] * rb[n, h, pl.ds(p, 1), :]
        return val.astype(jnp.int32).astype(f32) * sc

    def where(t, i):
        p = 2 * (i // 4) + t // 2
        q = 2 * (i % 4) + (i // 4 + c) % 2
        return t % 2, p, q, q >= p

    def slot(u, m):
        return m * 4 + (u - m + 4) % 4

    def source(p, q, h, v):
        core = (p // 2 + q) % 2
        t, u = 2 * (p % 2) + h, (p // 2 + q // 2) % 4
        return 2 * u + core, t * (4 - 3 * core) + v * (1 + 3 * core)

    def place(p, q, h):
        return (p // 2) * 4 + q // 2, (2 * (p % 2) + h - me1 + 4) % 4

    def far(i, n):
        return rcopy(s1f.at[i, pl.ds(n * HR, HR)], r1f.at[n, i], q1fs.at[i, n], q1fr.at[n, i], ring1(1 + 2 * n))

    def near(i, way, dev):
        return rcopy(s1n.at[way, i], r1n.at[way, i], q1ns.at[way, i], q1nr.at[way, i], dev)

    def tile2(role, m):
        return rcopy(s2.at[role - 1, m], r2.at[3 - role, m], q2s.at[role - 1, m], q2r.at[3 - role, m], ring2(role))

    def pair(k):
        fcopy(k).wait_recv()
        both = fb[k]
        ft[k] = both.T
        wide = both.astype(f32)
        wide = wide * wide
        norm = jnp.sum(wide[:CH], axis=0, keepdims=True) + jnp.sum(wide[CH:], axis=0, keepdims=True)
        dvr[0, k] = norm
        for o in range(1, 4):
            dcopy(k, o).start()
        tables1(k, pl.ds(0, 1), norm)

    def each(k, body):
        @pl.loop(0, k + 1)
        def _(p):
            @pl.when((p // 2 + k) % 2 == c)
            def _():
                body(p)

    def compute(k):
        def body(p):
            tile = jnp.dot(ft[p], fb[k], preferred_element_type=f32)
            for h in range(2):
                i, role = place(p, k, h)
                part = tile[h * TR:(h + 1) * TR]

                @pl.when(role == 2)
                def _():
                    s1f[i] = enc1(part, 0, h, p, k)
                    far(i, 0).start()
                    far(i, 1).start()

                @pl.when(role != 2)
                def _():
                    kbuf[(role + 1) // 2, i] = part

        each(k, body)

    def pass_on(k):
        def body(p):
            for h in range(2):
                i, role = place(p, k, h)

                @pl.when(role % 2 == 1)
                def _():
                    way = role // 2
                    rcopy(s1f.at[i, pl.ds(0, HR)], r1f.at[way, i], q1fs.at[i, 0], q1fr.at[way, i], ring1(1)).wait_recv()
                    rows = pl.ds(pl.multiple_of(way * HR, 32), HR)
                    kbuf[1 + way, i, rows, :] = kbuf[1 + way, i, rows, :] + dec1(r1f[way, i], 1 + way, h, p, k)
                    s1n[way, i] = enc1(kbuf[1 + way, i], 3 + way, h, p, k)
                    near(i, way, ring1(role)).start()

        each(k, body)

    def norms(k):
        for o in range(1, 4):
            rcopy(dvr.at[0, k], dvr.at[o, k], d1s.at[o, k], d1r.at[o, k], ring1(o)).wait_recv()
        d = [dvr[o, k] for o in range(4)]
        terms = [d[0], d[3], d[1], d[0] + d[3], d[0] + d[1], d[3] + d[2], d[1] + d[2], d[0]]
        tables1(k, slice(None), jnp.concatenate(terms, axis=0))
        dv[4, pl.ds(k, 1), :] = d[0] + d[1] + d[2] + d[3]

    @pl.loop(0, NCH)
    def _(k):
        for o in range(1, 8):
            arrival(k, (aux + o) % 8).wait_recv()
        fb[k, 0:CH, :] = jnp.dot(m3[...], rcv[k], preferred_element_type=f32).astype(jnp.bfloat16)
        fcopy(k).start()

        @pl.when(k > 0)
        def _():
            compute(k - 1)

        @pl.when(k >= LAG)
        def _():
            norms(k - LAG)
            pass_on(k - LAG)

        pair(k)

    compute(NCH - 1)

    @pl.loop(NCH - LAG, NCH)
    def _(k):
        norms(k)

    gather(1, ring2)

    @pl.loop(NCH - LAG, NCH)
    def _(k):
        pass_on(k)


    d1 = gathered(1, ring2)
    tables(0, d1)
    dv[8] = d1[0] + d1[1] + d1[2] + d1[3]

    gather(2, line3)
    @pl.loop(0, 16)
    def _(n):
        b = n // 4
        a = 2 * (n % 2) + (n % 4 // 2) * (1 - 2 * c) + c
        i = a * 4 + b
        h, p, q, ok = where(me1, i)
        role = (a + b - me2 + 4) % 4

        @pl.when(ok)
        def _():
            near(i, 0, ring1(1)).wait_recv()
            near(i, 1, ring1(1)).wait_recv()
            tile = kbuf[0, i] + dec1(r1n[0, i], 5, h, p, q) + dec1(r1n[1, i], 6, h, p, q)

            @pl.when(role == 0)
            def _():
                kbuf[0, i] = tile

            @pl.when(role > 0)
            def _():
                s2[role - 1, a] = enc(tile, 0, h, p, q)
                tile2(role, a).start()

    d2 = gathered(2, line3)
    tables(4, d2)

    def swap():
        return rcopy(dv.at[pl.ds(8, 4)], dvx, dxs, dxr, (sib, orb))

    swap().start()

    def last(m, h, p, q):
        return rcopy(s3.at[m], r3.at[me3], q3s.at[m], q3r.at[me3], (q, 2 * p + h))

    def turned(m, n, h, p, q):
        return rcopy(s4.at[m, n], r4.at[h, me3], q4s.at[m, n], q4r.at[h, me3], (p, 2 * q + n))

    def here(q, p, h):
        return jnp.logical_and(aux == q, orb == 2 * p + h)

    @pl.loop(0, 4)
    def _(b):
        m = (me2 - b + 4) % 4
        i = m * 4 + b
        h, p, q, ok = where(me1, i)

        @pl.when(ok)
        def _():
            tile = kbuf[0, i]
            for n in range(1, 4):
                rcopy(s2.at[0, m], r2.at[n - 1, m], q2s.at[0, m], q2r.at[n - 1, m], ring2(1)).wait_recv()
                tile = tile + dec(r2[n - 1, m], n, h, p, q)
            code = jnp.round(tile * (csi[4, pl.ds(q, 1), :] * rbi[4, h, pl.ds(p, 1), :]))
            full = code.astype(jnp.int32).astype(jnp.int16)

            @pl.when(here(q, p, h))
            def _():
                r3[me3] = full

            @pl.when(jnp.logical_not(here(q, p, h)))
            def _():
                s3[m] = full
                last(m, h, p, q).start()

            @pl.when(q > p)
            def _():
                for n in range(2):
                    part = code[:, n * TR:(n + 1) * TR]
                    flat = jnp.concatenate([part[:HR], part[HR:]], axis=1).astype(jnp.int32).astype(jnp.int16)

                    @pl.when(here(p, q, n))
                    def _():
                        r4[h, me3] = flat

                    @pl.when(jnp.logical_not(here(p, q, n)))
                    def _():
                        s4[m, n] = flat
                        turned(m, n, h, p, q).start()

    def other(p, q, h, v):
        a, o = source(p, q, h, v)
        return jnp.logical_not(jnp.logical_and(aux == a, orb == o))

    swap().wait_recv()
    tables(8, [dvx[o] for o in range(4)])

    def family(p, q):
        apart = (p // 2 + q + c) % 2
        return 4 + 4 * apart, me3 + apart * (me1 - me3)

    @pl.when(aux >= pr)
    def _():
        h = orb % 2
        first, v = family(pr, aux)
        for o in range(4):
            up = (v + o) % 4

            @pl.when(other(pr, aux, h, up))
            def _():
                rcopy(s3.at[0], r3.at[up], q3s.at[0], q3r.at[up], (sib, orb)).wait_recv()
        tile = dec(r3[v], first, h, pr, aux)
        for o in range(1, 4):
            tile = tile + dec(r3[(v + o) % 4], first + o, h, pr, aux)
        out[...] = tile

    @pl.when(aux < pr)
    def _():
        n = orb % 2
        first, v = family(aux, pr)
        for h in range(2):
            for o in range(4):
                up = (v + o) % 4

                @pl.when(other(aux, pr, h, up))
                def _():
                    rcopy(s4.at[0, 0], r4.at[h, up], q4s.at[0, 0], q4r.at[h, up], (sib, orb)).wait_recv()
        wide = []
        for h in range(2):
            flat = jnp.zeros((HR, CH), f32)
            for o in range(4):
                sc = cs[first + o, pl.ds(pr, 1), :]
                low = jnp.concatenate([sc[:, :TR], sc[:, :TR]], axis=1)
                high = jnp.concatenate([sc[:, TR:], sc[:, TR:]], axis=1)
                sc = jnp.where(n == 0, low, high) * rb[first + o, h, pl.ds(aux, 1), :]
                flat = flat + r4[h, (v + o) % 4].astype(jnp.int32).astype(f32) * sc
            wide.append(jnp.concatenate([flat[:, :TR], flat[:, TR:]], axis=0).T)
        out[...] = jnp.concatenate(wide, axis=1)

    swap().wait_send()
    for o in range(1, 8):
        mcopy(o).wait_send()

    @pl.loop(0, NCH)
    def _(q):
        for o, flip in ORDER:
            send(q, o, flip).wait_send()
        fcopy(q).wait_send()
        for o in range(1, 4):
            dcopy(q, o).wait_send()

    for level, dev in ((1, ring2), (2, line3)):
        for o in range(1, 4):
            rcopy(dv.at[4 * level], dv.at[4 * level], ds_.at[4 * level + o], dr.at[4 * level], dev(o)).wait_send()

    for role in range(1, 4):
        @pl.loop(0, 16)
        def _(i):
            @pl.when(where((me1 + role) % 4, i)[3])
            def _():
                if role == 2:
                    far(i, 0).wait_send()
                    far(i, 1).wait_send()
                else:
                    near(i, role // 2, ring1(1)).wait_send()

        @pl.loop(0, 4)
        def _(m):
            @pl.when(where(me1, slot((me2 + role) % 4, m))[3])
            def _():
                tile2(role, m).wait_send()

    @pl.loop(0, 4)
    def _(m):
        h, p, q, ok = where(me1, slot(me2, m))

        @pl.when(jnp.logical_and(ok, jnp.logical_not(here(q, p, h))))
        def _():
            last(m, h, p, q).wait_send()

        for n in range(2):
            @pl.when(jnp.logical_and(jnp.logical_and(ok, q > p), jnp.logical_not(here(p, q, n))))
            def _():
                turned(m, n, h, p, q).wait_send()


def shards(half, metric, survive):
    bf, f32, i16 = jnp.bfloat16, jnp.float32, jnp.int16
    rows = half.reshape(CH, half.shape[-1])
    vm, dma = pltpu.VMEM, pltpu.SemaphoreType.DMA
    scratch = [
        vm((NCH, CH, CH), bf), vm((CH, CH), bf), vm((128, 128), bf),
        vm((NCH, CH, CH), bf), vm((NCH, CH, CH), bf), vm((CH, CH), bf),
        vm((NCH, 2 * CH, CH), bf), vm((NCH, CH, 2 * CH), bf),
        vm((4, NCH, 1, CH), f32), vm((12, 8, CH), f32), vm((4, 8, CH), f32),
        vm((NCH, 8, CH), f32), vm((NCH, 8, CH), f32), vm((2, NCH, 8, CH), f32), vm((2, NCH, 8, CH), f32),
        vm((12, 8, CH), f32), vm((12, 8, CH), f32), vm((12, 2, 8, CH), f32), vm((12, 2, 8, CH), f32),
        vm((3, 16, TR, CH), f32),
        vm((16, TR, CH), i16), vm((2, 16, HR, CH), i16), vm((2, 16, TR, CH), i16), vm((2, 16, TR, CH), i16),
        vm((3, 4, TR, CH), i16), vm((3, 4, TR, CH), i16),
        vm((4, TR, CH), i16), vm((4, TR, CH), i16), vm((4, 2, HR, CH), i16), vm((2, 4, HR, CH), i16),
        dma((NCH,)), dma((NCH, 8)), dma((NCH, 8)), dma((8,)), dma((8,)), dma((NCH,)), dma((NCH,)),
        dma((4, NCH)), dma((4, NCH)), dma((12,)), dma((12,)), dma, dma,
        dma((16, 2)), dma((2, 16)), dma((2, 16)), dma((2, 16)), dma((3, 4)), dma((3, 4)),
        dma((4,)), dma((4,)), dma((4, 2)), dma((2, 4)),
    ]
    return pl.pallas_call(
        kernel,
        out_shape=jax.ShapeDtypeStruct((TR, CH), f32),
        in_specs=[pl.BlockSpec(memory_space=pl.ANY), pl.BlockSpec(memory_space=pltpu.SMEM),
                  pl.BlockSpec(memory_space=pltpu.VMEM)],
        out_specs=pl.BlockSpec(memory_space=pltpu.VMEM),
        scratch_shapes=scratch,
        compiler_params=pltpu.CompilerParams(collective_id=0, has_side_effects=True,
                                             vmem_limit_bytes=62 * 1024 * 1024),
    )(rows, survive, metric)


def solution(mesh):
    placed = (P("aux", "orb", None), P("aux", None), P("aux", "orb", None))
    return jax.shard_map(shards, mesh=mesh, in_specs=placed, out_specs=P("orb", "aux"), check_vma=False)
```

```python
import jax
import jax.numpy as jnp
from jax import lax
from jax.experimental import pallas as pl
from jax.experimental.pallas import tpu as pltpu
from jax.sharding import PartitionSpec as P

MESH = pl.DeviceIdType.MESH
CH = 384
NCH = 8
TR = 192
HR = 96
LAG = 2
TOP = 32700.0
TINY = 1e-36
ORDER = ((0, 1), (2, 0), (1, 0), (3, 0), (2, 1), (1, 1), (3, 1))


def third(n):
    return jnp.floor((n + 0.5) * (1.0 / 3.0))


def iota(shape, dim):
    return lax.broadcasted_iota(jnp.int32, shape, dim).astype(jnp.float32)


def sorting():
    row, col = iota((CH, CH), 0), iota((CH, CH), 1)
    d = jnp.floor((row + 0.5) * (1.0 / 48.0))
    rest = row - 48.0 * d
    aux = third(rest)
    return jnp.where(col == 21.0 * aux + 3.0 * d + rest, 1.0, 0.0).astype(jnp.bfloat16)


def spread(metric):
    f32, bf = jnp.float32, jnp.bfloat16
    left = jnp.where(third(iota((CH, 128), 0)) == iota((CH, 128), 1), 1.0, 0.0).astype(bf)
    right = jnp.where(third(iota((128, CH), 1)) == iota((128, CH), 0), 1.0, 0.0).astype(bf)
    rows = jnp.dot(left, metric, preferred_element_type=f32).astype(bf)
    wide = jnp.dot(rows, right, preferred_element_type=f32)
    a, b = iota((CH, CH), 0), iota((CH, CH), 1)
    return jnp.where(a - 3.0 * third(a) == b - 3.0 * third(b), wide, 0.0).astype(bf)


def kernel(half, survive, metric, out, block, perm, whole, snd, rcv, m3, fb, ft, dvr, dv, cs1, csi1, rb1, rbi1, cs, csi, rb, rbi,
           kbuf, s1f, r1f, s1n, r1n, s2, r2, s3, r3, s4, r4,
           lds, p1s, p1r, ks, kr, fs, fr, d1s, d1r, ds_, dr, q1fs, q1fr, q1ns, q1nr, q2s, q2r, q3s, q3r, q4s, q4r):
    f32 = jnp.float32
    aux = lax.axis_index("aux")
    orb = lax.axis_index("orb")
    z, c = aux // 2, aux % 2
    x, y = orb // 4, orb % 4
    me1 = x * (1 - c) + y * c
    me2 = y * (1 - c) + x * c
    sib = 2 * z + 1 - c

    def row_of(t, u):
        return t * (4 - 3 * c) + u * (1 + 3 * c)

    def ring1(o):
        return (aux, row_of((me1 + o) % 4, me2))

    def ring2(o):
        return (aux, row_of(me1, (me2 + o) % 4))

    def cross(o):
        return (sib, row_of(me1, (me2 + o) % 4))

    def zdev(o, core):
        return (2 * ((z + o) % 4) + core, orb)

    pr = orb // 2
    def cut(q):
        return pl.ds(pl.multiple_of(q * CH, 128), CH)

    def load(q):
        return pltpu.make_async_copy(half.at[:, cut(q)], block.at[q], lds.at[q])

    for q in range(NCH):
        load(q).start()

    bar = pltpu.get_barrier_semaphore()
    for o in range(1, 8):
        pl.semaphore_signal(bar, inc=1, device_id=((aux + o) % 8, orb), device_id_type=MESH)
    for o in range(1, 4):
        pl.semaphore_signal(bar, inc=1, device_id=ring1(o), device_id_type=MESH)
        pl.semaphore_signal(bar, inc=1, device_id=ring2(o), device_id_type=MESH)
        pl.semaphore_signal(bar, inc=1, device_id=cross(o), device_id_type=MESH)

    def rcopy(src, dst, ss, rs, dev):
        return pltpu.make_async_remote_copy(src_ref=src, dst_ref=dst, send_sem=ss, recv_sem=rs,
                                            device_id=dev, device_id_type=MESH)

    def al48(v):
        return pl.ds(pl.multiple_of(v * 48, 16), 48)

    def mcopy(o):
        rows = pl.ds(pl.multiple_of(aux * 16, 16), 16)
        return rcopy(metric, whole.at[rows], ks.at[o], kr.at[o], ((aux + o) % 8, orb))

    def send(q, o, flip):
        dev = 2 * ((z + o) % 4) + (c + flip) % 2
        return rcopy(snd.at[q, al48(dev)], rcv.at[q, al48(aux)], p1s.at[q, 2 * o + flip], p1r.at[q, aux], (dev, orb))

    def arrival(q, a):
        return rcopy(rcv.at[q, al48(a)], rcv.at[q, al48(a)], p1s.at[q, 0], p1r.at[q, a], (sib, orb))

    def gate(q):
        flags = [jnp.full((1, 128), survive[0, 0, 3 * q + n].astype(f32)) for n in range(3)]
        return jnp.concatenate(flags, axis=1).astype(jnp.bfloat16)

    def sort(q):
        load(q).wait()
        kept = block[q] * gate(q)
        snd[q] = jnp.dot(perm[...], kept, preferred_element_type=f32).astype(jnp.bfloat16)
        rcv[q, al48(aux), :] = snd[q, al48(aux), :]

    def sends(q):
        for o, flip in ORDER:
            send(q, o, flip).start()

    perm[...] = sorting()
    sort(0)
    pl.semaphore_wait(bar, 16)
    for o in range(1, 8):
        mcopy(o).start()
    sends(0)
    whole[pl.ds(pl.multiple_of(aux * 16, 16), 16), :] = metric[...]

    @pl.loop(1, NCH)
    def _(q):
        sort(q)
        sends(q)

    for o in range(1, 8):
        rows = pl.ds(pl.multiple_of((aux + 8 - o) % 8 * 16, 16), 16)
        rcopy(metric, whole.at[rows], ks.at[o], kr.at[o], (sib, orb)).wait_recv()
    m3[...] = spread(whole[...])

    def fcopy(q):
        return rcopy(fb.at[q, pl.ds(0, CH)], fb.at[q, pl.ds(CH, CH)], fs.at[q], fr.at[q], (sib, orb))

    def scales(val):
        val = jnp.maximum(val, TINY)
        lane = lax.broadcasted_iota(jnp.int32, val.shape, 1)
        inv = lax.rsqrt(val)
        yield val * inv, inv
        for h in range(2):
            part = jnp.where((lane >= TR) == (h == 1), val, TINY)
            top = jnp.broadcast_to(jnp.max(part, axis=1, keepdims=True), val.shape)
            tinv = lax.rsqrt(top)
            yield top * tinv * (1.0 / TOP), tinv * TOP

    def tables1(k, rows, val):
        for n, (sc, inv) in enumerate(scales(val)):
            if n == 0:
                cs1[k, rows, :], csi1[k, rows, :] = sc, inv
            else:
                rb1[n - 1, k, rows, :], rbi1[n - 1, k, rows, :] = sc, inv

    def tables(first, terms):
        for i, val in enumerate(terms):
            for n, (sc, inv) in enumerate(scales(val)):
                if n == 0:
                    cs[first + i], csi[first + i] = sc, inv
                else:
                    rb[first + i, n - 1], rbi[first + i, n - 1] = sc, inv

    def gather(level, dev):
        base = 4 * level
        for o in range(1, 4):
            rcopy(dv.at[base], dv.at[base + 4 - o], ds_.at[base + o], dr.at[base + 4 - o], dev(o)).start()

    def gathered(level, dev):
        base = 4 * level
        for o in range(1, 4):
            rcopy(dv.at[base], dv.at[base + o], ds_.at[base + o], dr.at[base + o], dev(o)).wait_recv()
        return [dv[base + o] for o in range(4)]

    def dcopy(q, o):
        return rcopy(dvr.at[0, q], dvr.at[4 - o, q], d1s.at[o, q], d1r.at[4 - o, q], cross(o))

    def enc1(val, n, h, p, q):
        inv = csi1[q, pl.ds(n, 1), :] * rbi1[h, p, pl.ds(n, 1), :]
        return jnp.round(val * inv).astype(jnp.int32).astype(jnp.int16)

    def dec1(val, n, h, p, q):
        sc = cs1[q, pl.ds(n, 1), :] * rb1[h, p, pl.ds(n, 1), :]
        return val.astype(jnp.int32).astype(f32) * sc

    def enc(val, n, h, p, q):
        inv = csi[n, pl.ds(q, 1), :] * rbi[n, h, pl.ds(p, 1), :]
        return jnp.round(val * inv).astype(jnp.int32).astype(jnp.int16)

    def dec(val, n, h, p, q):
        sc = cs[n, pl.ds(q, 1), :] * rb[n, h, pl.ds(p, 1), :]
        return val.astype(jnp.int32).astype(f32) * sc

    def where(t, i):
        p = 2 * (i // 4) + t // 2
        q = 2 * (i % 4) + (i // 4 + c) % 2
        return t % 2, p, q, q >= p

    def slot(u, m):
        return m * 4 + (u - m + 4) % 4

    def source(p, q, h):
        core = (p // 2 + q) % 2
        t, u = 2 * (p % 2) + h, (p // 2 + q // 2) % 4
        return t * (4 - 3 * core) + u * (1 + 3 * core), core

    def place(p, q, h):
        return (p // 2) * 4 + q // 2, (2 * (p % 2) + h - me1 + 4) % 4

    def far(i, n):
        return rcopy(s1f.at[i, pl.ds(n * HR, HR)], r1f.at[n, i], q1fs.at[i, n], q1fr.at[n, i], ring1(1 + 2 * n))

    def near(i, way, dev):
        return rcopy(s1n.at[way, i], r1n.at[way, i], q1ns.at[way, i], q1nr.at[way, i], dev)

    def tile2(role, m):
        return rcopy(s2.at[role - 1, m], r2.at[3 - role, m], q2s.at[role - 1, m], q2r.at[3 - role, m], ring2(role))

    def pair(k):
        fcopy(k).wait_recv()
        both = fb[k]
        ft[k] = both.T
        wide = both.astype(f32)
        wide = wide * wide
        norm = jnp.sum(wide[:CH], axis=0, keepdims=True) + jnp.sum(wide[CH:], axis=0, keepdims=True)
        dvr[0, k] = norm
        for o in range(1, 4):
            dcopy(k, o).start()
        tables1(k, pl.ds(0, 1), norm)

    def each(k, body):
        @pl.loop(0, k + 1)
        def _(p):
            @pl.when((p // 2 + k) % 2 == c)
            def _():
                body(p)

    def compute(k):
        def body(p):
            tile = jnp.dot(ft[p], fb[k], preferred_element_type=f32)
            for h in range(2):
                i, role = place(p, k, h)
                part = tile[h * TR:(h + 1) * TR]

                @pl.when(role == 2)
                def _():
                    s1f[i] = enc1(part, 0, h, p, k)
                    far(i, 0).start()
                    far(i, 1).start()

                @pl.when(role != 2)
                def _():
                    kbuf[(role + 1) // 2, i] = part

        each(k, body)

    def pass_on(k):
        def body(p):
            for h in range(2):
                i, role = place(p, k, h)

                @pl.when(role % 2 == 1)
                def _():
                    way = role // 2
                    rcopy(s1f.at[i, pl.ds(0, HR)], r1f.at[way, i], q1fs.at[i, 0], q1fr.at[way, i], ring1(1)).wait_recv()
                    rows = pl.ds(pl.multiple_of(way * HR, 32), HR)
                    kbuf[1 + way, i, rows, :] = kbuf[1 + way, i, rows, :] + dec1(r1f[way, i], 1 + way, h, p, k)
                    s1n[way, i] = enc1(kbuf[1 + way, i], 3 + way, h, p, k)
                    near(i, way, ring1(role)).start()

        each(k, body)

    def norms(k):
        for o in range(1, 4):
            rcopy(dvr.at[0, k], dvr.at[o, k], d1s.at[o, k], d1r.at[o, k], ring1(o)).wait_recv()
        d = [dvr[o, k] for o in range(4)]
        terms = [d[0], d[3], d[1], d[0] + d[3], d[0] + d[1], d[3] + d[2], d[1] + d[2], d[0]]
        tables1(k, slice(None), jnp.concatenate(terms, axis=0))
        dv[4, pl.ds(k, 1), :] = d[0] + d[1] + d[2] + d[3]

    @pl.loop(0, NCH)
    def _(k):
        for o in range(1, 8):
            arrival(k, (aux + o) % 8).wait_recv()
        fb[k, 0:CH, :] = jnp.dot(m3[...], rcv[k], preferred_element_type=f32).astype(jnp.bfloat16)
        fcopy(k).start()

        @pl.when(k > 0)
        def _():
            compute(k - 1)

        @pl.when(k >= LAG)
        def _():
            norms(k - LAG)
            pass_on(k - LAG)

        pair(k)

    compute(NCH - 1)

    norms(NCH - 2)
    pass_on(NCH - 2)
    norms(NCH - 1)
    gather(1, ring2)
    pass_on(NCH - 1)


    d1 = gathered(1, ring2)
    tables(0, d1)
    dv[8] = d1[0] + d1[1] + d1[2] + d1[3]

    def zline(o):
        return zdev(o, c)

    gather(2, zline)
    @pl.loop(0, 16)
    def _(n):
        b = n // 4
        a = 2 * (n % 2) + (n % 4 // 2) * (1 - 2 * c) + c
        i = a * 4 + b
        h, p, q, ok = where(me1, i)
        role = (a + b - me2 + 4) % 4

        @pl.when(ok)
        def _():
            near(i, 0, ring1(1)).wait_recv()
            near(i, 1, ring1(1)).wait_recv()
            tile = kbuf[0, i] + dec1(r1n[0, i], 5, h, p, q) + dec1(r1n[1, i], 6, h, p, q)

            @pl.when(role == 0)
            def _():
                kbuf[0, i] = tile

            @pl.when(role > 0)
            def _():
                s2[role - 1, a] = enc(tile, 0, h, p, q)
                tile2(role, a).start()

    d2 = gathered(2, zline)
    tables(4, d2)

    def last(m, h, p, q):
        return rcopy(s3.at[m], r3.at[z], q3s.at[m], q3r.at[z], (q, 2 * p + h))

    def turned(m, n, h, p, q):
        return rcopy(s4.at[m, n], r4.at[h, z], q4s.at[m, n], q4r.at[h, z], (p, 2 * q + n))

    def here(q, p, h):
        return jnp.logical_and(aux == q, orb == 2 * p + h)

    @pl.loop(0, 4)
    def _(b):
        m = (me2 - b + 4) % 4
        i = m * 4 + b
        h, p, q, ok = where(me1, i)

        @pl.when(ok)
        def _():
            tile = kbuf[0, i]
            for n in range(1, 4):
                rcopy(s2.at[0, m], r2.at[n - 1, m], q2s.at[0, m], q2r.at[n - 1, m], ring2(1)).wait_recv()
                tile = tile + dec(r2[n - 1, m], n, h, p, q)
            code = jnp.round(tile * (csi[4, pl.ds(q, 1), :] * rbi[4, h, pl.ds(p, 1), :]))
            full = code.astype(jnp.int32).astype(jnp.int16)

            @pl.when(here(q, p, h))
            def _():
                r3[z] = full

            @pl.when(jnp.logical_not(here(q, p, h)))
            def _():
                s3[m] = full
                last(m, h, p, q).start()

            @pl.when(q > p)
            def _():
                for n in range(2):
                    part = code[:, n * TR:(n + 1) * TR]
                    flat = jnp.concatenate([part[:HR], part[HR:]], axis=1).astype(jnp.int32).astype(jnp.int16)

                    @pl.when(here(p, q, n))
                    def _():
                        r4[h, z] = flat

                    @pl.when(jnp.logical_not(here(p, q, n)))
                    def _():
                        s4[m, n] = flat
                        turned(m, n, h, p, q).start()

    def other(p, q, h, level):
        src, core = source(p, q, h)
        return jnp.logical_not(jnp.logical_and(aux == 2 * level + core, orb == src))

    @pl.when(aux >= pr)
    def _():
        h = orb % 2
        for o in range(4):
            up = (z + o) % 4

            @pl.when(other(pr, aux, h, up))
            def _():
                rcopy(s3.at[0], r3.at[up], q3s.at[0], q3r.at[up], (sib, orb)).wait_recv()
        tile = dec(r3[z], 4, h, pr, aux)
        for o in range(1, 4):
            tile = tile + dec(r3[(z + o) % 4], 4 + o, h, pr, aux)
        out[...] = tile

    @pl.when(aux < pr)
    def _():
        n = orb % 2
        for h in range(2):
            for o in range(4):
                up = (z + o) % 4

                @pl.when(other(aux, pr, h, up))
                def _():
                    rcopy(s4.at[0, 0], r4.at[h, up], q4s.at[0, 0], q4r.at[h, up], (sib, orb)).wait_recv()
        wide = []
        for h in range(2):
            flat = jnp.zeros((HR, CH), f32)
            for o in range(4):
                sc = cs[4 + o, pl.ds(pr, 1), :]
                low = jnp.concatenate([sc[:, :TR], sc[:, :TR]], axis=1)
                high = jnp.concatenate([sc[:, TR:], sc[:, TR:]], axis=1)
                sc = jnp.where(n == 0, low, high) * rb[4 + o, h, pl.ds(aux, 1), :]
                flat = flat + r4[h, (z + o) % 4].astype(jnp.int32).astype(f32) * sc
            wide.append(jnp.concatenate([flat[:, :TR], flat[:, TR:]], axis=0).T)
        out[...] = jnp.concatenate(wide, axis=1)

    for o in range(1, 8):
        mcopy(o).wait_send()

    @pl.loop(0, NCH)
    def _(q):
        for o, flip in ORDER:
            send(q, o, flip).wait_send()
        fcopy(q).wait_send()
        for o in range(1, 4):
            dcopy(q, o).wait_send()

    for level, dev in ((1, ring2), (2, zline)):
        for o in range(1, 4):
            rcopy(dv.at[4 * level], dv.at[4 * level], ds_.at[4 * level + o], dr.at[4 * level], dev(o)).wait_send()

    for role in range(1, 4):
        @pl.loop(0, 16)
        def _(i):
            @pl.when(where((me1 + role) % 4, i)[3])
            def _():
                if role == 2:
                    far(i, 0).wait_send()
                    far(i, 1).wait_send()
                else:
                    near(i, role // 2, ring1(1)).wait_send()

        @pl.loop(0, 4)
        def _(m):
            @pl.when(where(me1, slot((me2 + role) % 4, m))[3])
            def _():
                tile2(role, m).wait_send()

    @pl.loop(0, 4)
    def _(m):
        h, p, q, ok = where(me1, slot(me2, m))

        @pl.when(jnp.logical_and(ok, jnp.logical_not(here(q, p, h))))
        def _():
            last(m, h, p, q).wait_send()

        for n in range(2):
            @pl.when(jnp.logical_and(jnp.logical_and(ok, q > p), jnp.logical_not(here(p, q, n))))
            def _():
                turned(m, n, h, p, q).wait_send()


def shards(half, metric, survive):
    bf, f32, i16 = jnp.bfloat16, jnp.float32, jnp.int16
    rows = half.reshape(CH, half.shape[-1])
    vm, dma = pltpu.VMEM, pltpu.SemaphoreType.DMA
    scratch = [
        vm((NCH, CH, CH), bf), vm((CH, CH), bf), vm((128, 128), bf),
        vm((NCH, CH, CH), bf), vm((NCH, CH, CH), bf), vm((CH, CH), bf),
        vm((NCH, 2 * CH, CH), bf), vm((NCH, CH, 2 * CH), bf),
        vm((4, NCH, 1, CH), f32), vm((12, 8, CH), f32),
        vm((NCH, 8, CH), f32), vm((NCH, 8, CH), f32), vm((2, NCH, 8, CH), f32), vm((2, NCH, 8, CH), f32),
        vm((8, 8, CH), f32), vm((8, 8, CH), f32), vm((8, 2, 8, CH), f32), vm((8, 2, 8, CH), f32),
        vm((3, 16, TR, CH), f32),
        vm((16, TR, CH), i16), vm((2, 16, HR, CH), i16), vm((2, 16, TR, CH), i16), vm((2, 16, TR, CH), i16),
        vm((3, 4, TR, CH), i16), vm((3, 4, TR, CH), i16),
        vm((4, TR, CH), i16), vm((4, TR, CH), i16), vm((4, 2, HR, CH), i16), vm((2, 4, HR, CH), i16),
        dma((NCH,)), dma((NCH, 8)), dma((NCH, 8)), dma((8,)), dma((8,)), dma((NCH,)), dma((NCH,)),
        dma((4, NCH)), dma((4, NCH)), dma((12,)), dma((12,)),
        dma((16, 2)), dma((2, 16)), dma((2, 16)), dma((2, 16)), dma((3, 4)), dma((3, 4)),
        dma((4,)), dma((4,)), dma((4, 2)), dma((2, 4)),
    ]
    return pl.pallas_call(
        kernel,
        out_shape=jax.ShapeDtypeStruct((TR, CH), f32),
        in_specs=[pl.BlockSpec(memory_space=pl.ANY), pl.BlockSpec(memory_space=pltpu.SMEM),
                  pl.BlockSpec(memory_space=pltpu.VMEM)],
        out_specs=pl.BlockSpec(memory_space=pltpu.VMEM),
        scratch_shapes=scratch,
        compiler_params=pltpu.CompilerParams(collective_id=0, has_side_effects=True,
                                             vmem_limit_bytes=62 * 1024 * 1024),
    )(rows, survive, metric)


def solution(mesh):
    placed = (P("aux", "orb", None), P("aux", None), P("aux", "orb", None))
    return jax.shard_map(shards, mesh=mesh, in_specs=placed, out_specs=P("orb", "aux"), check_vma=False)
```

```python
import jax
import jax.numpy as jnp
from jax import lax
from jax.experimental import pallas as pl
from jax.experimental.pallas import tpu as pltpu
from jax.sharding import PartitionSpec as P

MESH = pl.DeviceIdType.MESH
CH = 384
NCH = 8
TR = 192
HR = 96
LAG = 2
TOP = 32700.0
TINY = 1e-36
ORDER = ((0, 1), (2, 0), (1, 0), (3, 0), (2, 1), (1, 1), (3, 1))


def third(n):
    return jnp.floor((n + 0.5) * (1.0 / 3.0))


def iota(shape, dim):
    return lax.broadcasted_iota(jnp.int32, shape, dim).astype(jnp.float32)


def sorting():
    row, col = iota((CH, CH), 0), iota((CH, CH), 1)
    d = jnp.floor((row + 0.5) * (1.0 / 48.0))
    rest = row - 48.0 * d
    aux = third(rest)
    return jnp.where(col == 21.0 * aux + 3.0 * d + rest, 1.0, 0.0).astype(jnp.bfloat16)


def spread(metric):
    f32, bf = jnp.float32, jnp.bfloat16
    left = jnp.where(third(iota((CH, 128), 0)) == iota((CH, 128), 1), 1.0, 0.0).astype(bf)
    right = jnp.where(third(iota((128, CH), 1)) == iota((128, CH), 0), 1.0, 0.0).astype(bf)
    rows = jnp.dot(left, metric, preferred_element_type=f32).astype(bf)
    wide = jnp.dot(rows, right, preferred_element_type=f32)
    a, b = iota((CH, CH), 0), iota((CH, CH), 1)
    return jnp.where(a - 3.0 * third(a) == b - 3.0 * third(b), wide, 0.0).astype(bf)


def kernel(half, survive, metric, out, block, perm, whole, snd, rcv, m3, fb, ft, dvr, dv, cs1, csi1, rb1, rbi1, cs, csi, rb, rbi,
           kbuf, s1f, r1f, s1n, r1n, s2, r2, s3, r3, s4, r4,
           lds, p1s, p1r, ks, kr, fs, fr, d1s, d1r, ds_, dr, q1fs, q1fr, q1ns, q1nr, q2s, q2r, q3s, q3r, q4s, q4r):
    f32 = jnp.float32
    aux = lax.axis_index("aux")
    orb = lax.axis_index("orb")
    z, c = aux // 2, aux % 2
    x, y = orb // 4, orb % 4
    me1 = x * (1 - c) + y * c
    me2 = y * (1 - c) + x * c
    sib = 2 * z + 1 - c

    def row_of(t, u):
        return t * (4 - 3 * c) + u * (1 + 3 * c)

    def ring1(o):
        return (aux, row_of((me1 + o) % 4, me2))

    def ring2(o):
        return (aux, row_of(me1, (me2 + o) % 4))

    def cross(o):
        return (sib, row_of(me1, (me2 + o) % 4))

    def zdev(o, core):
        return (2 * ((z + o) % 4) + core, orb)

    pr = orb // 2
    def cut(q):
        return pl.ds(pl.multiple_of(q * CH, 128), CH)

    def load(q):
        return pltpu.make_async_copy(half.at[:, cut(q)], block.at[q], lds.at[q])

    for q in range(NCH):
        load(q).start()

    bar = pltpu.get_barrier_semaphore()
    for o in range(1, 8):
        pl.semaphore_signal(bar, inc=1, device_id=((aux + o) % 8, orb), device_id_type=MESH)
    for o in range(1, 4):
        pl.semaphore_signal(bar, inc=1, device_id=ring1(o), device_id_type=MESH)
        pl.semaphore_signal(bar, inc=1, device_id=ring2(o), device_id_type=MESH)
        pl.semaphore_signal(bar, inc=1, device_id=cross(o), device_id_type=MESH)

    def rcopy(src, dst, ss, rs, dev):
        return pltpu.make_async_remote_copy(src_ref=src, dst_ref=dst, send_sem=ss, recv_sem=rs,
                                            device_id=dev, device_id_type=MESH)

    def al48(v):
        return pl.ds(pl.multiple_of(v * 48, 16), 48)

    def mcopy(o):
        rows = pl.ds(pl.multiple_of(aux * 16, 16), 16)
        return rcopy(metric, whole.at[rows], ks.at[o], kr.at[o], ((aux + o) % 8, orb))

    def send(q, o, flip):
        dev = 2 * ((z + o) % 4) + (c + flip) % 2
        return rcopy(snd.at[q, al48(dev)], rcv.at[q, al48(aux)], p1s.at[q, 2 * o + flip], p1r.at[q, aux], (dev, orb))

    def arrival(q, a):
        return rcopy(rcv.at[q, al48(a)], rcv.at[q, al48(a)], p1s.at[q, 0], p1r.at[q, a], (sib, orb))

    def gate(q):
        flags = [jnp.full((1, 128), survive[0, 0, 3 * q + n].astype(f32)) for n in range(3)]
        return jnp.concatenate(flags, axis=1).astype(jnp.bfloat16)

    def sort(q):
        load(q).wait()
        kept = block[q] * gate(q)
        snd[q] = jnp.dot(perm[...], kept, preferred_element_type=f32).astype(jnp.bfloat16)
        rcv[q, al48(aux), :] = snd[q, al48(aux), :]

    def sends(q):
        for o, flip in ORDER:
            send(q, o, flip).start()

    perm[...] = sorting()
    sort(0)
    pl.semaphore_wait(bar, 16)
    for o in range(1, 8):
        mcopy(o).start()
    sends(0)
    whole[pl.ds(pl.multiple_of(aux * 16, 16), 16), :] = metric[...]

    @pl.loop(1, NCH)
    def _(q):
        sort(q)
        sends(q)

    for o in range(1, 8):
        rows = pl.ds(pl.multiple_of((aux + 8 - o) % 8 * 16, 16), 16)
        rcopy(metric, whole.at[rows], ks.at[o], kr.at[o], (sib, orb)).wait_recv()
    m3[...] = spread(whole[...])

    def fcopy(q):
        return rcopy(fb.at[q, pl.ds(0, CH)], fb.at[q, pl.ds(CH, CH)], fs.at[q], fr.at[q], (sib, orb))

    def scales(val):
        val = jnp.maximum(val, TINY)
        lane = lax.broadcasted_iota(jnp.int32, val.shape, 1)
        inv = lax.rsqrt(val)
        yield val * inv, inv
        for h in range(2):
            part = jnp.where((lane >= TR) == (h == 1), val, TINY)
            top = jnp.broadcast_to(jnp.max(part, axis=1, keepdims=True), val.shape)
            tinv = lax.rsqrt(top)
            yield top * tinv * (1.0 / TOP), tinv * TOP

    def tables1(k, rows, val):
        for n, (sc, inv) in enumerate(scales(val)):
            if n == 0:
                cs1[k, rows, :], csi1[k, rows, :] = sc, inv
            else:
                rb1[n - 1, k, rows, :], rbi1[n - 1, k, rows, :] = sc, inv

    def tables(first, terms):
        for i, val in enumerate(terms):
            for n, (sc, inv) in enumerate(scales(val)):
                if n == 0:
                    cs[first + i], csi[first + i] = sc, inv
                else:
                    rb[first + i, n - 1], rbi[first + i, n - 1] = sc, inv

    def gather(level, dev):
        base = 4 * level
        for o in range(1, 4):
            rcopy(dv.at[base], dv.at[base + 4 - o], ds_.at[base + o], dr.at[base + 4 - o], dev(o)).start()

    def gathered(level, dev):
        base = 4 * level
        for o in range(1, 4):
            rcopy(dv.at[base], dv.at[base + o], ds_.at[base + o], dr.at[base + o], dev(o)).wait_recv()
        return [dv[base + o] for o in range(4)]

    def dcopy(q, o):
        return rcopy(dvr.at[0, q], dvr.at[4 - o, q], d1s.at[o, q], d1r.at[4 - o, q], cross(o))

    def enc1(val, n, h, p, q):
        inv = csi1[q, pl.ds(n, 1), :] * rbi1[h, p, pl.ds(n, 1), :]
        return jnp.round(val * inv).astype(jnp.int32).astype(jnp.int16)

    def dec1(val, n, h, p, q):
        sc = cs1[q, pl.ds(n, 1), :] * rb1[h, p, pl.ds(n, 1), :]
        return val.astype(jnp.int32).astype(f32) * sc

    def enc(val, n, h, p, q):
        inv = csi[n, pl.ds(q, 1), :] * rbi[n, h, pl.ds(p, 1), :]
        return jnp.round(val * inv).astype(jnp.int32).astype(jnp.int16)

    def dec(val, n, h, p, q):
        sc = cs[n, pl.ds(q, 1), :] * rb[n, h, pl.ds(p, 1), :]
        return val.astype(jnp.int32).astype(f32) * sc

    def where(t, i):
        p = 2 * (i // 4) + t // 2
        q = 2 * (i % 4) + (i // 4 + c) % 2
        return t % 2, p, q, q >= p

    def slot(u, m):
        return m * 4 + (u - m + 4) % 4

    def source(p, q, h):
        core = (p // 2 + q) % 2
        t, u = 2 * (p % 2) + h, (p // 2 + q // 2) % 4
        return t * (4 - 3 * core) + u * (1 + 3 * core), core

    def place(p, q, h):
        return (p // 2) * 4 + q // 2, (2 * (p % 2) + h - me1 + 4) % 4

    def far(i, n):
        return rcopy(s1f.at[i, pl.ds(n * HR, HR)], r1f.at[n, i], q1fs.at[i, n], q1fr.at[n, i], ring1(1 + 2 * n))

    def near(i, way, dev):
        return rcopy(s1n.at[way, i], r1n.at[way, i], q1ns.at[way, i], q1nr.at[way, i], dev)

    def tile2(role, m):
        return rcopy(s2.at[role - 1, m], r2.at[3 - role, m], q2s.at[role - 1, m], q2r.at[3 - role, m], ring2(role))

    def pair(k):
        fcopy(k).wait_recv()
        both = fb[k]
        ft[k] = both.T
        wide = both.astype(f32)
        wide = wide * wide
        norm = jnp.sum(wide[:CH], axis=0, keepdims=True) + jnp.sum(wide[CH:], axis=0, keepdims=True)
        dvr[0, k] = norm
        for o in range(1, 4):
            dcopy(k, o).start()
        tables1(k, pl.ds(0, 1), norm)

    def each(k, body):
        @pl.loop(0, k + 1)
        def _(p):
            @pl.when((p // 2 + k) % 2 == c)
            def _():
                body(p)

    def compute(k):
        @pl.loop(0, k // 2 + 1)
        def _(a):
            @pl.when((a + k) % 2 == c)
            def _():
                both = ft[pl.ds(2 * a, 2)].reshape(2 * CH, 2 * CH)
                tile = jnp.dot(both, fb[k], preferred_element_type=f32)
                for n in range(4):
                    p, h = 2 * a + n // 2, n % 2
                    i, role = place(p, k, h)
                    part = tile[n * TR:(n + 1) * TR]

                    @pl.when(jnp.logical_and(role == 2, p <= k))
                    def _():
                        s1f[i] = enc1(part, 0, h, p, k)
                        far(i, 0).start()
                        far(i, 1).start()

                    @pl.when(jnp.logical_and(role != 2, p <= k))
                    def _():
                        kbuf[(role + 1) // 2, i] = part

    def pass_on(k):
        def body(p):
            for h in range(2):
                i, role = place(p, k, h)

                @pl.when(role % 2 == 1)
                def _():
                    way = role // 2
                    rcopy(s1f.at[i, pl.ds(0, HR)], r1f.at[way, i], q1fs.at[i, 0], q1fr.at[way, i], ring1(1)).wait_recv()
                    rows = pl.ds(pl.multiple_of(way * HR, 32), HR)
                    kbuf[1 + way, i, rows, :] = kbuf[1 + way, i, rows, :] + dec1(r1f[way, i], 1 + way, h, p, k)
                    s1n[way, i] = enc1(kbuf[1 + way, i], 3 + way, h, p, k)
                    near(i, way, ring1(role)).start()

        each(k, body)

    def norms(k):
        for o in range(1, 4):
            rcopy(dvr.at[0, k], dvr.at[o, k], d1s.at[o, k], d1r.at[o, k], ring1(o)).wait_recv()
        d = [dvr[o, k] for o in range(4)]
        terms = [d[0], d[3], d[1], d[0] + d[3], d[0] + d[1], d[3] + d[2], d[1] + d[2], d[0]]
        tables1(k, slice(None), jnp.concatenate(terms, axis=0))
        dv[4, pl.ds(k, 1), :] = d[0] + d[1] + d[2] + d[3]

    @pl.loop(0, NCH)
    def _(k):
        for o in range(1, 8):
            arrival(k, (aux + o) % 8).wait_recv()
        fb[k, 0:CH, :] = jnp.dot(m3[...], rcv[k], preferred_element_type=f32).astype(jnp.bfloat16)
        fcopy(k).start()

        @pl.when(k > 0)
        def _():
            compute(k - 1)

        @pl.when(k >= LAG)
        def _():
            norms(k - LAG)
            pass_on(k - LAG)

        pair(k)

    compute(NCH - 1)

    norms(NCH - 2)
    pass_on(NCH - 2)
    norms(NCH - 1)
    gather(1, ring2)
    pass_on(NCH - 1)


    d1 = gathered(1, ring2)
    tables(0, d1)
    dv[8] = d1[0] + d1[1] + d1[2] + d1[3]

    def zline(o):
        return zdev(o, c)

    gather(2, zline)
    @pl.loop(0, 16)
    def _(n):
        b = n // 4
        a = 2 * (n % 2) + (n % 4 // 2) * (1 - 2 * c) + c
        i = a * 4 + b
        h, p, q, ok = where(me1, i)
        role = (a + b - me2 + 4) % 4

        @pl.when(ok)
        def _():
            near(i, 0, ring1(1)).wait_recv()
            near(i, 1, ring1(1)).wait_recv()
            tile = kbuf[0, i] + dec1(r1n[0, i], 5, h, p, q) + dec1(r1n[1, i], 6, h, p, q)

            @pl.when(role == 0)
            def _():
                kbuf[0, i] = tile

            @pl.when(role > 0)
            def _():
                s2[role - 1, a] = enc(tile, 0, h, p, q)
                tile2(role, a).start()

    d2 = gathered(2, zline)
    tables(4, d2)

    def last(m, h, p, q):
        return rcopy(s3.at[m], r3.at[z], q3s.at[m], q3r.at[z], (q, 2 * p + h))

    def turned(m, n, h, p, q):
        return rcopy(s4.at[m, n], r4.at[h, z], q4s.at[m, n], q4r.at[h, z], (p, 2 * q + n))

    def here(q, p, h):
        return jnp.logical_and(aux == q, orb == 2 * p + h)

    @pl.loop(0, 4)
    def _(b):
        m = (me2 - b + 4) % 4
        i = m * 4 + b
        h, p, q, ok = where(me1, i)

        @pl.when(ok)
        def _():
            tile = kbuf[0, i]
            for n in range(1, 4):
                rcopy(s2.at[0, m], r2.at[n - 1, m], q2s.at[0, m], q2r.at[n - 1, m], ring2(1)).wait_recv()
                tile = tile + dec(r2[n - 1, m], n, h, p, q)
            code = jnp.round(tile * (csi[4, pl.ds(q, 1), :] * rbi[4, h, pl.ds(p, 1), :]))
            full = code.astype(jnp.int32).astype(jnp.int16)

            @pl.when(here(q, p, h))
            def _():
                r3[z] = full

            @pl.when(jnp.logical_not(here(q, p, h)))
            def _():
                s3[m] = full
                last(m, h, p, q).start()

            @pl.when(q > p)
            def _():
                for n in range(2):
                    part = code[:, n * TR:(n + 1) * TR]
                    flat = jnp.concatenate([part[:HR], part[HR:]], axis=1).astype(jnp.int32).astype(jnp.int16)

                    @pl.when(here(p, q, n))
                    def _():
                        r4[h, z] = flat

                    @pl.when(jnp.logical_not(here(p, q, n)))
                    def _():
                        s4[m, n] = flat
                        turned(m, n, h, p, q).start()

    def other(p, q, h, level):
        src, core = source(p, q, h)
        return jnp.logical_not(jnp.logical_and(aux == 2 * level + core, orb == src))

    @pl.when(aux >= pr)
    def _():
        h = orb % 2
        for o in range(4):
            up = (z + o) % 4

            @pl.when(other(pr, aux, h, up))
            def _():
                rcopy(s3.at[0], r3.at[up], q3s.at[0], q3r.at[up], (sib, orb)).wait_recv()
        tile = dec(r3[z], 4, h, pr, aux)
        for o in range(1, 4):
            tile = tile + dec(r3[(z + o) % 4], 4 + o, h, pr, aux)
        out[...] = tile

    @pl.when(aux < pr)
    def _():
        n = orb % 2
        for h in range(2):
            for o in range(4):
                up = (z + o) % 4

                @pl.when(other(aux, pr, h, up))
                def _():
                    rcopy(s4.at[0, 0], r4.at[h, up], q4s.at[0, 0], q4r.at[h, up], (sib, orb)).wait_recv()
        wide = []
        for h in range(2):
            flat = jnp.zeros((HR, CH), f32)
            for o in range(4):
                sc = cs[4 + o, pl.ds(pr, 1), :]
                low = jnp.concatenate([sc[:, :TR], sc[:, :TR]], axis=1)
                high = jnp.concatenate([sc[:, TR:], sc[:, TR:]], axis=1)
                sc = jnp.where(n == 0, low, high) * rb[4 + o, h, pl.ds(aux, 1), :]
                flat = flat + r4[h, (z + o) % 4].astype(jnp.int32).astype(f32) * sc
            wide.append(jnp.concatenate([flat[:, :TR], flat[:, TR:]], axis=0).T)
        out[...] = jnp.concatenate(wide, axis=1)

    for o in range(1, 8):
        mcopy(o).wait_send()

    @pl.loop(0, NCH)
    def _(q):
        for o, flip in ORDER:
            send(q, o, flip).wait_send()
        fcopy(q).wait_send()
        for o in range(1, 4):
            dcopy(q, o).wait_send()

    for level, dev in ((1, ring2), (2, zline)):
        for o in range(1, 4):
            rcopy(dv.at[4 * level], dv.at[4 * level], ds_.at[4 * level + o], dr.at[4 * level], dev(o)).wait_send()

    for role in range(1, 4):
        @pl.loop(0, 16)
        def _(i):
            @pl.when(where((me1 + role) % 4, i)[3])
            def _():
                if role == 2:
                    far(i, 0).wait_send()
                    far(i, 1).wait_send()
                else:
                    near(i, role // 2, ring1(1)).wait_send()

        @pl.loop(0, 4)
        def _(m):
            @pl.when(where(me1, slot((me2 + role) % 4, m))[3])
            def _():
                tile2(role, m).wait_send()

    @pl.loop(0, 4)
    def _(m):
        h, p, q, ok = where(me1, slot(me2, m))

        @pl.when(jnp.logical_and(ok, jnp.logical_not(here(q, p, h))))
        def _():
            last(m, h, p, q).wait_send()

        for n in range(2):
            @pl.when(jnp.logical_and(jnp.logical_and(ok, q > p), jnp.logical_not(here(p, q, n))))
            def _():
                turned(m, n, h, p, q).wait_send()


def shards(half, metric, survive):
    bf, f32, i16 = jnp.bfloat16, jnp.float32, jnp.int16
    rows = half.reshape(CH, half.shape[-1])
    vm, dma = pltpu.VMEM, pltpu.SemaphoreType.DMA
    scratch = [
        vm((NCH, CH, CH), bf), vm((CH, CH), bf), vm((128, 128), bf),
        vm((NCH, CH, CH), bf), vm((NCH, CH, CH), bf), vm((CH, CH), bf),
        vm((NCH, 2 * CH, CH), bf), vm((NCH, CH, 2 * CH), bf),
        vm((4, NCH, 1, CH), f32), vm((12, 8, CH), f32),
        vm((NCH, 8, CH), f32), vm((NCH, 8, CH), f32), vm((2, NCH, 8, CH), f32), vm((2, NCH, 8, CH), f32),
        vm((8, 8, CH), f32), vm((8, 8, CH), f32), vm((8, 2, 8, CH), f32), vm((8, 2, 8, CH), f32),
        vm((3, 16, TR, CH), f32),
        vm((16, TR, CH), i16), vm((2, 16, HR, CH), i16), vm((2, 16, TR, CH), i16), vm((2, 16, TR, CH), i16),
        vm((3, 4, TR, CH), i16), vm((3, 4, TR, CH), i16),
        vm((4, TR, CH), i16), vm((4, TR, CH), i16), vm((4, 2, HR, CH), i16), vm((2, 4, HR, CH), i16),
        dma((NCH,)), dma((NCH, 8)), dma((NCH, 8)), dma((8,)), dma((8,)), dma((NCH,)), dma((NCH,)),
        dma((4, NCH)), dma((4, NCH)), dma((12,)), dma((12,)),
        dma((16, 2)), dma((2, 16)), dma((2, 16)), dma((2, 16)), dma((3, 4)), dma((3, 4)),
        dma((4,)), dma((4,)), dma((4, 2)), dma((2, 4)),
    ]
    return pl.pallas_call(
        kernel,
        out_shape=jax.ShapeDtypeStruct((TR, CH), f32),
        in_specs=[pl.BlockSpec(memory_space=pl.ANY), pl.BlockSpec(memory_space=pltpu.SMEM),
                  pl.BlockSpec(memory_space=pltpu.VMEM)],
        out_specs=pl.BlockSpec(memory_space=pltpu.VMEM),
        scratch_shapes=scratch,
        compiler_params=pltpu.CompilerParams(collective_id=0, has_side_effects=True,
                                             vmem_limit_bytes=62 * 1024 * 1024),
    )(rows, survive, metric)


def solution(mesh):
    placed = (P("aux", "orb", None), P("aux", None), P("aux", "orb", None))
    return jax.shard_map(shards, mesh=mesh, in_specs=placed, out_specs=P("orb", "aux"), check_vma=False)
```

```python
import jax
import jax.numpy as jnp
from jax import lax
from jax.experimental import pallas as pl
from jax.experimental.pallas import tpu as pltpu
from jax.sharding import PartitionSpec as P

MESH = pl.DeviceIdType.MESH
CH = 384
NCH = 8
TR = 192
HR = 96
LAG = 2
TOP = 32700.0
TINY = 1e-36
ORDER = ((0, 1), (2, 0), (1, 0), (3, 0), (2, 1), (1, 1), (3, 1))


def third(n):
    return jnp.floor((n + 0.5) * (1.0 / 3.0))


def iota(shape, dim):
    return lax.broadcasted_iota(jnp.int32, shape, dim).astype(jnp.float32)


def sorting():
    row, col = iota((CH, CH), 0), iota((CH, CH), 1)
    d = jnp.floor((row + 0.5) * (1.0 / 48.0))
    rest = row - 48.0 * d
    aux = third(rest)
    return jnp.where(col == 21.0 * aux + 3.0 * d + rest, 1.0, 0.0).astype(jnp.bfloat16)


def spread(metric):
    f32, bf = jnp.float32, jnp.bfloat16
    left = jnp.where(third(iota((CH, 128), 0)) == iota((CH, 128), 1), 1.0, 0.0).astype(bf)
    right = jnp.where(third(iota((128, CH), 1)) == iota((128, CH), 0), 1.0, 0.0).astype(bf)
    rows = jnp.dot(left, metric, preferred_element_type=f32).astype(bf)
    wide = jnp.dot(rows, right, preferred_element_type=f32)
    a, b = iota((CH, CH), 0), iota((CH, CH), 1)
    return jnp.where(a - 3.0 * third(a) == b - 3.0 * third(b), wide, 0.0).astype(bf)


def kernel(half, survive, metric, out, block, perm, whole, snd, rcv, m3, fb, ft, dvr, dv, cs1, csi1, rb1, rbi1, cs, csi, rb, rbi,
           kbuf, s1f, r1f, s1n, r1n, s2, r2, s3, r3, s4, r4,
           lds, p1s, p1r, ks, kr, fs, fr, d1s, d1r, ds_, dr, q1fs, q1fr, q1ns, q1nr, q2s, q2r, q3s, q3r, q4s, q4r):
    f32 = jnp.float32
    aux = lax.axis_index("aux")
    orb = lax.axis_index("orb")
    z, c = aux // 2, aux % 2
    x, y = orb // 4, orb % 4
    me1 = x * (1 - c) + y * c
    me2 = y * (1 - c) + x * c
    sib = 2 * z + 1 - c

    def row_of(t, u):
        return t * (4 - 3 * c) + u * (1 + 3 * c)

    def ring1(o):
        return (aux, row_of((me1 + o) % 4, me2))

    def ring2(o):
        return (aux, row_of(me1, (me2 + o) % 4))

    def cross(o):
        return (sib, row_of(me1, (me2 + o) % 4))

    def zdev(o, core):
        return (2 * ((z + o) % 4) + core, orb)

    pr = orb // 2
    def cut(q):
        return pl.ds(pl.multiple_of(q * CH, 128), CH)

    def load(q):
        return pltpu.make_async_copy(half.at[:, cut(q)], block.at[q], lds.at[q])

    for q in range(NCH):
        load(q).start()

    bar = pltpu.get_barrier_semaphore()
    for o in range(1, 8):
        pl.semaphore_signal(bar, inc=1, device_id=((aux + o) % 8, orb), device_id_type=MESH)
    for o in range(1, 4):
        pl.semaphore_signal(bar, inc=1, device_id=ring1(o), device_id_type=MESH)
        pl.semaphore_signal(bar, inc=1, device_id=ring2(o), device_id_type=MESH)
        pl.semaphore_signal(bar, inc=1, device_id=cross(o), device_id_type=MESH)

    def rcopy(src, dst, ss, rs, dev):
        return pltpu.make_async_remote_copy(src_ref=src, dst_ref=dst, send_sem=ss, recv_sem=rs,
                                            device_id=dev, device_id_type=MESH)

    def al48(v):
        return pl.ds(pl.multiple_of(v * 48, 16), 48)

    def mcopy(o):
        rows = pl.ds(pl.multiple_of(aux * 16, 16), 16)
        return rcopy(metric, whole.at[rows], ks.at[o], kr.at[o], ((aux + o) % 8, orb))

    def send(q, o, flip):
        dev = 2 * ((z + o) % 4) + (c + flip) % 2
        return rcopy(snd.at[q, al48(dev)], rcv.at[q, al48(aux)], p1s.at[q, 2 * o + flip], p1r.at[q, aux], (dev, orb))

    def arrival(q, a):
        return rcopy(rcv.at[q, al48(a)], rcv.at[q, al48(a)], p1s.at[q, 0], p1r.at[q, a], (sib, orb))

    def gate(q):
        flags = [jnp.full((1, 128), survive[0, 0, 3 * q + n].astype(f32)) for n in range(3)]
        return jnp.concatenate(flags, axis=1).astype(jnp.bfloat16)

    def sort(q):
        load(q).wait()
        kept = block[q] * gate(q)
        snd[q] = jnp.dot(perm[...], kept, preferred_element_type=f32).astype(jnp.bfloat16)
        rcv[q, al48(aux), :] = snd[q, al48(aux), :]

    def sends(q):
        for o, flip in ORDER:
            send(q, o, flip).start()

    perm[...] = sorting()
    sort(0)
    pl.semaphore_wait(bar, 16)
    for o in range(1, 8):
        mcopy(o).start()
    sends(0)
    whole[pl.ds(pl.multiple_of(aux * 16, 16), 16), :] = metric[...]

    @pl.loop(1, NCH)
    def _(q):
        sort(q)
        sends(q)

    for o in range(1, 8):
        rows = pl.ds(pl.multiple_of((aux + 8 - o) % 8 * 16, 16), 16)
        rcopy(metric, whole.at[rows], ks.at[o], kr.at[o], (sib, orb)).wait_recv()
    m3[...] = spread(whole[...])

    def fcopy(q):
        return rcopy(fb.at[q, pl.ds(0, CH)], fb.at[q, pl.ds(CH, CH)], fs.at[q], fr.at[q], (sib, orb))

    def scales(val):
        val = jnp.maximum(val, TINY)
        lane = lax.broadcasted_iota(jnp.int32, val.shape, 1)
        inv = lax.rsqrt(val)
        yield val * inv, inv
        for h in range(2):
            part = jnp.where((lane >= TR) == (h == 1), val, TINY)
            top = jnp.broadcast_to(jnp.max(part, axis=1, keepdims=True), val.shape)
            tinv = lax.rsqrt(top)
            yield top * tinv * (1.0 / TOP), tinv * TOP

    def tables1(k, rows, val):
        for n, (sc, inv) in enumerate(scales(val)):
            if n == 0:
                cs1[k, rows, :], csi1[k, rows, :] = sc, inv
            else:
                rb1[n - 1, k, rows, :], rbi1[n - 1, k, rows, :] = sc, inv

    def tables(first, terms):
        for i, val in enumerate(terms):
            for n, (sc, inv) in enumerate(scales(val)):
                if n == 0:
                    cs[first + i], csi[first + i] = sc, inv
                else:
                    rb[first + i, n - 1], rbi[first + i, n - 1] = sc, inv

    def gather(level, dev):
        base = 4 * level
        for o in range(1, 4):
            rcopy(dv.at[base], dv.at[base + 4 - o], ds_.at[base + o], dr.at[base + 4 - o], dev(o)).start()

    def gathered(level, dev):
        base = 4 * level
        for o in range(1, 4):
            rcopy(dv.at[base], dv.at[base + o], ds_.at[base + o], dr.at[base + o], dev(o)).wait_recv()
        return [dv[base + o] for o in range(4)]

    def dcopy(q, o):
        return rcopy(dvr.at[0, q], dvr.at[4 - o, q], d1s.at[o, q], d1r.at[4 - o, q], cross(o))

    def enc1(val, n, h, p, q):
        inv = csi1[q, pl.ds(n, 1), :] * rbi1[h, p, pl.ds(n, 1), :]
        return jnp.round(val * inv).astype(jnp.int32).astype(jnp.int16)

    def dec1(val, n, h, p, q):
        sc = cs1[q, pl.ds(n, 1), :] * rb1[h, p, pl.ds(n, 1), :]
        return val.astype(jnp.int32).astype(f32) * sc

    def enc(val, n, h, p, q):
        inv = csi[n, pl.ds(q, 1), :] * rbi[n, h, pl.ds(p, 1), :]
        return jnp.round(val * inv).astype(jnp.int32).astype(jnp.int16)

    def dec(val, n, h, p, q):
        sc = cs[n, pl.ds(q, 1), :] * rb[n, h, pl.ds(p, 1), :]
        return val.astype(jnp.int32).astype(f32) * sc

    def where(t, i):
        p = 2 * (i // 4) + t // 2
        q = 2 * (i % 4) + (i // 4 + c) % 2
        return t % 2, p, q, q >= p

    def slot(u, m):
        return m * 4 + (u - m + 4) % 4

    def source(p, q, h):
        core = (p // 2 + q) % 2
        t, u = 2 * (p % 2) + h, (p // 2 + q // 2) % 4
        return t * (4 - 3 * core) + u * (1 + 3 * core), core

    def place(p, q, h):
        return (p // 2) * 4 + q // 2, (2 * (p % 2) + h - me1 + 4) % 4

    def far(i, n):
        return rcopy(s1f.at[i, pl.ds(n * HR, HR)], r1f.at[n, i], q1fs.at[i, n], q1fr.at[n, i], ring1(1 + 2 * n))

    def near(i, way, dev):
        return rcopy(s1n.at[way, i], r1n.at[way, i], q1ns.at[way, i], q1nr.at[way, i], dev)

    def tile2(role, m):
        return rcopy(s2.at[role - 1, m], r2.at[3 - role, m], q2s.at[role - 1, m], q2r.at[3 - role, m], ring2(role))

    def pair(k):
        fcopy(k).wait_recv()
        both = fb[k]
        ft[k] = both.T
        wide = both.astype(f32)
        wide = wide * wide
        norm = jnp.sum(wide[:CH], axis=0, keepdims=True) + jnp.sum(wide[CH:], axis=0, keepdims=True)
        dvr[0, k] = norm
        for o in range(1, 4):
            dcopy(k, o).start()
        tables1(k, pl.ds(0, 1), norm)

    def each(k, body):
        @pl.loop(0, k + 1)
        def _(p):
            @pl.when((p // 2 + k) % 2 == c)
            def _():
                body(p)

    def compute(k):
        @pl.loop(0, k // 2 + 1)
        def _(a):
            @pl.when((a + k) % 2 == c)
            def _():
                both = ft[pl.ds(2 * a, 2)].reshape(2 * CH, 2 * CH)
                tile = jnp.dot(both, fb[k], preferred_element_type=f32)
                for n in range(4):
                    p, h = 2 * a + n // 2, n % 2
                    i, role = place(p, k, h)
                    part = tile[n * TR:(n + 1) * TR]

                    @pl.when(jnp.logical_and(role == 2, p <= k))
                    def _():
                        s1f[i] = enc1(part, 0, h, p, k)
                        far(i, 0).start()
                        far(i, 1).start()

                    @pl.when(jnp.logical_and(role != 2, p <= k))
                    def _():
                        kbuf[(role + 1) // 2, i] = part

    def pass_on(k):
        def body(p):
            for h in range(2):
                i, role = place(p, k, h)

                @pl.when(role % 2 == 1)
                def _():
                    way = role // 2
                    rcopy(s1f.at[i, pl.ds(0, HR)], r1f.at[way, i], q1fs.at[i, 0], q1fr.at[way, i], ring1(1)).wait_recv()
                    rows = pl.ds(pl.multiple_of(way * HR, 32), HR)
                    kbuf[1 + way, i, rows, :] = kbuf[1 + way, i, rows, :] + dec1(r1f[way, i], 1 + way, h, p, k)
                    s1n[way, i] = enc1(kbuf[1 + way, i], 3 + way, h, p, k)
                    near(i, way, ring1(role)).start()

        each(k, body)

    def norms(k):
        for o in range(1, 4):
            rcopy(dvr.at[0, k], dvr.at[o, k], d1s.at[o, k], d1r.at[o, k], ring1(o)).wait_recv()
        d = [dvr[o, k] for o in range(4)]
        terms = [d[0], d[3], d[1], d[0] + d[3], d[0] + d[1], d[3] + d[2], d[1] + d[2], d[0]]
        tables1(k, slice(None), jnp.concatenate(terms, axis=0))
        dv[4, pl.ds(k, 1), :] = d[0] + d[1] + d[2] + d[3]

    @pl.loop(0, NCH)
    def _(k):
        for o in range(1, 8):
            arrival(k, (aux + o) % 8).wait_recv()
        fb[k, 0:CH, :] = jnp.dot(m3[...], rcv[k], preferred_element_type=f32).astype(jnp.bfloat16)
        fcopy(k).start()

        @pl.when(k > 0)
        def _():
            compute(k - 1)

        @pl.when(k >= LAG)
        def _():
            norms(k - LAG)
            pass_on(k - LAG)

        pair(k)

    compute(NCH - 1)

    norms(NCH - 2)
    pass_on(NCH - 2)
    norms(NCH - 1)
    gather(1, ring2)
    pass_on(NCH - 1)


    d1 = gathered(1, ring2)
    dv[8] = d1[0] + d1[1] + d1[2] + d1[3]

    def zline(o):
        return zdev(o, c)

    gather(2, zline)
    tables(0, d1)
    @pl.loop(0, 16)
    def _(n):
        b = n // 4
        a = 2 * (n % 2) + (n % 4 // 2) * (1 - 2 * c) + c
        i = a * 4 + b
        h, p, q, ok = where(me1, i)
        role = (a + b - me2 + 4) % 4

        @pl.when(ok)
        def _():
            near(i, 0, ring1(1)).wait_recv()
            near(i, 1, ring1(1)).wait_recv()
            tile = kbuf[0, i] + dec1(r1n[0, i], 5, h, p, q) + dec1(r1n[1, i], 6, h, p, q)

            @pl.when(role == 0)
            def _():
                kbuf[0, i] = tile

            @pl.when(role > 0)
            def _():
                s2[role - 1, a] = enc(tile, 0, h, p, q)
                tile2(role, a).start()

    d2 = gathered(2, zline)
    tables(4, d2)

    def last(m, h, p, q):
        return rcopy(s3.at[m], r3.at[z], q3s.at[m], q3r.at[z], (q, 2 * p + h))

    def turned(m, n, h, p, q):
        return rcopy(s4.at[m, n], r4.at[h, z], q4s.at[m, n], q4r.at[h, z], (p, 2 * q + n))

    def here(q, p, h):
        return jnp.logical_and(aux == q, orb == 2 * p + h)

    @pl.loop(0, 4)
    def _(b):
        m = (me2 - b + 4) % 4
        i = m * 4 + b
        h, p, q, ok = where(me1, i)

        @pl.when(ok)
        def _():
            tile = kbuf[0, i]
            for n in range(1, 4):
                rcopy(s2.at[0, m], r2.at[n - 1, m], q2s.at[0, m], q2r.at[n - 1, m], ring2(1)).wait_recv()
                tile = tile + dec(r2[n - 1, m], n, h, p, q)
            code = jnp.round(tile * (csi[4, pl.ds(q, 1), :] * rbi[4, h, pl.ds(p, 1), :]))
            full = code.astype(jnp.int32).astype(jnp.int16)

            @pl.when(here(q, p, h))
            def _():
                r3[z] = full

            @pl.when(jnp.logical_not(here(q, p, h)))
            def _():
                s3[m] = full
                last(m, h, p, q).start()

            @pl.when(q > p)
            def _():
                for n in range(2):
                    part = code[:, n * TR:(n + 1) * TR]
                    flat = jnp.concatenate([part[:HR], part[HR:]], axis=1).astype(jnp.int32).astype(jnp.int16)

                    @pl.when(here(p, q, n))
                    def _():
                        r4[h, z] = flat

                    @pl.when(jnp.logical_not(here(p, q, n)))
                    def _():
                        s4[m, n] = flat
                        turned(m, n, h, p, q).start()

    def other(p, q, h, level):
        src, core = source(p, q, h)
        return jnp.logical_not(jnp.logical_and(aux == 2 * level + core, orb == src))

    @pl.when(aux >= pr)
    def _():
        h = orb % 2
        for o in range(4):
            up = (z + o) % 4

            @pl.when(other(pr, aux, h, up))
            def _():
                rcopy(s3.at[0], r3.at[up], q3s.at[0], q3r.at[up], (sib, orb)).wait_recv()
        tile = dec(r3[z], 4, h, pr, aux)
        for o in range(1, 4):
            tile = tile + dec(r3[(z + o) % 4], 4 + o, h, pr, aux)
        out[...] = tile

    @pl.when(aux < pr)
    def _():
        n = orb % 2
        for h in range(2):
            for o in range(4):
                up = (z + o) % 4

                @pl.when(other(aux, pr, h, up))
                def _():
                    rcopy(s4.at[0, 0], r4.at[h, up], q4s.at[0, 0], q4r.at[h, up], (sib, orb)).wait_recv()
        wide = []
        for h in range(2):
            flat = jnp.zeros((HR, CH), f32)
            for o in range(4):
                sc = cs[4 + o, pl.ds(pr, 1), :]
                low = jnp.concatenate([sc[:, :TR], sc[:, :TR]], axis=1)
                high = jnp.concatenate([sc[:, TR:], sc[:, TR:]], axis=1)
                sc = jnp.where(n == 0, low, high) * rb[4 + o, h, pl.ds(aux, 1), :]
                flat = flat + r4[h, (z + o) % 4].astype(jnp.int32).astype(f32) * sc
            wide.append(jnp.concatenate([flat[:, :TR], flat[:, TR:]], axis=0).T)
        out[...] = jnp.concatenate(wide, axis=1)

    for o in range(1, 8):
        mcopy(o).wait_send()

    @pl.loop(0, NCH)
    def _(q):
        for o, flip in ORDER:
            send(q, o, flip).wait_send()
        fcopy(q).wait_send()
        for o in range(1, 4):
            dcopy(q, o).wait_send()

    for level, dev in ((1, ring2), (2, zline)):
        for o in range(1, 4):
            rcopy(dv.at[4 * level], dv.at[4 * level], ds_.at[4 * level + o], dr.at[4 * level], dev(o)).wait_send()

    for role in range(1, 4):
        @pl.loop(0, 16)
        def _(i):
            @pl.when(where((me1 + role) % 4, i)[3])
            def _():
                if role == 2:
                    far(i, 0).wait_send()
                    far(i, 1).wait_send()
                else:
                    near(i, role // 2, ring1(1)).wait_send()

        @pl.loop(0, 4)
        def _(m):
            @pl.when(where(me1, slot((me2 + role) % 4, m))[3])
            def _():
                tile2(role, m).wait_send()

    @pl.loop(0, 4)
    def _(m):
        h, p, q, ok = where(me1, slot(me2, m))

        @pl.when(jnp.logical_and(ok, jnp.logical_not(here(q, p, h))))
        def _():
            last(m, h, p, q).wait_send()

        for n in range(2):
            @pl.when(jnp.logical_and(jnp.logical_and(ok, q > p), jnp.logical_not(here(p, q, n))))
            def _():
                turned(m, n, h, p, q).wait_send()


def shards(half, metric, survive):
    bf, f32, i16 = jnp.bfloat16, jnp.float32, jnp.int16
    rows = half.reshape(CH, half.shape[-1])
    vm, dma = pltpu.VMEM, pltpu.SemaphoreType.DMA
    scratch = [
        vm((NCH, CH, CH), bf), vm((CH, CH), bf), vm((128, 128), bf),
        vm((NCH, CH, CH), bf), vm((NCH, CH, CH), bf), vm((CH, CH), bf),
        vm((NCH, 2 * CH, CH), bf), vm((NCH, CH, 2 * CH), bf),
        vm((4, NCH, 1, CH), f32), vm((12, 8, CH), f32),
        vm((NCH, 8, CH), f32), vm((NCH, 8, CH), f32), vm((2, NCH, 8, CH), f32), vm((2, NCH, 8, CH), f32),
        vm((8, 8, CH), f32), vm((8, 8, CH), f32), vm((8, 2, 8, CH), f32), vm((8, 2, 8, CH), f32),
        vm((3, 16, TR, CH), f32),
        vm((16, TR, CH), i16), vm((2, 16, HR, CH), i16), vm((2, 16, TR, CH), i16), vm((2, 16, TR, CH), i16),
        vm((3, 4, TR, CH), i16), vm((3, 4, TR, CH), i16),
        vm((4, TR, CH), i16), vm((4, TR, CH), i16), vm((4, 2, HR, CH), i16), vm((2, 4, HR, CH), i16),
        dma((NCH,)), dma((NCH, 8)), dma((NCH, 8)), dma((8,)), dma((8,)), dma((NCH,)), dma((NCH,)),
        dma((4, NCH)), dma((4, NCH)), dma((12,)), dma((12,)),
        dma((16, 2)), dma((2, 16)), dma((2, 16)), dma((2, 16)), dma((3, 4)), dma((3, 4)),
        dma((4,)), dma((4,)), dma((4, 2)), dma((2, 4)),
    ]
    return pl.pallas_call(
        kernel,
        out_shape=jax.ShapeDtypeStruct((TR, CH), f32),
        in_specs=[pl.BlockSpec(memory_space=pl.ANY), pl.BlockSpec(memory_space=pltpu.SMEM),
                  pl.BlockSpec(memory_space=pltpu.VMEM)],
        out_specs=pl.BlockSpec(memory_space=pltpu.VMEM),
        scratch_shapes=scratch,
        compiler_params=pltpu.CompilerParams(collective_id=0, has_side_effects=True,
                                             vmem_limit_bytes=62 * 1024 * 1024),
    )(rows, survive, metric)


def solution(mesh):
    placed = (P("aux", "orb", None), P("aux", None), P("aux", "orb", None))
    return jax.shard_map(shards, mesh=mesh, in_specs=placed, out_specs=P("orb", "aux"), check_vma=False)
```
